32 devices in a mesh: tok: 8 (over z, y), voc: 4 (over x, core).
Axes of the slice: x: 2, y: 2, z: 4, core: 2. Of those that a mesh axis runs over, the one named last changes fastest.
Arguments:
- hidden: bfloat16 [1024, 2048], P('tok'), may hold values from -6 to 6
- mix_weight: bfloat16 [4, 2048], P(None, 'voc'), may hold values from -0.0546875 to 0.0546875
- comp_proj: bfloat16 [2048, 4, 2048], P(None, None, 'voc'), may hold values from -0.110485435 to 0.110485435
- vocab_weight: bfloat16 [2048, 1024], P(None, 'voc'), may hold values from -0.625 to 0.625
- log_normalizer: float32 [4, 1024], P(None, 'tok'), may hold values from 11 to 11.6
- targets: int32 [1024], P('tok'), may hold values from 0 to 1023
- loss_grad: float32 [1024], P('tok'), may hold values from 0.5 to 1.5
Outputs:
- hidden_grad: bfloat16 [1024, 2048], P('tok', 'voc')
- proj_grad: bfloat16 [2048, 4, 2048], P('tok', None, 'voc')
- vocab_grad: bfloat16 [2048, 1024], P('tok', 'voc')
The draws below stay inside these ranges and needn't reach their ends.
All inputs are finite; a program needn't handle non-finite values.
Results may differ from the reference program's by a relative error of at most 0.02.
Values may be sent and summed in bfloat16 or wider, within the bound.
A program may use at most 64 MiB of HBM per device.

```python
import jax
import jax.numpy as jnp
from jax import lax

D = 2048
K = 4
TOK_DEV = 128
V_DEV = 256
TOKENS = 1024
VOCAB = 1024
N_TOK = 8
N_VOC = 4


def draw_comp_proj(key, part):
    base_key = jax.random.fold_in(key, 11)
    noise_key = jax.random.fold_in(key, 12)
    shared = jax.random.truncated_normal(base_key, -4.0, 4.0, (D, 1, D), jnp.float32)
    private = jax.random.truncated_normal(noise_key, -4.0, 4.0, (D, K, D), jnp.float32)
    values = (0.98869 * shared + 0.15 * private) * D ** (-0.5)
    return values.astype(jnp.bfloat16)


def set_ends(array, stream_key, low, top_value):
    longest = array.shape.index(max(array.shape))
    spots = []
    for shift in (0, 1):
        where = [jax.random.randint(jax.random.fold_in(stream_key, axis), (), 0, length) for axis, length in enumerate(array.shape)]
        where[longest] = (where[longest] + shift) % array.shape[longest]
        spots.append(tuple(where))
    return array.at[spots[0]].set(low).at[spots[1]].set(top_value)


def level_of(key, shape, cuts, smallest, high):
    def one(position, parts):
        heights = jax.random.uniform(jax.random.fold_in(jax.random.fold_in(key, 6), position), (parts,), jnp.float32, smallest / len(cuts), high / len(cuts))
        return jnp.repeat(jnp.exp(heights), shape[position] // parts).reshape((-1,) + (1,) * (len(shape) - position - 1))

    level = one(*cuts[0])
    for cut in cuts[1:]:
        level = level * one(*cut)
    return level


def noise(key, extent, width, reach, split=(), kind=jnp.bfloat16):
    entries = jax.random.normal(key, extent, jnp.float32) * width
    if len(split) > 0:
        entries = level_of(key, extent, split, -0.22, 0.18) * entries
    return jnp.clip(entries, min=-reach, max=reach).astype(kind)


def setup_inputs(seed: int = 0) -> dict:
    key_of = jax.random.split(jax.random.key(seed), 8)
    hidden = noise(key_of[0], (TOKENS, D), 1.0, 6.0, ((0, 8),))
    mix_weight = noise(key_of[1], (K, D), (6 * D) ** -0.5, 0.0546875, ((1, 4),))
    comp_proj = draw_comp_proj(jax.random.fold_in(key_of[7], 71), 0)
    vocab_weight = noise(key_of[3], (D, VOCAB), 0.1, 0.625, ((1, 4),))
    log_normalizer = jnp.clip(11.0 + 0.6000004 * jax.random.uniform(key_of[4], (K, TOKENS), jnp.float32) ** level_of(key_of[4], (K, TOKENS), ((1, 8),), -0.2, 0.2), 11.0, 11.6)
    targets = set_ends(jax.random.randint(key_of[5], (TOKENS,), 0, VOCAB), jax.random.fold_in(key_of[5], 1), 0, VOCAB - 1).astype(jnp.int32)
    loss_grad = jnp.clip(0.5 + 1.0 * jax.random.uniform(key_of[6], (TOKENS,), jnp.float32) ** level_of(key_of[6], (TOKENS,), ((0, 8),), -0.2, 0.2), 0.5, 1.5)
    return {"hidden": hidden, "mix_weight": mix_weight, "comp_proj": comp_proj, "vocab_weight": vocab_weight, "log_normalizer": log_normalizer, "targets": targets, "loss_grad": loss_grad}


def rounded(values):
    return lax.optimization_barrier(values.astype(jnp.bfloat16)).astype(jnp.float32)


def reference(hidden, mix_weight, comp_proj, vocab_weight, log_normalizer, targets, loss_grad):
    highest = lax.Precision.HIGHEST
    weight_full = vocab_weight.astype(jnp.float32)
    proj_full = comp_proj.astype(jnp.float32)
    mix_full = mix_weight.astype(jnp.float32)
    vocab_ids = jnp.arange(VOCAB, dtype=jnp.int32)
    hidden_groups = hidden.reshape(N_TOK, TOK_DEV, D)
    norm_groups = jnp.transpose(log_normalizer.reshape(K, N_TOK, TOK_DEV), (1, 0, 2))
    target_groups = targets.reshape(N_TOK, TOK_DEV)
    cotangent_groups = loss_grad.reshape(N_TOK, TOK_DEV)

    def one_group(running, inputs):
        vocab_sum, proj_sum = running
        states, normalizer, wanted, cotangent = inputs
        states_f = states.astype(jnp.float32)
        contexts = jnp.tanh(jnp.einsum("td,dke->tke", states_f, proj_full, precision=highest)).astype(jnp.bfloat16)
        context_f = contexts.astype(jnp.float32)
        logits = jnp.einsum("tkd,dv->ktv", context_f, weight_full, precision=highest)
        mixing = jnp.einsum("td,kd->kt", states_f, mix_full, precision=highest)
        onehot = (wanted[:, None] == vocab_ids[None, :]).astype(jnp.float32)
        target = jnp.sum(logits * onehot[None], axis=2)
        exp_mix = jnp.exp(mixing)
        weights = exp_mix / jnp.sum(exp_mix, axis=0, keepdims=True)
        likely = jnp.exp(target - normalizer)
        joint_mass = weights * likely
        posterior = joint_mass / jnp.sum(joint_mass, axis=0, keepdims=True)
        factor = cotangent[None, :] * posterior
        logit_grad = (factor[:, :, None] * (jnp.exp(logits - normalizer[:, :, None]) - onehot[None])).astype(jnp.bfloat16)
        mixing_grad = cotangent[None, :] * (weights - posterior)
        grad_f = logit_grad.astype(jnp.float32)
        vocab_part = jnp.einsum("tkd,ktv->dv", context_f, grad_f, precision=highest)
        vocab_sum = vocab_sum + rounded(vocab_part)
        blocks = jnp.einsum("ktbv,dbv->btkd", grad_f.reshape(K, TOK_DEV, N_VOC, V_DEV), weight_full.reshape(D, N_VOC, V_DEV), precision=highest)
        context_grad = jnp.sum(rounded(blocks), axis=0)
        pre_grad = rounded(context_grad * (1.0 - context_f * context_f))
        hidden_grad = (jnp.einsum("tke,jke->tj", pre_grad, proj_full, precision=highest) + jnp.einsum("kt,kd->td", mixing_grad, mix_full, precision=highest)).astype(jnp.bfloat16)
        proj_sum = proj_sum + jnp.einsum("tj,tke->jke", states_f, pre_grad, precision=highest)
        return (vocab_sum, proj_sum), hidden_grad

    start_state = (jnp.zeros((D, VOCAB), jnp.float32), jnp.zeros((D, K, D), jnp.float32))
    final_state, hidden_grads = lax.scan(one_group, start_state, (hidden_groups, norm_groups, target_groups, cotangent_groups))
    vocab_sum, proj_sum = final_state
    return hidden_grads.reshape(TOKENS, D), proj_sum.astype(jnp.bfloat16), vocab_sum.astype(jnp.bfloat16)
```

```python
import functools

import jax
import jax.numpy as jnp
from jax import lax
from jax.experimental import pallas as pl
from jax.experimental.pallas import tpu as pltpu
from jax.sharding import PartitionSpec as P

MESH = pl.DeviceIdType.MESH
F32 = jnp.float32
BF16 = jnp.bfloat16
NT = (((1,), (1,)), ((), ()))
TN = (((0,), (0,)), ((), ()))


def column(row, lanes):
    wide = jnp.broadcast_to(row, (128, row.shape[1])).T
    return jnp.concatenate([wide] * (lanes // 128), axis=1)


def kernel(
    M, N,
    hidden, mix, proj_hbm, vw, logz, targets, loss,
    out_hidden, out_proj, out_vocab,
    w, ctx, mix_all, hblk, hrow, htr, logit, lg, tgt,
    cgs, cgr, cgx, xr, own_cg, vgb, vgy, vsum, vout, vin, pg, hss, hsr, own_hs, acc, psend, precv, mgrad,
    w_sem, ctx_s, ctx_f, ctx_r, mix_s, mix_r, hid_s, hid_r, tgt_s, tgt_r,
    cgp_s, cgp_r, cgx_s, cgx_r, vy_s, vy_r, vz_s, vz_r, hs_s, hs_r, ag_s, ag_r, pp_s, pp_r,
):
    K, D, E = w.shape
    T = hidden.shape[0]
    V = vw.shape[1]
    R = D // M
    half = N // 2
    Z = M // 2
    me_t = lax.axis_index("tok")
    me_v = lax.axis_index("voc")
    chip = me_v // 2
    core = me_v % 2
    partner = me_v + 1 - 2 * core
    z = me_t // 2
    y = me_t % 2
    ypart = me_t + 1 - 2 * y
    sends = []

    def remote(src, dst, ss, rs, dev):
        return pltpu.make_async_remote_copy(
            src_ref=src, dst_ref=dst, send_sem=ss, recv_sem=rs,
            device_id=dev, device_id_type=MESH,
        )

    def send(src, dst, ss, rs, dev):
        c = remote(src, dst, ss, rs, dev)
        c.start()
        sends.append((None, c))

    def arrived(ref, rs, ss):
        remote(ref, ref, ss, rs, {"voc": partner}).wait_recv()

    for k in range(K):
        pltpu.make_async_copy(proj_hbm.at[k], w.at[k], w_sem.at[k]).start()
    for j in range(M):
        hblk[j // 2, j % 2] = hidden[:, j * R:(j + 1) * R]

    bar = pltpu.get_barrier_semaphore()
    for d in range(1, M):
        pl.semaphore_signal(bar, inc=1, device_id={"tok": lax.rem(me_t + d, M)}, device_id_type=MESH)
    for d in range(1, N):
        pl.semaphore_signal(bar, inc=1, device_id={"voc": lax.rem(me_v + d, N)}, device_id_type=MESH)
    pl.semaphore_wait(bar, M + N - 2)

    for d in range(1, N):
        send(mix, mix_all.at[d], mix_s.at[d], mix_r.at[d], {"voc": lax.rem(me_v + d, N)})
    mix_all[0] = mix[...]
    for d in range(1, Z):
        zz = lax.rem(z + d, Z)
        send(hblk.at[zz], hrow.at[:, pl.ds(z * T, T)], hid_s.at[d], hid_r.at[d],
             {"tok": zz * 2 + y})
    hrow[:, rows_of(z, T), :] = hblk[z]

    for k in range(K):
        pltpu.make_async_copy(proj_hbm.at[k], w.at[k], w_sem.at[k]).wait()
        ctx[me_v, k * T:(k + 1) * T, :] = jnp.tanh(
            jnp.dot(hidden[...], w[k], preferred_element_type=F32)
        ).astype(BF16)
        piece = ctx.at[me_v, pl.ds(k * T, T)]
        for i in range(1, half):
            send(piece, piece, ctx_s.at[i, k], ctx_r.at[me_v, k],
                 {"voc": lax.rem(chip + i, half) * 2 + core})
        send(piece, piece, ctx_s.at[0, k], ctx_r.at[me_v, k], {"voc": partner})

    def add_logits(s, first=False):
        part = jnp.dot(ctx[s], vw[pl.ds(pl.multiple_of(s * E, E), E), :],
                       preferred_element_type=F32)
        logit[...] = part if first else logit[...] + part

    add_logits(me_v, True)
    for k in range(K):
        arrived(ctx.at[partner, pl.ds(k * T, T)], ctx_r.at[partner, k], ctx_s.at[0, k])
    add_logits(partner)

    tcol = column(targets[...].astype(F32), V)
    ids = (me_v * V + lax.broadcasted_iota(jnp.int32, (T, V), 1)).astype(F32)
    onehot = (tcol == ids).astype(F32)
    for d in range(1, N):
        arrived(mix_all.at[d], mix_r.at[d], mix_s.at[d])
    mixing = jnp.zeros((K, T), F32)
    for d in range(N):
        s = lax.rem(me_v - d + N, N)
        mixing = mixing + lax.dot_general(
            mix_all[d], hidden[:, pl.ds(pl.multiple_of(s * E, E), E)], NT,
            preferred_element_type=F32)
    exp_mix = jnp.exp(mixing)
    weights = exp_mix / jnp.sum(exp_mix, axis=0, keepdims=True)

    for i in range(1, half):
        s = lax.rem(chip - i + half, half) * 2 + core
        for k in range(K):
            piece = ctx.at[s, pl.ds(k * T, T)]
            arrived(piece, ctx_r.at[s, k], ctx_s.at[i, k])
            send(piece, piece, ctx_f.at[i, k], ctx_r.at[s, k], {"voc": partner})
        add_logits(s)
    for i in range(1, half):
        s = lax.rem(chip - i + half, half) * 2 + 1 - core
        for k in range(K):
            arrived(ctx.at[s, pl.ds(k * T, T)], ctx_r.at[s, k], ctx_s.at[i, k])
        add_logits(s)

    lane = lax.broadcasted_iota(jnp.int32, (T, 128), 1)
    table = jnp.zeros((T, 128), F32)
    for k in range(K):
        part = jnp.sum(logit[k * T:(k + 1) * T, :] * onehot, axis=1, keepdims=True)
        table = jnp.where(lane == k, part, table)
    tgt[0] = table.T[0:8, :]
    for d in range(1, N):
        send(tgt.at[0], tgt.at[d], tgt_s.at[d], tgt_r.at[d], {"voc": lax.rem(me_v + d, N)})
    for k in range(K):
        rows = slice(k * T, (k + 1) * T)
        logit[rows, :] = jnp.exp(logit[rows, :] - column(logz[k:k + 1, :], V)) - onehot
    for d in range(1, N):
        arrived(tgt.at[d], tgt_r.at[d], tgt_s.at[d])
    target = tgt[0]
    for d in range(1, N):
        target = target + tgt[d]
    likely = jnp.exp(target[0:K, :] - logz[...])
    joint = weights * likely
    posterior = joint / jnp.sum(joint, axis=0, keepdims=True)
    factor = loss[...] * posterior
    mgrad[...] = loss[...] * (weights - posterior)
    for k in range(K):
        rows = slice(k * T, (k + 1) * T)
        lg[rows, :] = (column(factor[k:k + 1, :], V) * logit[rows, :]).astype(BF16)

    def cg_part(s, k):
        return lax.dot_general(
            lg[k * T:(k + 1) * T, :], vw[pl.ds(pl.multiple_of(s * E, E), E), :], NT,
            preferred_element_type=F32)

    for i in list(range(1, half)) + [0]:
        s = lax.rem(chip + i, half) * 2
        for k in range(K):
            cgs[i, k] = cg_part(s + 1 - core, k).astype(BF16)
            send(cgs.at[i, k], cgr.at[i, k], cgp_s.at[i, k], cgp_r.at[i, k], {"voc": partner})
        for k in range(K):
            part = cg_part(s + core, k)
            if i == 0:
                own_cg[k] = part
            else:
                arrived(cgr.at[i, k], cgp_r.at[i, k], cgp_s.at[i, k])
                cgx[i, k] = (part + cgr[i, k].astype(F32)).astype(BF16)
                send(cgx.at[i, k], xr.at[i, k], cgx_s.at[i, k], cgx_r.at[i, k], {"voc": s + core})

    for s in range(N):
        vgb[s * E:(s + 1) * E, :] = lax.dot_general(
            ctx[s], lg[...], TN, preferred_element_type=F32).astype(BF16)
    for zz in range(Z):
        send(vgb.at[pl.ds((zz * 2 + 1 - y) * R, R)], vgy.at[zz], vy_s.at[zz], vy_r.at[zz],
             {"tok": ypart})

    for d in range(1, Z):
        src = lax.rem(z - d + Z, Z)
        arrived(hrow.at[:, pl.ds(src * T, T)], hid_r.at[d], hid_s.at[d])
    for b in range(2):
        htr[b] = hrow[b].T

    pieces = [(k, 0, E) for k in range(K)]
    if E % 256 == 0:
        pieces[-1:] = [(K - 1, 0, E // 2), (K - 1, E // 2, E // 2)]

    def relay(t, p, way, pred):
        k, lo, wide = pieces[p]
        piece = pg.at[k, rows_of(t, T), pl.ds(lo, wide)]
        c = remote(piece, piece, ag_s.at[way, t, p], ag_r.at[t, p],
                   {"tok": me_t + 2 - 4 * way})
        pl.when(pred)(c.start)
        sends.append((pred, c))

    has_r = z + 1 < Z
    has_l = z >= 1
    for k in range(K):
        total = own_cg[k]
        arrived(cgr.at[0, k], cgp_r.at[0, k], cgp_s.at[0, k])
        total = total + cgr[0, k].astype(F32)
        for i in range(1, half):
            arrived(xr.at[i, k], cgx_r.at[i, k], cgx_s.at[i, k])
            total = total + xr[i, k].astype(F32)
        c = ctx[me_v, k * T:(k + 1) * T, :].astype(F32)
        pg[k, rows_of(z, T), :] = (total * (1.0 - c * c)).astype(BF16)
        if Z > 1:
            for p in range(len(pieces)):
                if pieces[p][0] == k:
                    relay(z, p, 0, has_r)
                    relay(z, p, 1, has_l)

    def hid_part(s):
        total = jnp.zeros((T, E), F32)
        for k in range(K):
            total = total + lax.dot_general(
                pg[k, rows_of(z, T), :], w[k, pl.ds(pl.multiple_of(s * E, E), E), :], NT,
                preferred_element_type=F32)
        return total

    def hid_send(d):
        s = lax.rem(me_v + d, N)
        if d == 0:
            own_hs[...] = hid_part(s)
        else:
            hss[d] = hid_part(s).astype(BF16)
            send(hss.at[d], hsr.at[d], hs_s.at[d], hs_r.at[d], {"voc": s})

    hid_order = list(range(1, N)) + [0]
    hid_per = -(-N // (len(pieces) - 1))

    def pair_sums():
        for zz in range(Z):
            arrived(vgy.at[zz], vy_r.at[zz], vy_s.at[zz])
            vsum[zz] = vgb[rows_of(zz * 2 + y, R), :].astype(F32) + vgy[zz].astype(F32)

    def hop(h):
        for way, at, ends in ((0, h, range(h + 1, Z)), (1, Z - 1 - h, range(Z - 1 - h))):
            copies = [
                remote(vout.at[way, e], vin.at[way, e], vz_s.at[way, e], vz_r.at[way, e],
                       {"tok": me_t + 2 - 4 * way})
                for e in ends
            ]

            @pl.when(z == at)
            def _(way=way, ends=ends, copies=copies):
                for e, c in zip(ends, copies):
                    part = vsum[e]
                    if h > 0:
                        arrived(vin.at[way, e], vz_r.at[way, e], vz_s.at[way, e])
                        part = part + vin[way, e].astype(F32)
                    vout[way, e] = part.astype(BF16)
                    c.start()
            for c in copies:
                sends.append((z == at, c))

    if Z == 1:
        for e in hid_order:
            hid_send(e)
    per = -(-(Z - 1) // (len(pieces) - 1))
    for p, (k, lo, wide) in enumerate(pieces):
        lanes = slice(lo, lo + wide)
        for d in range(1, Z):
            for there, t, way, more in (
                (z >= d, z - d, 0, has_r), (z + d < Z, z + d, 1, has_l),
            ):
                def _(t=t):
                    arrived(pg.at[k, rows_of(t, T), pl.ds(lo, wide)], ag_r.at[t, p], ag_s.at[0, t, p])
                pl.when(there)(_)
                if d < Z - 1:
                    relay(t, p, way, there & more)
            if d == 1:
                for e in hid_order[p * hid_per:(p + 1) * hid_per]:
                    hid_send(e)
        psend[k, :, lanes] = jnp.dot(
            htr[1 - y], pg[k, :, lanes], preferred_element_type=F32).astype(BF16)
        send(psend.at[k, :, pl.ds(lo, wide)], precv.at[k, :, pl.ds(lo, wide)],
             pp_s.at[p], pp_r.at[p], {"tok": ypart})
        acc[k, :, lanes] = jnp.dot(htr[y], pg[k, :, lanes], preferred_element_type=F32)
        if p == 0:
            pair_sums()
        for h in range(p * per, min((p + 1) * per, Z - 1)):
            hop(h)

    acc_v = vsum.at[z]
    for way, pred in ((0, has_l), (1, has_r)):
        @pl.when(pred)
        def _(way=way):
            arrived(vin.at[way, z], vz_r.at[way, z], vz_s.at[way, z])
            acc_v[...] += vin[way, z].astype(F32)
    out_vocab[...] = acc_v[...].astype(BF16)
    htot = own_hs[...]
    for d in range(1, N):
        arrived(hsr.at[d], hs_r.at[d], hs_s.at[d])
        htot = htot + hsr[d].astype(F32)
    mixf = mix[...].astype(F32)
    for k in range(K):
        htot = htot + column(mgrad[k:k + 1, :], E) * mixf[k:k + 1, :]
    out_hidden[...] = htot.astype(BF16)

    for p, (k, lo, wide) in enumerate(pieces):
        lanes = slice(lo, lo + wide)
        arrived(precv.at[k, :, pl.ds(lo, wide)], pp_r.at[p], pp_s.at[p])
        out_proj[k, :, lanes] = (acc[k, :, lanes] + precv[k, :, lanes].astype(F32)).astype(BF16)
    for pred, c in sends:
        if pred is None:
            c.wait_send()
        else:
            pl.when(pred)(c.wait_send)


def rows_of(block, size):
    return pl.ds(pl.multiple_of(block * size, size), size)


def body_base(M, N, hidden, mix_weight, comp_proj, vocab_weight, log_normalizer, targets, loss_grad):
    T, D = hidden.shape
    K, E = mix_weight.shape
    V = vocab_weight.shape[1]
    R = D // M
    half = N // 2
    Z = M // 2
    w = jnp.transpose(comp_proj, (1, 0, 2))
    vm = pltpu.VMEM
    dma = pltpu.SemaphoreType.DMA
    scratch = [
        vm((K, D, E), BF16), vm((N, K * T, E), BF16), vm((N, K, E), BF16),
        vm((Z, 2, T, R), BF16), vm((2, Z * T, R), BF16), vm((2, R, Z * T), BF16), vm((K * T, V), F32), vm((K * T, V), BF16),
        vm((N, 8, T), F32),
        vm((half, K, T, E), BF16), vm((half, K, T, E), BF16),
        vm((half, K, T, E), BF16), vm((half, K, T, E), BF16),
        vm((K, T, E), F32), vm((D, V), BF16), vm((Z, R, V), BF16),
        vm((Z, R, V), F32), vm((2, Z, R, V), BF16), vm((2, Z, R, V), BF16),
        vm((K, Z * T, E), BF16), vm((N, T, E), BF16), vm((N, T, E), BF16),
        vm((T, E), F32), vm((K, R, E), F32), vm((K, R, E), BF16), vm((K, R, E), BF16),
        vm((K, T), F32),
        dma((K,)), dma((half, K)), dma((half, K)), dma((N, K)), dma((N,)), dma((N,)),
        dma((Z,)), dma((Z,)), dma((N,)), dma((N,)),
        dma((half, K)), dma((half, K)), dma((half, K)), dma((half, K)),
        dma((Z,)), dma((Z,)), dma((2, Z)), dma((2, Z)), dma((N,)), dma((N,)),
        dma((2, Z, K + 1)), dma((Z, K + 1)), dma((K + 1,)), dma((K + 1,)),
    ]
    spec = pl.BlockSpec(memory_space=pltpu.VMEM)
    hidden_grad, proj_grad, vocab_grad = pl.pallas_call(
        functools.partial(kernel, M, N),
        out_shape=(
            jax.ShapeDtypeStruct((T, E), BF16),
            jax.ShapeDtypeStruct((K, R, E), BF16),
            jax.ShapeDtypeStruct((R, V), BF16),
        ),
        in_specs=[spec, spec, pl.BlockSpec(memory_space=pltpu.MemorySpace.HBM)] + [spec] * 4,
        out_specs=(spec, spec, spec),
        scratch_shapes=scratch,
        compiler_params=pltpu.CompilerParams(
            collective_id=0, has_side_effects=True, vmem_limit_bytes=48 * 1024 * 1024
        ),
    )(hidden, mix_weight, w, vocab_weight, log_normalizer, targets[None, :], loss_grad[None, :])
    return hidden_grad, jnp.transpose(proj_grad, (1, 0, 2)), vocab_grad


def scoped(fn):
    def run(*args, **kw):
        tag = "_".join(str(a) for a in args if isinstance(a, int))
        with jax.named_scope(fn.__name__ + "_" + tag):
            return fn(*args, **kw)
    return run


def mix_rows(K, flip=False):
    B = 256 // K
    r = lax.broadcasted_iota(jnp.int32, (256, 256), 1 if flip else 0)
    c = lax.broadcasted_iota(jnp.int32, (256, 256), 0 if flip else 1)
    return (c == K * (r % B) + r // B).astype(F32).astype(BF16)


def fast_kernel(
    M, N,
    hid_hbm, mix_hbm, proj_hbm, vw_hbm, logz_hbm, tg_hbm, loss_hbm,
    out_hidden, out_proj, out_vocab,
    raw, w, hida, vw, vwe, vwt, mix, logz, targets, loss,
    ctx, ctxz, mix_all, htr, logit, lgall, tgt, pg,
    vgb, vgy, vsum, vout, vin, hss, hsr, own_hs, acc, psend, precv, mgrad,
    l_sem, w_sem, ctx_s, ctx_f, ctx_r, mix_s, mix_r, hz_s, hz_r, hp_s, hp_r,
    vx_s, vx_r, vp_s, vp_r, vwz_s, vwy_s, vw_r, tgt_s, tgt_r,
    lz_s, lx_s, lp_s, lg_r, vy_s, vy_r, vz_s, vz_r, hs_s, hs_r, pp_s, pp_r,
):
    K, D, E = w.shape
    T = hida.shape[2]
    H = D // 2
    V = vw.shape[1]
    R = D // M
    J = E // 128
    S = E // M
    half = N // 2
    Z = M // 2
    B = 256 // K
    me_t = lax.axis_index("tok")
    me_v = lax.axis_index("voc")
    chip = me_v // 2
    core = me_v % 2
    partner = me_v + 1 - 2 * core
    z = me_t // 2
    y = me_t % 2
    ypart = me_t + 1 - 2 * y
    has_r = z + 1 < Z
    has_l = z >= 1
    sends = []

    def remote(src, dst, ss, rs, dev):
        return pltpu.make_async_remote_copy(
            src_ref=src, dst_ref=dst, send_sem=ss, recv_sem=rs,
            device_id=dev, device_id_type=MESH,
        )

    def send(src, dst, ss, rs, dev, pred=None):
        c = remote(src, dst, ss, rs, dev)
        if pred is None:
            c.start()
        else:
            pl.when(pred)(c.start)
        sends.append((pred, c))

    def arrived(ref, rs, ss):
        remote(ref, ref, ss, rs, {"voc": partner}).wait_recv()

    def mate(j):
        if j == 0:
            return z
        near = jnp.minimum(z, Z - 1 - z)
        d = (j + 1) // 2
        both = z + d if j % 2 == 1 else z - d
        return jnp.where(j <= 2 * near, both, jnp.where(2 * z < Z, j, Z - 1 - j))

    def onward(zz):
        right = zz < z
        there = (right & has_r) | (jnp.logical_not(right) & has_l)
        return there, me_t + jnp.where(right, 2, -2)

    chunks = 4
    n = D // chunks

    def w_copy(c, j):
        return pltpu.make_async_copy(
            proj_hbm.at[pl.ds(c * n, n), :, pl.ds(j * 128, 128)],
            raw.at[j, pl.ds(c * n, n)], w_sem.at[c, j])

    loads = [
        pltpu.make_async_copy(hid_hbm.at[:, pl.ds(0, H)], hida.at[z, 0], l_sem.at[0]),
        pltpu.make_async_copy(hid_hbm.at[:, pl.ds(H, H)], hida.at[z, 1], l_sem.at[1]),
        pltpu.make_async_copy(vw_hbm, vw, l_sem.at[2]),
        pltpu.make_async_copy(mix_hbm, mix, l_sem.at[3]),
        pltpu.make_async_copy(logz_hbm, logz, l_sem.at[4]),
        pltpu.make_async_copy(tg_hbm, targets, l_sem.at[5]),
        pltpu.make_async_copy(loss_hbm, loss, l_sem.at[6]),
    ]
    for c in loads:
        c.start()

    bar = pltpu.get_barrier_semaphore()
    for d in range(1, M):
        pl.semaphore_signal(bar, inc=1, device_id={"tok": lax.rem(me_t + d, M)}, device_id_type=MESH)
    for d in range(1, N):
        pl.semaphore_signal(bar, inc=1, device_id={"voc": lax.rem(me_v + d, N)}, device_id_type=MESH)

    perm = mix_rows(K)

    @scoped
    def unmix(c):
        for j in range(J):
            w_copy(c, j).wait()
        for b in range(c * n // B, (c + 1) * n // B):
            x = jnp.concatenate(
                [raw.at[j].reshape(D * K, 128)[b * 256:(b + 1) * 256, :] for j in range(J)], axis=1)
            rows = jnp.dot(perm, x, preferred_element_type=F32).astype(BF16)
            for k in range(K):
                w[k, b * B:(b + 1) * B, :] = rows[k * B:(k + 1) * B]

    with jax.named_scope("loads"):
        for c in loads[:3]:
            c.wait()
    for c in range(chunks):
        for j in range(J):
            w_copy(c, j).start()
    with jax.named_scope("barrier"):
        pl.semaphore_wait(bar, M + N - 2)

    def vw_piece(ci, t):
        return vwe.at[pl.ds(ci * 2, 2), rows_of(t, S)]

    @scoped
    def vw_own():
        for i in range(1, half):
            ci = lax.rem(chip + i, half)
            for c in range(2):
                arrived(vwe.at[ci * 2 + c, rows_of(me_t, S)], vx_r.at[ci * 2 + c], vx_s.at[i, c])
            piece = vw_piece(ci, me_t)
            send(piece, piece, vwy_s.at[i, z], vw_r.at[ci, me_t], {"tok": ypart})
            for d in range(1, Z):
                send(piece, piece, vwz_s.at[i, d], vw_r.at[ci, me_t], {"tok": lax.rem(me_t + 2 * d, M)})

    def slab(v, t):
        return pl.ds(pl.multiple_of(v * E + t * S, S), S)

    for i in range(1, half):
        for c in range(2):
            v = lax.rem(chip + i, half) * 2 + c
            send(vw.at[slab(v, me_t)], vwe.at[me_v, rows_of(me_t, S)],
                 vx_s.at[i, c], vx_r.at[me_v], {"voc": v})
    send(hida.at[z, core], hida.at[z, core], hz_s.at[0, z], hz_r.at[z], {"tok": me_t + 2}, has_r)
    send(hida.at[z, core], hida.at[z, core], hz_s.at[1, z], hz_r.at[z], {"tok": me_t - 2}, has_l)
    for c in loads[3:]:
        c.wait()
    for d in range(1, N):
        send(mix, mix_all.at[d], mix_s.at[d], mix_r.at[d], {"voc": lax.rem(me_v + d, N)})
    send(vw.at[rows_of(partner, E)], vwe.at[me_v], vp_s.at[0], vp_r.at[0], {"voc": partner})
    for c in range(chunks):
        unmix(c)
    vw_own()

    def context(zz, k):
        both = jnp.dot(hida[zz, 0], w[k, 0:H, :], preferred_element_type=F32)
        both = both + jnp.dot(hida[zz, 1], w[k, H:D, :], preferred_element_type=F32)
        return jnp.tanh(both).astype(BF16)

    for k in range(K):
        with jax.named_scope("context"):
            ctx[me_v, k * T:(k + 1) * T, :] = context(z, k)
        piece = ctx.at[me_v, pl.ds(k * T, T)]
        for i in range(1, half):
            send(piece, piece, ctx_s.at[i, k], ctx_r.at[me_v, k],
                 {"voc": lax.rem(chip + i, half) * 2 + core})
        send(piece, piece, ctx_s.at[0, k], ctx_r.at[me_v, k], {"voc": partner})

    @scoped
    def add_logits(s, first=False):
        part = jnp.dot(ctx[s], vw[rows_of(s, E), :], preferred_element_type=F32)
        logit[...] = part if first else logit[...] + part

    @scoped
    def relay_vw(j):
        zz = mate(j)
        t = zz * 2 + y
        for i in range(1, half):
            ci = lax.rem(chip + i, half)
            piece = vw_piece(ci, t)
            arrived(piece, vw_r.at[ci, t], vwy_s.at[i, zz])
            send(piece, piece, vwy_s.at[i, zz], vw_r.at[ci, t], {"tok": ypart})

    @scoped
    def relay_hid(j, fwd):
        zz = mate(j)
        there, to = onward(zz)
        piece = hida.at[zz, core]
        on = remote(piece, piece, hz_s.at[0, zz], hz_r.at[zz], {"tok": to})
        over = remote(piece, piece, hp_s.at[zz], hp_r.at[zz], {"voc": partner})

        @pl.when(there if fwd else jnp.logical_not(there))
        def _():
            arrived(piece, hz_r.at[zz], hz_s.at[0, zz])
            if fwd:
                on.start()
            over.start()
        if fwd:
            sends.append((there, on))
            sends.append((None, over))

    @scoped
    def ctx_mate(j, ks):
        zz = mate(j)
        if ks[0] == 0:
            arrived(hida.at[zz, 1 - core], hp_r.at[zz], hp_s.at[zz])
        for k in ks:
            ctxz[zz, k * T:(k + 1) * T, :] = context(zz, k)

    @scoped
    def ctx_pass(k):
        for i in range(1, half):
            s = lax.rem(chip - i + half, half) * 2 + core
            piece = ctx.at[s, pl.ds(k * T, T)]
            arrived(piece, ctx_r.at[s, k], ctx_s.at[i, k])
            send(piece, piece, ctx_f.at[i, k], ctx_r.at[s, k], {"voc": partner})

    add_logits(me_v, True)
    for k in range(K):
        arrived(ctx.at[partner, pl.ds(k * T, T)], ctx_r.at[partner, k], ctx_s.at[0, k])
    add_logits(partner)

    tcol = column(targets[...].astype(F32), V)
    ids = (me_v * V + lax.broadcasted_iota(jnp.int32, (T, V), 1)).astype(F32)
    onehot = (tcol == ids).astype(F32)
    mix_all[0] = mix[...]
    for d in range(1, N):
        arrived(mix_all.at[d], mix_r.at[d], mix_s.at[d])
    mixing = jnp.zeros((K, T), F32)
    for d in range(N):
        s = lax.rem(me_v - d + N, N)
        mixing = mixing + lax.dot_general(
            mix_all[d],
            hida[z, s // half, :, pl.ds(pl.multiple_of((s % half) * E, E), E)], NT,
            preferred_element_type=F32)
    exp_mix = jnp.exp(mixing)
    weights = exp_mix / jnp.sum(exp_mix, axis=0, keepdims=True)

    ctx_pass(0)
    for j in range(1, min(Z, 3)):
        relay_hid(j, True)
    if Z > 1:
        relay_hid(1, False)
    ctx_pass(1)
    for j in range(1, Z):
        relay_vw(j)
    if Z > 1:
        ctx_mate(1, range(K))
    for k in range(2, K):
        ctx_pass(k)
    for i in range(1, half):
        add_logits(lax.rem(chip - i + half, half) * 2 + core)
    for i in range(1, half):
        s = lax.rem(chip - i + half, half) * 2 + 1 - core
        for k in range(K):
            arrived(ctx.at[s, pl.ds(k * T, T)], ctx_r.at[s, k], ctx_s.at[i, k])
        add_logits(s)

    lane = lax.broadcasted_iota(jnp.int32, (T, 128), 1)
    table = jnp.zeros((T, 128), F32)
    for k in range(K):
        part = jnp.sum(logit[k * T:(k + 1) * T, :] * onehot, axis=1, keepdims=True)
        table = jnp.where(lane == k, part, table)
    tgt[0] = table.T[0:8, :]
    for d in range(1, N):
        send(tgt.at[0], tgt.at[d], tgt_s.at[d], tgt_r.at[d], {"voc": lax.rem(me_v + d, N)})
    for j in range(3, Z):
        relay_hid(j, True)
    if Z > 2:
        relay_hid(2, False)
    for k in range(K):
        rows = slice(k * T, (k + 1) * T)
        logit[rows, :] = jnp.exp(logit[rows, :] - column(logz[k:k + 1, :], V)) - onehot
    with jax.named_scope("targets"):
        for d in range(1, N):
            arrived(tgt.at[d], tgt_r.at[d], tgt_s.at[d])
    target = tgt[0]
    for d in range(1, N):
        target = target + tgt[d]
    likely = jnp.exp(target[0:K, :] - logz[...])
    joint = weights * likely
    posterior = joint / jnp.sum(joint, axis=0, keepdims=True)
    factor = loss[...] * posterior
    mgrad[...] = loss[...] * (weights - posterior)

    def shares(zz, k):
        piece = lgall.at[zz, me_v, k]
        return [
            remote(piece, piece, lx_s.at[i, zz, k], lg_r.at[zz, me_v, k],
                   {"voc": lax.rem(chip + i, half) * 2 + core})
            for i in range(1, half)
        ] + [remote(piece, piece, lp_s.at[0, zz, k], lg_r.at[zz, me_v, k], {"voc": partner})]

    def share(zz, k):
        for c in shares(zz, k):
            c.start()
            sends.append((None, c))

    def fill(ks):
        for k in ks:
            rows = slice(k * T, (k + 1) * T)
            lgall[z, me_v, k] = (column(factor[k:k + 1, :], V) * logit[rows, :]).astype(BF16)

    @scoped
    def own_out(k):
        if k < 2:
            fill(range(K)[k:] if k else range(1))
        piece = lgall.at[z, me_v, k]
        send(piece, piece, lz_s.at[0, z, k], lg_r.at[z, me_v, k], {"tok": me_t + 2}, has_r)
        send(piece, piece, lz_s.at[1, z, k], lg_r.at[z, me_v, k], {"tok": me_t - 2}, has_l)
        share(z, k)

    @scoped
    def relay_lg(k, j, fwd):
        zz = mate(j)
        there, to = onward(zz)
        piece = lgall.at[zz, me_v, k]
        on = remote(piece, piece, lz_s.at[0, zz, k], lg_r.at[zz, me_v, k], {"tok": to})

        @pl.when(there if fwd else jnp.logical_not(there))
        def _():
            arrived(piece, lg_r.at[zz, me_v, k], lp_s.at[0, zz, k])
            if fwd:
                on.start()
            for c in shares(zz, k):
                c.start()
        if fwd:
            sends.append((there, on))
            for c in shares(zz, k):
                sends.append((None, c))

    @scoped
    def cross_lg(k, j):
        zz = mate(j)
        for i in range(1, half):
            s = lax.rem(chip - i + half, half) * 2 + core
            piece = lgall.at[zz, s, k]
            arrived(piece, lg_r.at[zz, s, k], lp_s.at[0, zz, k])
            send(piece, piece, lp_s.at[i, zz, k], lg_r.at[zz, s, k], {"voc": partner})

    @scoped
    def pre_grad(k, j):
        zz = mate(j)
        rows = slice(k * T, (k + 1) * T)
        for i in range(half):
            s = lax.rem(chip + i, half) * 2 + 1 - core
            arrived(lgall.at[zz, s, k], lg_r.at[zz, s, k], lp_s.at[0, zz, k])
        total = None
        for s in range(N):
            part = jnp.dot(lgall[zz, s, k], vwt[s], preferred_element_type=F32)
            total = part if total is None else total + part
        c = (ctx[me_v, rows, :] if j == 0 else ctxz[zz, rows, :]).astype(F32)
        pg[k, rows_of(zz, T), :] = (total * (1.0 - c * c)).astype(BF16)

    def hid_part(s):
        total = jnp.zeros((T, E), F32)
        for k in range(K):
            total = total + lax.dot_general(
                pg[k, rows_of(z, T), :], w[k, rows_of(s, E), :], NT,
                preferred_element_type=F32)
        return total

    @scoped
    def hid_send(d):
        s = lax.rem(me_v + d, N)
        if d == 0:
            own_hs[...] = hid_part(s)
        else:
            hss[d] = hid_part(s).astype(BF16)
            send(hss.at[d], hsr.at[d], hs_s.at[d], hs_r.at[d], {"voc": s})

    @scoped
    def pair_sums():
        for zz in range(Z):
            arrived(vgy.at[zz], vy_r.at[zz], vy_s.at[zz])
            vsum[zz] = vgb[rows_of(zz * 2 + y, R), :].astype(F32) + vgy[zz].astype(F32)

    @scoped
    def hop(h):
        for way, at, ends in ((0, h, range(h + 1, Z)), (1, Z - 1 - h, range(Z - 1 - h))):
            copies = [
                remote(vout.at[way, e], vin.at[way, e], vz_s.at[way, e], vz_r.at[way, e],
                       {"tok": me_t + 2 - 4 * way})
                for e in ends
            ]

            @pl.when(z == at)
            def _(way=way, ends=ends, copies=copies):
                for e, c in zip(ends, copies):
                    part = vsum[e]
                    if h > 0:
                        arrived(vin.at[way, e], vz_r.at[way, e], vz_s.at[way, e])
                        part = part + vin[way, e].astype(F32)
                    vout[way, e] = part.astype(BF16)
                    c.start()
            for c in copies:
                sends.append((z == at, c))

    pieces = [(k, 0, E) for k in range(K)]
    if E % 256 == 0:
        pieces[-1:] = [(K - 1, 0, E // 2), (K - 1, E // 2, E // 2)]

    @scoped
    def proj_part(k):
        for p, (kk, lo, wide) in enumerate(pieces):
            if kk == k:
                lanes = slice(lo, lo + wide)
                psend[k, :, lanes] = jnp.dot(
                    htr[1 - y], pg[k, :, lanes], preferred_element_type=F32).astype(BF16)
                send(psend.at[k, :, pl.ds(lo, wide)], precv.at[k, :, pl.ds(lo, wide)],
                     pp_s.at[p], pp_r.at[p], {"tok": ypart})
        acc[k] = jnp.dot(htr[y], pg[k], preferred_element_type=F32)

    @scoped
    def vocab_part():
        for s in range(N):
            total = None
            for k in range(K):
                part = lax.dot_general(ctx[s, k * T:(k + 1) * T, :], lgall[z, me_v, k], TN,
                                       preferred_element_type=F32)
                total = part if total is None else total + part
            vgb[s * E:(s + 1) * E, :] = total.astype(BF16)
        for zz in range(Z):
            send(vgb.at[pl.ds((zz * 2 + 1 - y) * R, R)], vgy.at[zz], vy_s.at[zz], vy_r.at[zz],
                 {"tok": ypart})

    @scoped
    def vw_done():
        vwe[me_v] = vw[rows_of(me_v, E), :]
        arrived(vwe.at[partner], vp_r.at[0], vp_s.at[0])
        for i in range(1, half):
            ci = lax.rem(chip + i, half)
            for zz in range(Z):
                t = zz * 2 + 1 - y
                arrived(vw_piece(ci, t), vw_r.at[ci, t], vwy_s.at[i, zz])
        for s in range(N):
            vwt[s] = vwe[s].T

    @scoped
    def turn():
        for b in range(2):
            col = (z * 2 + b) * R
            for zz in range(Z):
                htr[b, :, zz * T:(zz + 1) * T] = hida[
                    zz, col // H, :, pl.ds(pl.multiple_of(col % H, R), R)].T

    lag = 2
    hid_order = list(range(1, N)) + [0]
    for step in range(K + Z + lag):
        if step < K:
            own_out(step)
        if step == 1:
            vocab_part()
        for j in range(1, Z):
            if 0 <= step - (j + 1) // 2 < K:
                relay_lg(step - (j + 1) // 2, j, True)
        for j in range(1, Z):
            if 0 <= step - j < K:
                relay_lg(step - j, j, False)
        if step == 3:
            for j in range(3, Z):
                relay_hid(j, False)
        for j in range(Z):
            if 0 <= step - j - 1 < K:
                cross_lg(step - j - 1, j)
        for j in range(Z):
            k = step - lag - j
            if not 0 <= k < K:
                continue
            if k == 0 and j > 1:
                ctx_mate(j, range(K))
            if k == 0 and j == 0:
                vw_done()
            pre_grad(k, j)
            if k == 0 and j == Z - 1:
                turn()
            if j == Z - 1:
                proj_part(k)
                for d in hid_order[k * N // K:(k + 1) * N // K]:
                    hid_send(d)
        if step == K:
            pair_sums()
        if K <= step < K + Z - 1:
            hop(step - K)

    acc_v = vsum.at[z]
    for way, pred in ((0, has_l), (1, has_r)):
        @pl.when(pred)
        def _(way=way):
            arrived(vin.at[way, z], vz_r.at[way, z], vz_s.at[way, z])
            acc_v[...] += vin[way, z].astype(F32)
    out_vocab[...] = acc_v[...].astype(BF16)
    htot = own_hs[...]
    for d in range(1, N):
        arrived(hsr.at[d], hs_r.at[d], hs_s.at[d])
        htot = htot + hsr[d].astype(F32)
    mixf = mix[...].astype(F32)
    for k in range(K):
        htot = htot + column(mgrad[k:k + 1, :], E) * mixf[k:k + 1, :]
    out_hidden[...] = htot.astype(BF16)

    back = mix_rows(K, True)
    for p, (k, lo, wide) in enumerate(pieces):
        lanes = slice(lo, lo + wide)
        with jax.named_scope("precv"):
            arrived(precv.at[k, :, pl.ds(lo, wide)], pp_r.at[p], pp_s.at[p])
        psum = (acc[k, :, lanes] + precv[k, :, lanes].astype(F32)).astype(BF16)
        if k < K - 1:
            precv[k, :, lanes] = psum
            continue
        for b in range(R // B):
            rows = slice(b * B, (b + 1) * B)
            x = jnp.concatenate([precv[q, rows, lanes] for q in range(K - 1)] + [psum[rows]], axis=0)
            out = jnp.dot(back, x, preferred_element_type=F32).astype(BF16)
            for j in range(wide // 128):
                out_proj.at[lo // 128 + j].reshape(R * K, 128)[b * 256:(b + 1) * 256, :] = (
                    out[:, j * 128:(j + 1) * 128])
    with jax.named_scope("drain"):
        for pred, c in sends:
            if pred is None:
                c.wait_send()
            else:
                pl.when(pred)(c.wait_send)


def body_fast(M, N, hidden, mix_weight, comp_proj, vocab_weight, log_normalizer, targets, loss_grad):
    T, D = hidden.shape
    K, E = mix_weight.shape
    V = vocab_weight.shape[1]
    R = D // M
    J = E // 128
    half = N // 2
    Z = M // 2
    vm = pltpu.VMEM
    dma = pltpu.SemaphoreType.DMA
    scratch = [
        vm((J, D, K, 128), BF16), vm((K, D, E), BF16), vm((Z, 2, T, D // 2), BF16), vm((D, V), BF16),
        vm((N, E, V), BF16), vm((N, V, E), BF16), vm((K, E), BF16), vm((K, T), F32), vm((1, T), jnp.int32), vm((1, T), F32),
        vm((N, K * T, E), BF16), vm((Z, K * T, E), BF16), vm((N, K, E), BF16), vm((2, R, Z * T), BF16),
        vm((K * T, V), F32), vm((Z, N, K, T, V), BF16), vm((N, 8, T), F32), vm((K, Z * T, E), BF16),
        vm((D, V), BF16), vm((Z, R, V), BF16),
        vm((Z, R, V), F32), vm((2, Z, R, V), BF16), vm((2, Z, R, V), BF16),
        vm((N, T, E), BF16), vm((N, T, E), BF16),
        vm((T, E), F32), vm((K, R, E), F32), vm((K, R, E), BF16), vm((K, R, E), BF16),
        vm((K, T), F32),
        dma((7,)), dma((4, J)),
        dma((half, K)), dma((half, K)), dma((N, K)), dma((N,)), dma((N,)),
        dma((2, Z)), dma((Z,)), dma((Z,)), dma((Z,)),
        dma((half, 2)), dma((N,)), dma((1,)), dma((1,)),
        dma((half, Z)), dma((half, Z)), dma((half, M)), dma((N,)), dma((N,)),
        dma((2, Z, K)), dma((half, Z, K)), dma((half, Z, K)), dma((Z, N, K)),
        dma((Z,)), dma((Z,)), dma((2, Z)), dma((2, Z)), dma((N,)), dma((N,)),
        dma((K + 1,)), dma((K + 1,)),
    ]
    spec = pl.BlockSpec(memory_space=pltpu.VMEM)
    hbm = pl.BlockSpec(memory_space=pltpu.MemorySpace.HBM)
    hid, proj, voc = pl.pallas_call(
        functools.partial(fast_kernel, M, N),
        out_shape=(
            jax.ShapeDtypeStruct((T, E), BF16),
            jax.ShapeDtypeStruct((J, R, K, 128), BF16),
            jax.ShapeDtypeStruct((R, V), BF16),
        ),
        in_specs=[hbm] * 7,
        out_specs=(spec, spec, spec),
        scratch_shapes=scratch,
        compiler_params=pltpu.CompilerParams(
            collective_id=0, has_side_effects=True, vmem_limit_bytes=47 * 1024 * 1024
        ),
    )(*[
        pltpu.with_memory_space_constraint(x, pltpu.MemorySpace.HBM)
        for x in (hidden, mix_weight, comp_proj, vocab_weight, log_normalizer, targets[None, :], loss_grad[None, :])
    ])
    return pl.pallas_call(
        store_kernel,
        out_shape=(
            jax.ShapeDtypeStruct((T, E), BF16),
            jax.ShapeDtypeStruct((R, K, E), BF16),
            jax.ShapeDtypeStruct((R, V), BF16),
        ),
        in_specs=[spec] * 3,
        out_specs=(hbm, hbm, hbm),
        scratch_shapes=[dma((J + 2,))],
        compiler_params=pltpu.CompilerParams(vmem_limit_bytes=4 * 1024 * 1024),
    )(hid, proj, voc)


def store_kernel(hid, proj, voc, out_hid, out_proj, out_voc, sem):
    J = proj.shape[0]
    copies = [pltpu.make_async_copy(hid, out_hid, sem.at[J]), pltpu.make_async_copy(voc, out_voc, sem.at[J + 1])]
    for j in range(J):
        copies.append(pltpu.make_async_copy(proj.at[j], out_proj.at[:, :, pl.ds(j * 128, 128)], sem.at[j]))
    for c in copies:
        c.start()
    for c in copies:
        c.wait()


def body(M, N, *args):
    hidden, mix_weight, comp_proj, vocab_weight = args[:4]
    T, D = hidden.shape
    K, E = mix_weight.shape
    V = vocab_weight.shape[1]
    gathered = 2 * (M // 2) * T * (K * N * V + D + 2 * K * E)
    shapes = K == 4 and E % 128 == 0 and (E // M) % 16 == 0 and (D // M) % (256 // K) == 0
    if shapes and gathered + 4 * K * D * E <= 28 * 1024 * 1024:
        return body_fast(M, N, *args)
    return body_base(M, N, *args)


def solution(mesh):
    in_specs = (
        P("tok", None),
        P(None, "voc"),
        P(None, None, "voc"),
        P(None, "voc"),
        P(None, "tok"),
        P("tok"),
        P("tok"),
    )
    out_specs = (P("tok", "voc"), P("tok", None, "voc"), P("tok", "voc"))
    return jax.shard_map(
        functools.partial(body, mesh.shape["tok"], mesh.shape["voc"]),
        mesh=mesh, in_specs=in_specs, out_specs=out_specs, check_vma=False,
    )
```

```python
import functools

import jax
import jax.numpy as jnp
from jax import lax
from jax.experimental import pallas as pl
from jax.experimental.pallas import tpu as pltpu
from jax.sharding import PartitionSpec as P

MESH = pl.DeviceIdType.MESH
F32 = jnp.float32
BF16 = jnp.bfloat16
NT = (((1,), (1,)), ((), ()))
TN = (((0,), (0,)), ((), ()))


def column(row, lanes):
    wide = jnp.broadcast_to(row, (128, row.shape[1])).T
    return jnp.concatenate([wide] * (lanes // 128), axis=1)


def kernel(
    M, N,
    hidden, mix, proj_hbm, vw, logz, targets, loss,
    out_hidden, out_proj, out_vocab,
    w, ctx, mix_all, hblk, hrow, htr, logit, lg, tgt,
    cgs, cgr, cgx, xr, own_cg, vgb, vgy, vsum, vout, vin, pg, hss, hsr, own_hs, acc, psend, precv, mgrad,
    w_sem, ctx_s, ctx_f, ctx_r, mix_s, mix_r, hid_s, hid_r, tgt_s, tgt_r,
    cgp_s, cgp_r, cgx_s, cgx_r, vy_s, vy_r, vz_s, vz_r, hs_s, hs_r, ag_s, ag_r, pp_s, pp_r,
):
    K, D, E = w.shape
    T = hidden.shape[0]
    V = vw.shape[1]
    R = D // M
    half = N // 2
    Z = M // 2
    me_t = lax.axis_index("tok")
    me_v = lax.axis_index("voc")
    chip = me_v // 2
    core = me_v % 2
    partner = me_v + 1 - 2 * core
    z = me_t // 2
    y = me_t % 2
    ypart = me_t + 1 - 2 * y
    sends = []

    def remote(src, dst, ss, rs, dev):
        return pltpu.make_async_remote_copy(
            src_ref=src, dst_ref=dst, send_sem=ss, recv_sem=rs,
            device_id=dev, device_id_type=MESH,
        )

    def send(src, dst, ss, rs, dev):
        c = remote(src, dst, ss, rs, dev)
        c.start()
        sends.append((None, c))

    def arrived(ref, rs, ss):
        remote(ref, ref, ss, rs, {"voc": partner}).wait_recv()

    for k in range(K):
        pltpu.make_async_copy(proj_hbm.at[k], w.at[k], w_sem.at[k]).start()
    for j in range(M):
        hblk[j // 2, j % 2] = hidden[:, j * R:(j + 1) * R]

    bar = pltpu.get_barrier_semaphore()
    for d in range(1, M):
        pl.semaphore_signal(bar, inc=1, device_id={"tok": lax.rem(me_t + d, M)}, device_id_type=MESH)
    for d in range(1, N):
        pl.semaphore_signal(bar, inc=1, device_id={"voc": lax.rem(me_v + d, N)}, device_id_type=MESH)
    pl.semaphore_wait(bar, M + N - 2)

    for d in range(1, N):
        send(mix, mix_all.at[d], mix_s.at[d], mix_r.at[d], {"voc": lax.rem(me_v + d, N)})
    mix_all[0] = mix[...]
    for d in range(1, Z):
        zz = lax.rem(z + d, Z)
        send(hblk.at[zz], hrow.at[:, pl.ds(z * T, T)], hid_s.at[d], hid_r.at[d],
             {"tok": zz * 2 + y})
    hrow[:, rows_of(z, T), :] = hblk[z]

    for k in range(K):
        pltpu.make_async_copy(proj_hbm.at[k], w.at[k], w_sem.at[k]).wait()
        ctx[me_v, k * T:(k + 1) * T, :] = jnp.tanh(
            jnp.dot(hidden[...], w[k], preferred_element_type=F32)
        ).astype(BF16)
        piece = ctx.at[me_v, pl.ds(k * T, T)]
        for i in range(1, half):
            send(piece, piece, ctx_s.at[i, k], ctx_r.at[me_v, k],
                 {"voc": lax.rem(chip + i, half) * 2 + core})
        send(piece, piece, ctx_s.at[0, k], ctx_r.at[me_v, k], {"voc": partner})

    def add_logits(s, first=False):
        part = jnp.dot(ctx[s], vw[pl.ds(pl.multiple_of(s * E, E), E), :],
                       preferred_element_type=F32)
        logit[...] = part if first else logit[...] + part

    add_logits(me_v, True)
    for k in range(K):
        arrived(ctx.at[partner, pl.ds(k * T, T)], ctx_r.at[partner, k], ctx_s.at[0, k])
    add_logits(partner)

    tcol = column(targets[...].astype(F32), V)
    ids = (me_v * V + lax.broadcasted_iota(jnp.int32, (T, V), 1)).astype(F32)
    onehot = (tcol == ids).astype(F32)
    for d in range(1, N):
        arrived(mix_all.at[d], mix_r.at[d], mix_s.at[d])
    mixing = jnp.zeros((K, T), F32)
    for d in range(N):
        s = lax.rem(me_v - d + N, N)
        mixing = mixing + lax.dot_general(
            mix_all[d], hidden[:, pl.ds(pl.multiple_of(s * E, E), E)], NT,
            preferred_element_type=F32)
    exp_mix = jnp.exp(mixing)
    weights = exp_mix / jnp.sum(exp_mix, axis=0, keepdims=True)

    for i in range(1, half):
        s = lax.rem(chip - i + half, half) * 2 + core
        for k in range(K):
            piece = ctx.at[s, pl.ds(k * T, T)]
            arrived(piece, ctx_r.at[s, k], ctx_s.at[i, k])
            send(piece, piece, ctx_f.at[i, k], ctx_r.at[s, k], {"voc": partner})
        add_logits(s)
    for i in range(1, half):
        s = lax.rem(chip - i + half, half) * 2 + 1 - core
        for k in range(K):
            arrived(ctx.at[s, pl.ds(k * T, T)], ctx_r.at[s, k], ctx_s.at[i, k])
        add_logits(s)

    lane = lax.broadcasted_iota(jnp.int32, (T, 128), 1)
    table = jnp.zeros((T, 128), F32)
    for k in range(K):
        part = jnp.sum(logit[k * T:(k + 1) * T, :] * onehot, axis=1, keepdims=True)
        table = jnp.where(lane == k, part, table)
    tgt[0] = table.T[0:8, :]
    for d in range(1, N):
        send(tgt.at[0], tgt.at[d], tgt_s.at[d], tgt_r.at[d], {"voc": lax.rem(me_v + d, N)})
    for k in range(K):
        rows = slice(k * T, (k + 1) * T)
        logit[rows, :] = jnp.exp(logit[rows, :] - column(logz[k:k + 1, :], V)) - onehot
    for d in range(1, N):
        arrived(tgt.at[d], tgt_r.at[d], tgt_s.at[d])
    target = tgt[0]
    for d in range(1, N):
        target = target + tgt[d]
    likely = jnp.exp(target[0:K, :] - logz[...])
    joint = weights * likely
    posterior = joint / jnp.sum(joint, axis=0, keepdims=True)
    factor = loss[...] * posterior
    mgrad[...] = loss[...] * (weights - posterior)
    for k in range(K):
        rows = slice(k * T, (k + 1) * T)
        lg[rows, :] = (column(factor[k:k + 1, :], V) * logit[rows, :]).astype(BF16)

    def cg_part(s, k):
        return lax.dot_general(
            lg[k * T:(k + 1) * T, :], vw[pl.ds(pl.multiple_of(s * E, E), E), :], NT,
            preferred_element_type=F32)

    for i in list(range(1, half)) + [0]:
        s = lax.rem(chip + i, half) * 2
        for k in range(K):
            cgs[i, k] = cg_part(s + 1 - core, k).astype(BF16)
            send(cgs.at[i, k], cgr.at[i, k], cgp_s.at[i, k], cgp_r.at[i, k], {"voc": partner})
        for k in range(K):
            part = cg_part(s + core, k)
            if i == 0:
                own_cg[k] = part
            else:
                arrived(cgr.at[i, k], cgp_r.at[i, k], cgp_s.at[i, k])
                cgx[i, k] = (part + cgr[i, k].astype(F32)).astype(BF16)
                send(cgx.at[i, k], xr.at[i, k], cgx_s.at[i, k], cgx_r.at[i, k], {"voc": s + core})

    for s in range(N):
        vgb[s * E:(s + 1) * E, :] = lax.dot_general(
            ctx[s], lg[...], TN, preferred_element_type=F32).astype(BF16)
    for zz in range(Z):
        send(vgb.at[pl.ds((zz * 2 + 1 - y) * R, R)], vgy.at[zz], vy_s.at[zz], vy_r.at[zz],
             {"tok": ypart})

    for d in range(1, Z):
        src = lax.rem(z - d + Z, Z)
        arrived(hrow.at[:, pl.ds(src * T, T)], hid_r.at[d], hid_s.at[d])
    for b in range(2):
        htr[b] = hrow[b].T

    pieces = [(k, 0, E) for k in range(K)]
    if E % 256 == 0:
        pieces[-1:] = [(K - 1, 0, E // 2), (K - 1, E // 2, E // 2)]

    def relay(t, p, way, pred):
        k, lo, wide = pieces[p]
        piece = pg.at[k, rows_of(t, T), pl.ds(lo, wide)]
        c = remote(piece, piece, ag_s.at[way, t, p], ag_r.at[t, p],
                   {"tok": me_t + 2 - 4 * way})
        pl.when(pred)(c.start)
        sends.append((pred, c))

    has_r = z + 1 < Z
    has_l = z >= 1
    for k in range(K):
        total = own_cg[k]
        arrived(cgr.at[0, k], cgp_r.at[0, k], cgp_s.at[0, k])
        total = total + cgr[0, k].astype(F32)
        for i in range(1, half):
            arrived(xr.at[i, k], cgx_r.at[i, k], cgx_s.at[i, k])
            total = total + xr[i, k].astype(F32)
        c = ctx[me_v, k * T:(k + 1) * T, :].astype(F32)
        pg[k, rows_of(z, T), :] = (total * (1.0 - c * c)).astype(BF16)
        if Z > 1:
            for p in range(len(pieces)):
                if pieces[p][0] == k:
                    relay(z, p, 0, has_r)
                    relay(z, p, 1, has_l)

    def hid_part(s):
        total = jnp.zeros((T, E), F32)
        for k in range(K):
            total = total + lax.dot_general(
                pg[k, rows_of(z, T), :], w[k, pl.ds(pl.multiple_of(s * E, E), E), :], NT,
                preferred_element_type=F32)
        return total

    def hid_send(d):
        s = lax.rem(me_v + d, N)
        if d == 0:
            own_hs[...] = hid_part(s)
        else:
            hss[d] = hid_part(s).astype(BF16)
            send(hss.at[d], hsr.at[d], hs_s.at[d], hs_r.at[d], {"voc": s})

    hid_order = list(range(1, N)) + [0]
    hid_per = -(-N // (len(pieces) - 1))

    def pair_sums():
        for zz in range(Z):
            arrived(vgy.at[zz], vy_r.at[zz], vy_s.at[zz])
            vsum[zz] = vgb[rows_of(zz * 2 + y, R), :].astype(F32) + vgy[zz].astype(F32)

    def hop(h):
        for way, at, ends in ((0, h, range(h + 1, Z)), (1, Z - 1 - h, range(Z - 1 - h))):
            copies = [
                remote(vout.at[way, e], vin.at[way, e], vz_s.at[way, e], vz_r.at[way, e],
                       {"tok": me_t + 2 - 4 * way})
                for e in ends
            ]

            @pl.when(z == at)
            def _(way=way, ends=ends, copies=copies):
                for e, c in zip(ends, copies):
                    part = vsum[e]
                    if h > 0:
                        arrived(vin.at[way, e], vz_r.at[way, e], vz_s.at[way, e])
                        part = part + vin[way, e].astype(F32)
                    vout[way, e] = part.astype(BF16)
                    c.start()
            for c in copies:
                sends.append((z == at, c))

    if Z == 1:
        for e in hid_order:
            hid_send(e)
    per = -(-(Z - 1) // (len(pieces) - 1))
    for p, (k, lo, wide) in enumerate(pieces):
        lanes = slice(lo, lo + wide)
        for d in range(1, Z):
            for there, t, way, more in (
                (z >= d, z - d, 0, has_r), (z + d < Z, z + d, 1, has_l),
            ):
                def _(t=t):
                    arrived(pg.at[k, rows_of(t, T), pl.ds(lo, wide)], ag_r.at[t, p], ag_s.at[0, t, p])
                pl.when(there)(_)
                if d < Z - 1:
                    relay(t, p, way, there & more)
            if d == 1:
                for e in hid_order[p * hid_per:(p + 1) * hid_per]:
                    hid_send(e)
        psend[k, :, lanes] = jnp.dot(
            htr[1 - y], pg[k, :, lanes], preferred_element_type=F32).astype(BF16)
        send(psend.at[k, :, pl.ds(lo, wide)], precv.at[k, :, pl.ds(lo, wide)],
             pp_s.at[p], pp_r.at[p], {"tok": ypart})
        acc[k, :, lanes] = jnp.dot(htr[y], pg[k, :, lanes], preferred_element_type=F32)
        if p == 0:
            pair_sums()
        for h in range(p * per, min((p + 1) * per, Z - 1)):
            hop(h)

    acc_v = vsum.at[z]
    for way, pred in ((0, has_l), (1, has_r)):
        @pl.when(pred)
        def _(way=way):
            arrived(vin.at[way, z], vz_r.at[way, z], vz_s.at[way, z])
            acc_v[...] += vin[way, z].astype(F32)
    out_vocab[...] = acc_v[...].astype(BF16)
    htot = own_hs[...]
    for d in range(1, N):
        arrived(hsr.at[d], hs_r.at[d], hs_s.at[d])
        htot = htot + hsr[d].astype(F32)
    mixf = mix[...].astype(F32)
    for k in range(K):
        htot = htot + column(mgrad[k:k + 1, :], E) * mixf[k:k + 1, :]
    out_hidden[...] = htot.astype(BF16)

    for p, (k, lo, wide) in enumerate(pieces):
        lanes = slice(lo, lo + wide)
        arrived(precv.at[k, :, pl.ds(lo, wide)], pp_r.at[p], pp_s.at[p])
        out_proj[k, :, lanes] = (acc[k, :, lanes] + precv[k, :, lanes].astype(F32)).astype(BF16)
    for pred, c in sends:
        if pred is None:
            c.wait_send()
        else:
            pl.when(pred)(c.wait_send)


def rows_of(block, size):
    return pl.ds(pl.multiple_of(block * size, size), size)


def body_base(M, N, hidden, mix_weight, comp_proj, vocab_weight, log_normalizer, targets, loss_grad):
    T, D = hidden.shape
    K, E = mix_weight.shape
    V = vocab_weight.shape[1]
    R = D // M
    half = N // 2
    Z = M // 2
    w = jnp.transpose(comp_proj, (1, 0, 2))
    vm = pltpu.VMEM
    dma = pltpu.SemaphoreType.DMA
    scratch = [
        vm((K, D, E), BF16), vm((N, K * T, E), BF16), vm((N, K, E), BF16),
        vm((Z, 2, T, R), BF16), vm((2, Z * T, R), BF16), vm((2, R, Z * T), BF16), vm((K * T, V), F32), vm((K * T, V), BF16),
        vm((N, 8, T), F32),
        vm((half, K, T, E), BF16), vm((half, K, T, E), BF16),
        vm((half, K, T, E), BF16), vm((half, K, T, E), BF16),
        vm((K, T, E), F32), vm((D, V), BF16), vm((Z, R, V), BF16),
        vm((Z, R, V), F32), vm((2, Z, R, V), BF16), vm((2, Z, R, V), BF16),
        vm((K, Z * T, E), BF16), vm((N, T, E), BF16), vm((N, T, E), BF16),
        vm((T, E), F32), vm((K, R, E), F32), vm((K, R, E), BF16), vm((K, R, E), BF16),
        vm((K, T), F32),
        dma((K,)), dma((half, K)), dma((half, K)), dma((N, K)), dma((N,)), dma((N,)),
        dma((Z,)), dma((Z,)), dma((N,)), dma((N,)),
        dma((half, K)), dma((half, K)), dma((half, K)), dma((half, K)),
        dma((Z,)), dma((Z,)), dma((2, Z)), dma((2, Z)), dma((N,)), dma((N,)),
        dma((2, Z, K + 1)), dma((Z, K + 1)), dma((K + 1,)), dma((K + 1,)),
    ]
    spec = pl.BlockSpec(memory_space=pltpu.VMEM)
    hidden_grad, proj_grad, vocab_grad = pl.pallas_call(
        functools.partial(kernel, M, N),
        out_shape=(
            jax.ShapeDtypeStruct((T, E), BF16),
            jax.ShapeDtypeStruct((K, R, E), BF16),
            jax.ShapeDtypeStruct((R, V), BF16),
        ),
        in_specs=[spec, spec, pl.BlockSpec(memory_space=pltpu.MemorySpace.HBM)] + [spec] * 4,
        out_specs=(spec, spec, spec),
        scratch_shapes=scratch,
        compiler_params=pltpu.CompilerParams(
            collective_id=0, has_side_effects=True, vmem_limit_bytes=48 * 1024 * 1024
        ),
    )(hidden, mix_weight, w, vocab_weight, log_normalizer, targets[None, :], loss_grad[None, :])
    return hidden_grad, jnp.transpose(proj_grad, (1, 0, 2)), vocab_grad


def scoped(fn):
    def run(*args, **kw):
        tag = "_".join(str(a) for a in args if isinstance(a, int))
        with jax.named_scope(fn.__name__ + "_" + tag):
            return fn(*args, **kw)
    return run


def mix_rows(K, flip=False):
    B = 256 // K
    r = lax.broadcasted_iota(jnp.int32, (256, 256), 1 if flip else 0)
    c = lax.broadcasted_iota(jnp.int32, (256, 256), 0 if flip else 1)
    return (c == K * (r % B) + r // B).astype(F32).astype(BF16)


def fast_kernel(
    M, N,
    hid_hbm, mix_hbm, proj_hbm, vw_hbm, logz_hbm, tg_hbm, loss_hbm,
    out_hidden, out_proj, out_vocab,
    raw, w, hida, vw, vwe, vwt, mix, logz, targets, loss,
    ctx, ctxz, mix_all, htr, logit, lg, lgall, tgt, scale, pg,
    vgb, vgy, vsum, vout, vin, hss, hsr, own_hs, acc, psend, precv, mgrad,
    l_sem, w_sem, ctx_s, ctx_f, ctx_r, mix_s, mix_r, hz_s, hz_r, hp_s, hp_r,
    vx_s, vx_r, vp_s, vp_r, vwz_s, vwy_s, vw_r, tgt_s, tgt_r,
    lz_s, lx_s, lp_s, lg_r, vy_s, vy_r, vz_s, vz_r, hs_s, hs_r, pp_s, pp_r, sc_s, sc_r,
):
    K, D, E = w.shape
    T = hida.shape[2]
    H = D // 2
    V = vw.shape[1]
    R = D // M
    J = E // 128
    S = E // M
    half = N // 2
    Z = M // 2
    B = 256 // K
    me_t = lax.axis_index("tok")
    me_v = lax.axis_index("voc")
    chip = me_v // 2
    core = me_v % 2
    partner = me_v + 1 - 2 * core
    z = me_t // 2
    y = me_t % 2
    ypart = me_t + 1 - 2 * y
    has_r = z + 1 < Z
    has_l = z >= 1
    sends = []

    def remote(src, dst, ss, rs, dev):
        return pltpu.make_async_remote_copy(
            src_ref=src, dst_ref=dst, send_sem=ss, recv_sem=rs,
            device_id=dev, device_id_type=MESH,
        )

    def send(src, dst, ss, rs, dev, pred=None):
        c = remote(src, dst, ss, rs, dev)
        if pred is None:
            c.start()
        else:
            pl.when(pred)(c.start)
        sends.append((pred, c))

    def arrived(ref, rs, ss):
        remote(ref, ref, ss, rs, {"voc": partner}).wait_recv()

    def mate(j):
        if j == 0:
            return z
        near = jnp.minimum(z, Z - 1 - z)
        d = (j + 1) // 2
        both = z + d if j % 2 == 1 else z - d
        return jnp.where(j <= 2 * near, both, jnp.where(2 * z < Z, j, Z - 1 - j))

    def onward(zz):
        right = zz < z
        there = (right & has_r) | (jnp.logical_not(right) & has_l)
        return there, me_t + jnp.where(right, 2, -2)

    chunks = 4
    n = D // chunks

    def w_copy(c, j):
        return pltpu.make_async_copy(
            proj_hbm.at[pl.ds(c * n, n), :, pl.ds(j * 128, 128)],
            raw.at[j, pl.ds(c * n, n)], w_sem.at[c, j])

    loads = [
        pltpu.make_async_copy(hid_hbm.at[:, pl.ds(0, H)], hida.at[z, 0], l_sem.at[0]),
        pltpu.make_async_copy(hid_hbm.at[:, pl.ds(H, H)], hida.at[z, 1], l_sem.at[1]),
        pltpu.make_async_copy(vw_hbm, vw, l_sem.at[2]),
        pltpu.make_async_copy(mix_hbm, mix, l_sem.at[3]),
        pltpu.make_async_copy(logz_hbm, logz, l_sem.at[4]),
        pltpu.make_async_copy(tg_hbm, targets, l_sem.at[5]),
        pltpu.make_async_copy(loss_hbm, loss, l_sem.at[6]),
    ]
    for c in loads:
        c.start()

    bar = pltpu.get_barrier_semaphore()
    for d in range(1, M):
        pl.semaphore_signal(bar, inc=1, device_id={"tok": lax.rem(me_t + d, M)}, device_id_type=MESH)
    for d in range(1, N):
        pl.semaphore_signal(bar, inc=1, device_id={"voc": lax.rem(me_v + d, N)}, device_id_type=MESH)

    perm = mix_rows(K)

    @scoped
    def unmix(c):
        for j in range(J):
            w_copy(c, j).wait()
        for b in range(c * n // B, (c + 1) * n // B):
            x = jnp.concatenate(
                [raw.at[j].reshape(D * K, 128)[b * 256:(b + 1) * 256, :] for j in range(J)], axis=1)
            rows = jnp.dot(perm, x, preferred_element_type=F32).astype(BF16)
            for k in range(K):
                w[k, b * B:(b + 1) * B, :] = rows[k * B:(k + 1) * B]

    with jax.named_scope("loads"):
        for c in loads[:3]:
            c.wait()
    for c in range(chunks):
        for j in range(J):
            w_copy(c, j).start()
    with jax.named_scope("barrier"):
        pl.semaphore_wait(bar, M + N - 2)

    def vw_piece(ci, t):
        return vwe.at[pl.ds(ci * 2, 2), rows_of(t, S)]

    @scoped
    def vw_own():
        for i in range(1, half):
            ci = lax.rem(chip + i, half)
            for c in range(2):
                arrived(vwe.at[ci * 2 + c, rows_of(me_t, S)], vx_r.at[ci * 2 + c], vx_s.at[i, c])
            piece = vw_piece(ci, me_t)
            send(piece, piece, vwy_s.at[i, z], vw_r.at[ci, me_t], {"tok": ypart})
            for d in range(1, Z):
                send(piece, piece, vwz_s.at[i, d], vw_r.at[ci, me_t], {"tok": lax.rem(me_t + 2 * d, M)})

    def hid_piece(zz, side, p):
        return hida.at[zz, side, pl.ds(p * (T // 2), T // 2)]

    def slab(v, t):
        return pl.ds(pl.multiple_of(v * E + t * S, S), S)

    for i in range(1, half):
        for c in range(2):
            v = lax.rem(chip + i, half) * 2 + c
            send(vw.at[slab(v, me_t)], vwe.at[me_v, rows_of(me_t, S)],
                 vx_s.at[i, c], vx_r.at[me_v], {"voc": v})
    for p in range(2):
        piece = hid_piece(z, core, p)
        send(piece, piece, hz_s.at[0, z, p], hz_r.at[z, p], {"tok": me_t + 2}, has_r)
        send(piece, piece, hz_s.at[1, z, p], hz_r.at[z, p], {"tok": me_t - 2}, has_l)
    for c in loads[3:]:
        c.wait()
    for d in range(1, N):
        send(mix, mix_all.at[d], mix_s.at[d], mix_r.at[d], {"voc": lax.rem(me_v + d, N)})
    send(vw.at[rows_of(partner, E)], vwe.at[me_v], vp_s.at[0], vp_r.at[0], {"voc": partner})
    for c in range(chunks):
        unmix(c)
    vw_own()

    def context(zz, k):
        both = jnp.dot(hida[zz, 0], w[k, 0:H, :], preferred_element_type=F32)
        both = both + jnp.dot(hida[zz, 1], w[k, H:D, :], preferred_element_type=F32)
        return jnp.tanh(both).astype(BF16)

    for k in range(K):
        with jax.named_scope("context"):
            ctx[me_v, k * T:(k + 1) * T, :] = context(z, k)
        piece = ctx.at[me_v, pl.ds(k * T, T)]
        for i in range(1, half):
            send(piece, piece, ctx_s.at[i, k], ctx_r.at[me_v, k],
                 {"voc": lax.rem(chip + i, half) * 2 + core})
        send(piece, piece, ctx_s.at[0, k], ctx_r.at[me_v, k], {"voc": partner})

    @scoped
    def add_logits(s, first=False):
        part = jnp.dot(ctx[s], vw[rows_of(s, E), :], preferred_element_type=F32)
        logit[...] = part if first else logit[...] + part

    @scoped
    def relay_vw(j):
        zz = mate(j)
        t = zz * 2 + y
        for i in range(1, half):
            ci = lax.rem(chip + i, half)
            piece = vw_piece(ci, t)
            arrived(piece, vw_r.at[ci, t], vwy_s.at[i, zz])
            send(piece, piece, vwy_s.at[i, zz], vw_r.at[ci, t], {"tok": ypart})

    @scoped
    def relay_hid(j, p, fwd):
        zz = mate(j)
        there, to = onward(zz)
        piece = hid_piece(zz, core, p)
        on = remote(piece, piece, hz_s.at[0, zz, p], hz_r.at[zz, p], {"tok": to})
        over = remote(piece, piece, hp_s.at[zz, p], hp_r.at[zz, p], {"voc": partner})

        @pl.when(there if fwd else jnp.logical_not(there))
        def _():
            arrived(piece, hz_r.at[zz, p], hz_s.at[0, zz, p])
            if fwd:
                on.start()
            over.start()
        if fwd:
            sends.append((there, on))
            sends.append((None, over))

    @scoped
    def ctx_mate(j, ks):
        zz = mate(j)
        if ks[0] == 0:
            for p in range(2):
                arrived(hid_piece(zz, 1 - core, p), hp_r.at[zz, p], hp_s.at[zz, p])
        for k in ks:
            ctxz[zz, k * T:(k + 1) * T, :] = context(zz, k)

    @scoped
    def ctx_pass(k):
        for i in range(1, half):
            s = lax.rem(chip - i + half, half) * 2 + core
            piece = ctx.at[s, pl.ds(k * T, T)]
            arrived(piece, ctx_r.at[s, k], ctx_s.at[i, k])
            send(piece, piece, ctx_f.at[i, k], ctx_r.at[s, k], {"voc": partner})

    add_logits(me_v, True)
    for j in range(1, min(Z, 3)):
        relay_hid(j, 0, True)
    for k in range(K):
        arrived(ctx.at[partner, pl.ds(k * T, T)], ctx_r.at[partner, k], ctx_s.at[0, k])
    add_logits(partner)

    tcol = column(targets[...].astype(F32), V)
    ids = (me_v * V + lax.broadcasted_iota(jnp.int32, (T, V), 1)).astype(F32)
    onehot = (tcol == ids).astype(F32)
    mix_all[0] = mix[...]
    for d in range(1, N):
        arrived(mix_all.at[d], mix_r.at[d], mix_s.at[d])
    mixing = jnp.zeros((K, T), F32)
    for d in range(N):
        s = lax.rem(me_v - d + N, N)
        mixing = mixing + lax.dot_general(
            mix_all[d],
            hida[z, s // half, :, pl.ds(pl.multiple_of((s % half) * E, E), E)], NT,
            preferred_element_type=F32)
    exp_mix = jnp.exp(mixing)
    weights = exp_mix / jnp.sum(exp_mix, axis=0, keepdims=True)

    for j in range(1, min(Z, 3)):
        relay_hid(j, 1, True)
    ctx_pass(0)
    if Z > 1:
        relay_hid(1, 0, False)
        relay_hid(1, 1, False)
    ctx_pass(1)
    for j in range(1, Z):
        relay_vw(j)
    if Z > 1:
        ctx_mate(1, range(K))
    ctx_pass(2)
    for j in range(3, Z):
        relay_hid(j, 0, True)
    if Z > 2:
        relay_hid(2, 0, False)
    for k in range(3, K):
        ctx_pass(k)
    if Z > 2:
        relay_hid(2, 1, False)
    for i in range(1, half):
        add_logits(lax.rem(chip - i + half, half) * 2 + core)
    for i in range(1, half):
        s = lax.rem(chip - i + half, half) * 2 + 1 - core
        for k in range(K):
            arrived(ctx.at[s, pl.ds(k * T, T)], ctx_r.at[s, k], ctx_s.at[i, k])
        add_logits(s)

    lane = lax.broadcasted_iota(jnp.int32, (T, 128), 1)
    table = jnp.zeros((T, 128), F32)
    for k in range(K):
        part = jnp.sum(logit[k * T:(k + 1) * T, :] * onehot, axis=1, keepdims=True)
        table = jnp.where(lane == k, part, table)
    tgt[0] = table.T[0:8, :]
    for d in range(1, N):
        send(tgt.at[0], tgt.at[d], tgt_s.at[d], tgt_r.at[d], {"voc": lax.rem(me_v + d, N)})
    @scoped
    def scales():
        for d in range(1, N):
            arrived(tgt.at[d], tgt_r.at[d], tgt_s.at[d])
        target = tgt[0]
        for d in range(1, N):
            target = target + tgt[d]
        likely = jnp.exp(target[0:K, :] - logz[...])
        joint = weights * likely
        posterior = joint / jnp.sum(joint, axis=0, keepdims=True)
        scale[z, 0:K, :] = loss[...] * posterior
        mgrad[...] = loss[...] * (weights - posterior)
        for d in range(1, Z):
            send(scale.at[z], scale.at[z], sc_s.at[d], sc_r.at[z], {"tok": lax.rem(me_t + 2 * d, M)})

    def shares(zz, k):
        piece = lgall.at[zz, me_v, k]
        return [
            remote(piece, piece, lx_s.at[i, zz, k], lg_r.at[zz, me_v, k],
                   {"voc": lax.rem(chip + i, half) * 2 + core})
            for i in range(1, half)
        ] + [remote(piece, piece, lp_s.at[0, zz, k], lg_r.at[zz, me_v, k], {"voc": partner})]

    def share(zz, k):
        for c in shares(zz, k):
            c.start()
            sends.append((None, c))

    @scoped
    def own_out(k):
        rows = slice(k * T, (k + 1) * T)
        logit[rows, :] = jnp.exp(logit[rows, :] - column(logz[k:k + 1, :], V)) - onehot
        lgall[z, me_v, k] = logit[rows, :].astype(BF16)
        share(z, k)

    @scoped
    def own_line(k):
        piece = lgall.at[z, me_v, k]
        send(piece, piece, lz_s.at[0, z, k], lg_r.at[z, me_v, k], {"tok": me_t + 2}, has_r)
        send(piece, piece, lz_s.at[1, z, k], lg_r.at[z, me_v, k], {"tok": me_t - 2}, has_l)

    @scoped
    def relay_lg(k, j, fwd):
        zz = mate(j)
        there, to = onward(zz)
        piece = lgall.at[zz, me_v, k]
        on = remote(piece, piece, lz_s.at[0, zz, k], lg_r.at[zz, me_v, k], {"tok": to})

        @pl.when(there if fwd else jnp.logical_not(there))
        def _():
            arrived(piece, lg_r.at[zz, me_v, k], lp_s.at[0, zz, k])
            if fwd:
                on.start()
            for c in shares(zz, k):
                c.start()
        if fwd:
            sends.append((there, on))
            for c in shares(zz, k):
                sends.append((None, c))

    @scoped
    def cross_lg(k, j):
        zz = mate(j)
        for i in range(1, half):
            s = lax.rem(chip - i + half, half) * 2 + core
            piece = lgall.at[zz, s, k]
            arrived(piece, lg_r.at[zz, s, k], lp_s.at[0, zz, k])
            send(piece, piece, lp_s.at[i, zz, k], lg_r.at[zz, s, k], {"voc": partner})

    @scoped
    def pre_grad(k, j):
        zz = mate(j)
        rows = slice(k * T, (k + 1) * T)
        for i in range(half):
            s = lax.rem(chip + i, half) * 2 + 1 - core
            arrived(lgall.at[zz, s, k], lg_r.at[zz, s, k], lp_s.at[0, zz, k])
        total = None
        for s in range(N):
            part = jnp.dot(lgall[zz, s, k], vwt[s], preferred_element_type=F32)
            total = part if total is None else total + part
        c = (ctx[me_v, rows, :] if j == 0 else ctxz[zz, rows, :]).astype(F32)
        if k == 0:
            if j > 0:
                arrived(scale.at[zz], sc_r.at[zz], sc_s.at[1])
        total = total * column(scale[zz, k:k + 1, :], E)
        pg[k, rows_of(zz, T), :] = (total * (1.0 - c * c)).astype(BF16)

    def hid_part(s):
        total = jnp.zeros((T, E), F32)
        for k in range(K):
            total = total + lax.dot_general(
                pg[k, rows_of(z, T), :], w[k, rows_of(s, E), :], NT,
                preferred_element_type=F32)
        return total

    @scoped
    def hid_send(d):
        s = lax.rem(me_v + d, N)
        if d == 0:
            own_hs[...] = hid_part(s)
        else:
            hss[d] = hid_part(s).astype(BF16)
            send(hss.at[d], hsr.at[d], hs_s.at[d], hs_r.at[d], {"voc": s})

    @scoped
    def pair_sums():
        for d in list(range(1, Z)) + [0]:
            zz = lax.rem(z + d, Z)
            arrived(vgy.at[zz], vy_r.at[zz], vy_s.at[zz])
            total = vgb[rows_of(zz * 2 + y, R), :].astype(F32) + vgy[zz].astype(F32)
            if d == 0:
                vsum[...] = total
            else:
                vout[zz] = total.astype(BF16)
                send(vout.at[zz], vin.at[z], vz_s.at[d], vz_r.at[z], {"tok": zz * 2 + y})

    pieces = [(k, 0, E) for k in range(K)]
    if E % 256 == 0:
        pieces[-1:] = [(K - 1, 0, E // 2), (K - 1, E // 2, E // 2)]

    @scoped
    def proj_part(k):
        for p, (kk, lo, wide) in enumerate(pieces):
            if kk == k:
                lanes = slice(lo, lo + wide)
                psend[k, :, lanes] = jnp.dot(
                    htr[1 - y], pg[k, :, lanes], preferred_element_type=F32).astype(BF16)
                send(psend.at[k, :, pl.ds(lo, wide)], precv.at[k, :, pl.ds(lo, wide)],
                     pp_s.at[p], pp_r.at[p], {"tok": ypart})
        acc[k] = jnp.dot(htr[y], pg[k], preferred_element_type=F32)

    @scoped
    def vocab_part():
        for k in range(K):
            rows = slice(k * T, (k + 1) * T)
            lg[rows, :] = (column(scale[z, k:k + 1, :], V) * logit[rows, :]).astype(BF16)
        for s in range(N):
            vgb[s * E:(s + 1) * E, :] = lax.dot_general(
                ctx[s], lg[...], TN, preferred_element_type=F32).astype(BF16)
        for zz in range(Z):
            send(vgb.at[pl.ds((zz * 2 + 1 - y) * R, R)], vgy.at[zz], vy_s.at[zz], vy_r.at[zz],
                 {"tok": ypart})

    @scoped
    def vw_done():
        vwe[me_v] = vw[rows_of(me_v, E), :]
        arrived(vwe.at[partner], vp_r.at[0], vp_s.at[0])
        for i in range(1, half):
            ci = lax.rem(chip + i, half)
            for zz in range(Z):
                t = zz * 2 + 1 - y
                arrived(vw_piece(ci, t), vw_r.at[ci, t], vwy_s.at[i, zz])
        for s in range(N):
            vwt[s] = vwe[s].T

    @scoped
    def turn():
        for b in range(2):
            col = (z * 2 + b) * R
            for zz in range(Z):
                htr[b, :, zz * T:(zz + 1) * T] = hida[
                    zz, col // H, :, pl.ds(pl.multiple_of(col % H, R), R)].T

    hid_order = list(range(1, N)) + [0]
    events = []

    def at(time, fn, *args):
        events.append((time, len(events), fn, args))

    late = [1.2 + 2.2 * (k - 1) if k else 0.0 for k in range(K)]
    for k in range(K):
        at(0.01 * k, own_out, k)
        at(0.01 * k if k < 2 else 3.0 + 1.62 * (k - 2), own_line, k)
        for j in range(1, Z):
            at(late[k] + 2.2 * ((j + 1) // 2), relay_lg, k, j, True)
        for j in range(1, Z):
            at(late[k] + 2.2 * j, relay_lg, k, j, False)
        for j in range(Z):
            time = 2.2 * (j + 1) + (1.2 * k if j == 0 else 1.2 * late[k])
            at(time, cross_lg, k, j)
            at(time + (0.8 if j == Z - 1 else 1.2), pre_grad, k, j)
        at(2.2 * Z + 1.2 * late[k] + 0.81, proj_part, k)
        if k > 0:
            for d in hid_order[(k - 1) * N // K:(k if k < K - 1 else K) * N // K]:
                at(2.2 * Z + 1.2 * late[k] + 0.82, hid_send, d)
    at(2.201, scales)
    if Z > 2:
        at(0.3, ctx_mate, 2, range(K))
    at(2.202, vocab_part)
    for j in range(3, Z):
        at(0.2, relay_hid, j, 1, True)
        at(2.25, relay_hid, j, 0, False)
        at(3.35, relay_hid, j, 1, False)
        at(4.5, ctx_mate, j, range(K))
    at(2.21, vw_done)
    at(4.6, turn)
    at(13.5, pair_sums)
    for _, _, fn, args in sorted(events, key=lambda e: e[:2]):
        fn(*args)

    vtot = vsum[...]
    for d in range(1, Z):
        zz = lax.rem(z + d, Z)
        arrived(vin.at[zz], vz_r.at[zz], vz_s.at[d])
        vtot = vtot + vin[zz].astype(F32)
    out_vocab[...] = vtot.astype(BF16)
    htot = own_hs[...]
    for d in range(1, N):
        arrived(hsr.at[d], hs_r.at[d], hs_s.at[d])
        htot = htot + hsr[d].astype(F32)
    mixf = mix[...].astype(F32)
    for k in range(K):
        htot = htot + column(mgrad[k:k + 1, :], E) * mixf[k:k + 1, :]
    out_hidden[...] = htot.astype(BF16)

    back = mix_rows(K, True)
    for p, (k, lo, wide) in enumerate(pieces):
        lanes = slice(lo, lo + wide)
        with jax.named_scope("precv"):
            arrived(precv.at[k, :, pl.ds(lo, wide)], pp_r.at[p], pp_s.at[p])
        psum = (acc[k, :, lanes] + precv[k, :, lanes].astype(F32)).astype(BF16)
        if k < K - 1:
            precv[k, :, lanes] = psum
            continue
        for b in range(R // B):
            rows = slice(b * B, (b + 1) * B)
            x = jnp.concatenate([precv[q, rows, lanes] for q in range(K - 1)] + [psum[rows]], axis=0)
            out = jnp.dot(back, x, preferred_element_type=F32).astype(BF16)
            for j in range(wide // 128):
                out_proj.at[lo // 128 + j].reshape(R * K, 128)[b * 256:(b + 1) * 256, :] = (
                    out[:, j * 128:(j + 1) * 128])
    with jax.named_scope("drain"):
        for pred, c in sends:
            if pred is None:
                c.wait_send()
            else:
                pl.when(pred)(c.wait_send)


def body_fast(M, N, hidden, mix_weight, comp_proj, vocab_weight, log_normalizer, targets, loss_grad):
    T, D = hidden.shape
    K, E = mix_weight.shape
    V = vocab_weight.shape[1]
    R = D // M
    J = E // 128
    half = N // 2
    Z = M // 2
    vm = pltpu.VMEM
    dma = pltpu.SemaphoreType.DMA
    scratch = [
        vm((J, D, K, 128), BF16), vm((K, D, E), BF16), vm((Z, 2, T, D // 2), BF16), vm((D, V), BF16),
        vm((N, E, V), BF16), vm((N, V, E), BF16), vm((K, E), BF16), vm((K, T), F32), vm((1, T), jnp.int32), vm((1, T), F32),
        vm((N, K * T, E), BF16), vm((Z, K * T, E), BF16), vm((N, K, E), BF16), vm((2, R, Z * T), BF16),
        vm((K * T, V), F32), vm((K * T, V), BF16), vm((Z, N, K, T, V), BF16), vm((N, 8, T), F32), vm((Z, 8, T), F32), vm((K, Z * T, E), BF16),
        vm((D, V), BF16), vm((Z, R, V), BF16),
        vm((R, V), F32), vm((Z, R, V), BF16), vm((Z, R, V), BF16),
        vm((N, T, E), BF16), vm((N, T, E), BF16),
        vm((T, E), F32), vm((K, R, E), F32), vm((K, R, E), BF16), vm((K, R, E), BF16),
        vm((K, T), F32),
        dma((7,)), dma((4, J)),
        dma((half, K)), dma((half, K)), dma((N, K)), dma((N,)), dma((N,)),
        dma((2, Z, 2)), dma((Z, 2)), dma((Z, 2)), dma((Z, 2)),
        dma((half, 2)), dma((N,)), dma((1,)), dma((1,)),
        dma((half, Z)), dma((half, Z)), dma((half, M)), dma((N,)), dma((N,)),
        dma((2, Z, K)), dma((half, Z, K)), dma((half, Z, K)), dma((Z, N, K)),
        dma((Z,)), dma((Z,)), dma((Z,)), dma((Z,)), dma((N,)), dma((N,)),
        dma((K + 1,)), dma((K + 1,)), dma((Z,)), dma((Z,)),
    ]
    spec = pl.BlockSpec(memory_space=pltpu.VMEM)
    hbm = pl.BlockSpec(memory_space=pltpu.MemorySpace.HBM)
    hid, proj, voc = pl.pallas_call(
        functools.partial(fast_kernel, M, N),
        out_shape=(
            jax.ShapeDtypeStruct((T, E), BF16),
            jax.ShapeDtypeStruct((J, R, K, 128), BF16),
            jax.ShapeDtypeStruct((R, V), BF16),
        ),
        in_specs=[hbm] * 7,
        out_specs=(spec, spec, spec),
        scratch_shapes=scratch,
        compiler_params=pltpu.CompilerParams(
            collective_id=0, has_side_effects=True, vmem_limit_bytes=47 * 1024 * 1024
        ),
    )(*[
        pltpu.with_memory_space_constraint(x, pltpu.MemorySpace.HBM)
        for x in (hidden, mix_weight, comp_proj, vocab_weight, log_normalizer, targets[None, :], loss_grad[None, :])
    ])
    return pl.pallas_call(
        store_kernel,
        out_shape=(
            jax.ShapeDtypeStruct((T, E), BF16),
            jax.ShapeDtypeStruct((R, K, E), BF16),
            jax.ShapeDtypeStruct((R, V), BF16),
        ),
        in_specs=[spec] * 3,
        out_specs=(hbm, hbm, hbm),
        scratch_shapes=[dma((J + 2,))],
        compiler_params=pltpu.CompilerParams(vmem_limit_bytes=4 * 1024 * 1024),
    )(hid, proj, voc)


def store_kernel(hid, proj, voc, out_hid, out_proj, out_voc, sem):
    J = proj.shape[0]
    copies = [pltpu.make_async_copy(hid, out_hid, sem.at[J]), pltpu.make_async_copy(voc, out_voc, sem.at[J + 1])]
    for j in range(J):
        copies.append(pltpu.make_async_copy(proj.at[j], out_proj.at[:, :, pl.ds(j * 128, 128)], sem.at[j]))
    for c in copies:
        c.start()
    for c in copies:
        c.wait()


def body(M, N, *args):
    hidden, mix_weight, comp_proj, vocab_weight = args[:4]
    T, D = hidden.shape
    K, E = mix_weight.shape
    V = vocab_weight.shape[1]
    gathered = 2 * (M // 2) * T * (K * N * V + D + 2 * K * E)
    shapes = K == 4 and E % 128 == 0 and (E // M) % 16 == 0 and (D // M) % (256 // K) == 0
    if shapes and gathered + 4 * K * D * E <= 28 * 1024 * 1024:
        return body_fast(M, N, *args)
    return body_base(M, N, *args)


def solution(mesh):
    in_specs = (
        P("tok", None),
        P(None, "voc"),
        P(None, None, "voc"),
        P(None, "voc"),
        P(None, "tok"),
        P("tok"),
        P("tok"),
    )
    out_specs = (P("tok", "voc"), P("tok", None, "voc"), P("tok", "voc"))
    return jax.shard_map(
        functools.partial(body, mesh.shape["tok"], mesh.shape["voc"]),
        mesh=mesh, in_specs=in_specs, out_specs=out_specs, check_vma=False,
    )
```

```python
import functools

import jax
import jax.numpy as jnp
from jax import lax
from jax.experimental import pallas as pl
from jax.experimental.pallas import tpu as pltpu
from jax.sharding import PartitionSpec as P

MESH = pl.DeviceIdType.MESH
F32 = jnp.float32
BF16 = jnp.bfloat16
NT = (((1,), (1,)), ((), ()))
TN = (((0,), (0,)), ((), ()))


def column(row, lanes):
    wide = jnp.broadcast_to(row, (128, row.shape[1])).T
    return jnp.concatenate([wide] * (lanes // 128), axis=1)


def kernel(
    M, N,
    hidden, mix, proj_hbm, vw, logz, targets, loss,
    out_hidden, out_proj, out_vocab,
    w, ctx, mix_all, hblk, hrow, htr, logit, lg, tgt,
    cgs, cgr, cgx, xr, own_cg, vgb, vgy, vsum, vout, vin, pg, hss, hsr, own_hs, acc, psend, precv, mgrad,
    w_sem, ctx_s, ctx_f, ctx_r, mix_s, mix_r, hid_s, hid_r, tgt_s, tgt_r,
    cgp_s, cgp_r, cgx_s, cgx_r, vy_s, vy_r, vz_s, vz_r, hs_s, hs_r, ag_s, ag_r, pp_s, pp_r,
):
    K, D, E = w.shape
    T = hidden.shape[0]
    V = vw.shape[1]
    R = D // M
    half = N // 2
    Z = M // 2
    me_t = lax.axis_index("tok")
    me_v = lax.axis_index("voc")
    chip = me_v // 2
    core = me_v % 2
    partner = me_v + 1 - 2 * core
    z = me_t // 2
    y = me_t % 2
    ypart = me_t + 1 - 2 * y
    sends = []

    def remote(src, dst, ss, rs, dev):
        return pltpu.make_async_remote_copy(
            src_ref=src, dst_ref=dst, send_sem=ss, recv_sem=rs,
            device_id=dev, device_id_type=MESH,
        )

    def send(src, dst, ss, rs, dev):
        c = remote(src, dst, ss, rs, dev)
        c.start()
        sends.append((None, c))

    def arrived(ref, rs, ss):
        remote(ref, ref, ss, rs, {"voc": partner}).wait_recv()

    for k in range(K):
        pltpu.make_async_copy(proj_hbm.at[k], w.at[k], w_sem.at[k]).start()
    for j in range(M):
        hblk[j // 2, j % 2] = hidden[:, j * R:(j + 1) * R]

    bar = pltpu.get_barrier_semaphore()
    for d in range(1, M):
        pl.semaphore_signal(bar, inc=1, device_id={"tok": lax.rem(me_t + d, M)}, device_id_type=MESH)
    for d in range(1, N):
        pl.semaphore_signal(bar, inc=1, device_id={"voc": lax.rem(me_v + d, N)}, device_id_type=MESH)
    pl.semaphore_wait(bar, M + N - 2)

    for d in range(1, N):
        send(mix, mix_all.at[d], mix_s.at[d], mix_r.at[d], {"voc": lax.rem(me_v + d, N)})
    mix_all[0] = mix[...]
    for d in range(1, Z):
        zz = lax.rem(z + d, Z)
        send(hblk.at[zz], hrow.at[:, pl.ds(z * T, T)], hid_s.at[d], hid_r.at[d],
             {"tok": zz * 2 + y})
    hrow[:, rows_of(z, T), :] = hblk[z]

    for k in range(K):
        pltpu.make_async_copy(proj_hbm.at[k], w.at[k], w_sem.at[k]).wait()
        ctx[me_v, k * T:(k + 1) * T, :] = jnp.tanh(
            jnp.dot(hidden[...], w[k], preferred_element_type=F32)
        ).astype(BF16)
        piece = ctx.at[me_v, pl.ds(k * T, T)]
        for i in range(1, half):
            send(piece, piece, ctx_s.at[i, k], ctx_r.at[me_v, k],
                 {"voc": lax.rem(chip + i, half) * 2 + core})
        send(piece, piece, ctx_s.at[0, k], ctx_r.at[me_v, k], {"voc": partner})

    def add_logits(s, first=False):
        part = jnp.dot(ctx[s], vw[pl.ds(pl.multiple_of(s * E, E), E), :],
                       preferred_element_type=F32)
        logit[...] = part if first else logit[...] + part

    add_logits(me_v, True)
    for k in range(K):
        arrived(ctx.at[partner, pl.ds(k * T, T)], ctx_r.at[partner, k], ctx_s.at[0, k])
    add_logits(partner)

    tcol = column(targets[...].astype(F32), V)
    ids = (me_v * V + lax.broadcasted_iota(jnp.int32, (T, V), 1)).astype(F32)
    onehot = (tcol == ids).astype(F32)
    for d in range(1, N):
        arrived(mix_all.at[d], mix_r.at[d], mix_s.at[d])
    mixing = jnp.zeros((K, T), F32)
    for d in range(N):
        s = lax.rem(me_v - d + N, N)
        mixing = mixing + lax.dot_general(
            mix_all[d], hidden[:, pl.ds(pl.multiple_of(s * E, E), E)], NT,
            preferred_element_type=F32)
    exp_mix = jnp.exp(mixing)
    weights = exp_mix / jnp.sum(exp_mix, axis=0, keepdims=True)

    for i in range(1, half):
        s = lax.rem(chip - i + half, half) * 2 + core
        for k in range(K):
            piece = ctx.at[s, pl.ds(k * T, T)]
            arrived(piece, ctx_r.at[s, k], ctx_s.at[i, k])
            send(piece, piece, ctx_f.at[i, k], ctx_r.at[s, k], {"voc": partner})
        add_logits(s)
    for i in range(1, half):
        s = lax.rem(chip - i + half, half) * 2 + 1 - core
        for k in range(K):
            arrived(ctx.at[s, pl.ds(k * T, T)], ctx_r.at[s, k], ctx_s.at[i, k])
        add_logits(s)

    lane = lax.broadcasted_iota(jnp.int32, (T, 128), 1)
    table = jnp.zeros((T, 128), F32)
    for k in range(K):
        part = jnp.sum(logit[k * T:(k + 1) * T, :] * onehot, axis=1, keepdims=True)
        table = jnp.where(lane == k, part, table)
    tgt[0] = table.T[0:8, :]
    for d in range(1, N):
        send(tgt.at[0], tgt.at[d], tgt_s.at[d], tgt_r.at[d], {"voc": lax.rem(me_v + d, N)})
    for k in range(K):
        rows = slice(k * T, (k + 1) * T)
        logit[rows, :] = jnp.exp(logit[rows, :] - column(logz[k:k + 1, :], V)) - onehot
    for d in range(1, N):
        arrived(tgt.at[d], tgt_r.at[d], tgt_s.at[d])
    target = tgt[0]
    for d in range(1, N):
        target = target + tgt[d]
    likely = jnp.exp(target[0:K, :] - logz[...])
    joint = weights * likely
    posterior = joint / jnp.sum(joint, axis=0, keepdims=True)
    factor = loss[...] * posterior
    mgrad[...] = loss[...] * (weights - posterior)
    for k in range(K):
        rows = slice(k * T, (k + 1) * T)
        lg[rows, :] = (column(factor[k:k + 1, :], V) * logit[rows, :]).astype(BF16)

    def cg_part(s, k):
        return lax.dot_general(
            lg[k * T:(k + 1) * T, :], vw[pl.ds(pl.multiple_of(s * E, E), E), :], NT,
            preferred_element_type=F32)

    for i in list(range(1, half)) + [0]:
        s = lax.rem(chip + i, half) * 2
        for k in range(K):
            cgs[i, k] = cg_part(s + 1 - core, k).astype(BF16)
            send(cgs.at[i, k], cgr.at[i, k], cgp_s.at[i, k], cgp_r.at[i, k], {"voc": partner})
        for k in range(K):
            part = cg_part(s + core, k)
            if i == 0:
                own_cg[k] = part
            else:
                arrived(cgr.at[i, k], cgp_r.at[i, k], cgp_s.at[i, k])
                cgx[i, k] = (part + cgr[i, k].astype(F32)).astype(BF16)
                send(cgx.at[i, k], xr.at[i, k], cgx_s.at[i, k], cgx_r.at[i, k], {"voc": s + core})

    for s in range(N):
        vgb[s * E:(s + 1) * E, :] = lax.dot_general(
            ctx[s], lg[...], TN, preferred_element_type=F32).astype(BF16)
    for zz in range(Z):
        send(vgb.at[pl.ds((zz * 2 + 1 - y) * R, R)], vgy.at[zz], vy_s.at[zz], vy_r.at[zz],
             {"tok": ypart})

    for d in range(1, Z):
        src = lax.rem(z - d + Z, Z)
        arrived(hrow.at[:, pl.ds(src * T, T)], hid_r.at[d], hid_s.at[d])
    for b in range(2):
        htr[b] = hrow[b].T

    pieces = [(k, 0, E) for k in range(K)]
    if E % 256 == 0:
        pieces[-1:] = [(K - 1, 0, E // 2), (K - 1, E // 2, E // 2)]

    def relay(t, p, way, pred):
        k, lo, wide = pieces[p]
        piece = pg.at[k, rows_of(t, T), pl.ds(lo, wide)]
        c = remote(piece, piece, ag_s.at[way, t, p], ag_r.at[t, p],
                   {"tok": me_t + 2 - 4 * way})
        pl.when(pred)(c.start)
        sends.append((pred, c))

    has_r = z + 1 < Z
    has_l = z >= 1
    for k in range(K):
        total = own_cg[k]
        arrived(cgr.at[0, k], cgp_r.at[0, k], cgp_s.at[0, k])
        total = total + cgr[0, k].astype(F32)
        for i in range(1, half):
            arrived(xr.at[i, k], cgx_r.at[i, k], cgx_s.at[i, k])
            total = total + xr[i, k].astype(F32)
        c = ctx[me_v, k * T:(k + 1) * T, :].astype(F32)
        pg[k, rows_of(z, T), :] = (total * (1.0 - c * c)).astype(BF16)
        if Z > 1:
            for p in range(len(pieces)):
                if pieces[p][0] == k:
                    relay(z, p, 0, has_r)
                    relay(z, p, 1, has_l)

    def hid_part(s):
        total = jnp.zeros((T, E), F32)
        for k in range(K):
            total = total + lax.dot_general(
                pg[k, rows_of(z, T), :], w[k, pl.ds(pl.multiple_of(s * E, E), E), :], NT,
                preferred_element_type=F32)
        return total

    def hid_send(d):
        s = lax.rem(me_v + d, N)
        if d == 0:
            own_hs[...] = hid_part(s)
        else:
            hss[d] = hid_part(s).astype(BF16)
            send(hss.at[d], hsr.at[d], hs_s.at[d], hs_r.at[d], {"voc": s})

    hid_order = list(range(1, N)) + [0]
    hid_per = -(-N // (len(pieces) - 1))

    def pair_sums():
        for zz in range(Z):
            arrived(vgy.at[zz], vy_r.at[zz], vy_s.at[zz])
            vsum[zz] = vgb[rows_of(zz * 2 + y, R), :].astype(F32) + vgy[zz].astype(F32)

    def hop(h):
        for way, at, ends in ((0, h, range(h + 1, Z)), (1, Z - 1 - h, range(Z - 1 - h))):
            copies = [
                remote(vout.at[way, e], vin.at[way, e], vz_s.at[way, e], vz_r.at[way, e],
                       {"tok": me_t + 2 - 4 * way})
                for e in ends
            ]

            @pl.when(z == at)
            def _(way=way, ends=ends, copies=copies):
                for e, c in zip(ends, copies):
                    part = vsum[e]
                    if h > 0:
                        arrived(vin.at[way, e], vz_r.at[way, e], vz_s.at[way, e])
                        part = part + vin[way, e].astype(F32)
                    vout[way, e] = part.astype(BF16)
                    c.start()
            for c in copies:
                sends.append((z == at, c))

    if Z == 1:
        for e in hid_order:
            hid_send(e)
    per = -(-(Z - 1) // (len(pieces) - 1))
    for p, (k, lo, wide) in enumerate(pieces):
        lanes = slice(lo, lo + wide)
        for d in range(1, Z):
            for there, t, way, more in (
                (z >= d, z - d, 0, has_r), (z + d < Z, z + d, 1, has_l),
            ):
                def _(t=t):
                    arrived(pg.at[k, rows_of(t, T), pl.ds(lo, wide)], ag_r.at[t, p], ag_s.at[0, t, p])
                pl.when(there)(_)
                if d < Z - 1:
                    relay(t, p, way, there & more)
            if d == 1:
                for e in hid_order[p * hid_per:(p + 1) * hid_per]:
                    hid_send(e)
        psend[k, :, lanes] = jnp.dot(
            htr[1 - y], pg[k, :, lanes], preferred_element_type=F32).astype(BF16)
        send(psend.at[k, :, pl.ds(lo, wide)], precv.at[k, :, pl.ds(lo, wide)],
             pp_s.at[p], pp_r.at[p], {"tok": ypart})
        acc[k, :, lanes] = jnp.dot(htr[y], pg[k, :, lanes], preferred_element_type=F32)
        if p == 0:
            pair_sums()
        for h in range(p * per, min((p + 1) * per, Z - 1)):
            hop(h)

    acc_v = vsum.at[z]
    for way, pred in ((0, has_l), (1, has_r)):
        @pl.when(pred)
        def _(way=way):
            arrived(vin.at[way, z], vz_r.at[way, z], vz_s.at[way, z])
            acc_v[...] += vin[way, z].astype(F32)
    out_vocab[...] = acc_v[...].astype(BF16)
    htot = own_hs[...]
    for d in range(1, N):
        arrived(hsr.at[d], hs_r.at[d], hs_s.at[d])
        htot = htot + hsr[d].astype(F32)
    mixf = mix[...].astype(F32)
    for k in range(K):
        htot = htot + column(mgrad[k:k + 1, :], E) * mixf[k:k + 1, :]
    out_hidden[...] = htot.astype(BF16)

    for p, (k, lo, wide) in enumerate(pieces):
        lanes = slice(lo, lo + wide)
        arrived(precv.at[k, :, pl.ds(lo, wide)], pp_r.at[p], pp_s.at[p])
        out_proj[k, :, lanes] = (acc[k, :, lanes] + precv[k, :, lanes].astype(F32)).astype(BF16)
    for pred, c in sends:
        if pred is None:
            c.wait_send()
        else:
            pl.when(pred)(c.wait_send)


def rows_of(block, size):
    return pl.ds(pl.multiple_of(block * size, size), size)


def body_base(M, N, hidden, mix_weight, comp_proj, vocab_weight, log_normalizer, targets, loss_grad):
    T, D = hidden.shape
    K, E = mix_weight.shape
    V = vocab_weight.shape[1]
    R = D // M
    half = N // 2
    Z = M // 2
    w = jnp.transpose(comp_proj, (1, 0, 2))
    vm = pltpu.VMEM
    dma = pltpu.SemaphoreType.DMA
    scratch = [
        vm((K, D, E), BF16), vm((N, K * T, E), BF16), vm((N, K, E), BF16),
        vm((Z, 2, T, R), BF16), vm((2, Z * T, R), BF16), vm((2, R, Z * T), BF16), vm((K * T, V), F32), vm((K * T, V), BF16),
        vm((N, 8, T), F32),
        vm((half, K, T, E), BF16), vm((half, K, T, E), BF16),
        vm((half, K, T, E), BF16), vm((half, K, T, E), BF16),
        vm((K, T, E), F32), vm((D, V), BF16), vm((Z, R, V), BF16),
        vm((Z, R, V), F32), vm((2, Z, R, V), BF16), vm((2, Z, R, V), BF16),
        vm((K, Z * T, E), BF16), vm((N, T, E), BF16), vm((N, T, E), BF16),
        vm((T, E), F32), vm((K, R, E), F32), vm((K, R, E), BF16), vm((K, R, E), BF16),
        vm((K, T), F32),
        dma((K,)), dma((half, K)), dma((half, K)), dma((N, K)), dma((N,)), dma((N,)),
        dma((Z,)), dma((Z,)), dma((N,)), dma((N,)),
        dma((half, K)), dma((half, K)), dma((half, K)), dma((half, K)),
        dma((Z,)), dma((Z,)), dma((2, Z)), dma((2, Z)), dma((N,)), dma((N,)),
        dma((2, Z, K + 1)), dma((Z, K + 1)), dma((K + 1,)), dma((K + 1,)),
    ]
    spec = pl.BlockSpec(memory_space=pltpu.VMEM)
    hidden_grad, proj_grad, vocab_grad = pl.pallas_call(
        functools.partial(kernel, M, N),
        out_shape=(
            jax.ShapeDtypeStruct((T, E), BF16),
            jax.ShapeDtypeStruct((K, R, E), BF16),
            jax.ShapeDtypeStruct((R, V), BF16),
        ),
        in_specs=[spec, spec, pl.BlockSpec(memory_space=pltpu.MemorySpace.HBM)] + [spec] * 4,
        out_specs=(spec, spec, spec),
        scratch_shapes=scratch,
        compiler_params=pltpu.CompilerParams(
            collective_id=0, has_side_effects=True, vmem_limit_bytes=48 * 1024 * 1024
        ),
    )(hidden, mix_weight, w, vocab_weight, log_normalizer, targets[None, :], loss_grad[None, :])
    return hidden_grad, jnp.transpose(proj_grad, (1, 0, 2)), vocab_grad


ORDER = (
    (0, 0), (0, 2), (2, 0), (11, 3, 0), (0, 1), (2, 1), (1, 1), (1, 2), (10, 2), (0, 3), (1, 0), (8,),
    (3, 0, 2), (3, 0, 1), (9,), (3, 0, 3), (4, 0, 1), (3, 1, 1), (4, 1, 1), (11, 3, 1), (4, 0, 2),
    (3, 1, 2), (2, 2), (12,), (4, 0, 3), (10, 3), (4, 1, 2), (5, 0, 2), (1, 3), (5, 0, 1), (5, 0, 0),
    (13,), (3, 1, 3), (2, 3), (6, 0, 2), (5, 0, 3), (5, 1, 0), (6, 0, 1), (6, 0, 0), (3, 2, 1), (3, 2, 2),
    (4, 1, 3), (4, 2, 1), (5, 1, 1), (6, 0, 3), (7, 0), (4, 2, 2), (5, 2, 0), (3, 2, 3), (5, 1, 2),
    (3, 3, 2), (3, 3, 1), (6, 1, 0), (5, 3, 0), (4, 2, 3), (5, 1, 3), (6, 1, 1), (4, 3, 2), (6, 1, 2),
    (6, 1, 3), (7, 1), (3, 3, 3), (4, 3, 1), (5, 2, 3), (4, 3, 3), (5, 2, 1), (5, 2, 2), (6, 3, 0),
    (6, 2, 2), (6, 2, 0), (5, 3, 1), (6, 2, 3), (15,), (5, 3, 2), (6, 2, 1), (7, 2), (5, 3, 3), (6, 3, 1),
    (14, 1), (6, 3, 2), (6, 3, 3), (7, 3), (14, 0), (14, 2), (14, 3),
)


def scoped(fn):
    def run(*args, **kw):
        tag = "_".join(str(a) for a in args if isinstance(a, int))
        with jax.named_scope(fn.__name__ + "_" + tag):
            return fn(*args, **kw)
    return run


def mix_rows(K, flip=False):
    B = 256 // K
    r = lax.broadcasted_iota(jnp.int32, (256, 256), 1 if flip else 0)
    c = lax.broadcasted_iota(jnp.int32, (256, 256), 0 if flip else 1)
    return (c == K * (r % B) + r // B).astype(F32).astype(BF16)


def fast_kernel(
    M, N,
    hid_hbm, mix_hbm, proj_hbm, vw_hbm, logz_hbm, tg_hbm, loss_hbm,
    out_hidden, out_proj, out_vocab,
    raw, w, hida, vw, vwe, vwt, mix, logz, targets, loss,
    ctx, ctxz, mix_all, htr, logit, lg, lgall, tgt, scale, pg,
    vgb, vgy, vsum, vout, vin, hss, hsr, own_hs, acc, psend, precv, mgrad,
    l_sem, w_sem, ctx_s, ctx_f, ctx_r, mix_s, mix_r, hz_s, hz_r, hp_s, hp_r,
    vx_s, vx_r, vp_s, vp_r, vwz_s, vwz_r, vwy_s, vwy_r, tgt_s, tgt_r,
    lz_s, lx_s, lp_s, lg_r, vy_s, vy_r, vz_s, vz_r, hs_s, hs_r, pp_s, pp_r, sc_s, sc_r,
):
    K, D, E = w.shape
    T = hida.shape[2]
    H = D // 2
    V = vw.shape[1]
    R = D // M
    J = E // 128
    half = N // 2
    Z = M // 2
    B = 256 // K
    me_t = lax.axis_index("tok")
    me_v = lax.axis_index("voc")
    chip = me_v // 2
    core = me_v % 2
    partner = me_v + 1 - 2 * core
    z = me_t // 2
    y = me_t % 2
    ypart = me_t + 1 - 2 * y
    has_r = z + 1 < Z
    has_l = z >= 1
    sends = []

    def remote(src, dst, ss, rs, dev):
        return pltpu.make_async_remote_copy(
            src_ref=src, dst_ref=dst, send_sem=ss, recv_sem=rs,
            device_id=dev, device_id_type=MESH,
        )

    def send(src, dst, ss, rs, dev, pred=None):
        c = remote(src, dst, ss, rs, dev)
        if pred is None:
            c.start()
        else:
            pl.when(pred)(c.start)
        sends.append((pred, c))

    def arrived(ref, rs, ss):
        remote(ref, ref, ss, rs, {"voc": partner}).wait_recv()

    def mate(j):
        if j == 0:
            return z
        near = jnp.minimum(z, Z - 1 - z)
        d = (j + 1) // 2
        both = z + d if j % 2 == 1 else z - d
        return jnp.where(j <= 2 * near, both, jnp.where(2 * z < Z, j, Z - 1 - j))

    def onward(zz):
        right = zz < z
        there = (right & has_r) | (jnp.logical_not(right) & has_l)
        return there, me_t + jnp.where(right, 2, -2)

    chunks = 4
    n = D // chunks

    def w_copy(c, j):
        return pltpu.make_async_copy(
            proj_hbm.at[pl.ds(c * n, n), :, pl.ds(j * 128, 128)],
            raw.at[j, pl.ds(c * n, n)], w_sem.at[c, j])

    loads = [
        pltpu.make_async_copy(hid_hbm.at[:, pl.ds(0, H)], hida.at[z, 0], l_sem.at[0]),
        pltpu.make_async_copy(hid_hbm.at[:, pl.ds(H, H)], hida.at[z, 1], l_sem.at[1]),
        pltpu.make_async_copy(vw_hbm, vw, l_sem.at[2]),
        pltpu.make_async_copy(mix_hbm, mix, l_sem.at[3]),
        pltpu.make_async_copy(logz_hbm, logz, l_sem.at[4]),
        pltpu.make_async_copy(tg_hbm, targets, l_sem.at[5]),
        pltpu.make_async_copy(loss_hbm, loss, l_sem.at[6]),
    ]
    for c in loads:
        c.start()

    bar = pltpu.get_barrier_semaphore()
    for d in range(1, M):
        pl.semaphore_signal(bar, inc=1, device_id={"tok": lax.rem(me_t + d, M)}, device_id_type=MESH)
    for d in range(1, N):
        pl.semaphore_signal(bar, inc=1, device_id={"voc": lax.rem(me_v + d, N)}, device_id_type=MESH)

    perm = mix_rows(K)

    @scoped
    def unmix(c):
        for j in range(J):
            w_copy(c, j).wait()
        for b in range(c * n // B, (c + 1) * n // B):
            x = jnp.concatenate(
                [raw.at[j].reshape(D * K, 128)[b * 256:(b + 1) * 256, :] for j in range(J)], axis=1)
            rows = jnp.dot(perm, x, preferred_element_type=F32).astype(BF16)
            for k in range(K):
                w[k, b * B:(b + 1) * B, :] = rows[k * B:(k + 1) * B]

    with jax.named_scope("loads"):
        for c in loads[:3]:
            c.wait()
    for c in range(chunks):
        for j in range(J):
            w_copy(c, j).start()
    with jax.named_scope("barrier"):
        pl.semaphore_wait(bar, M + N - 2)

    g = z % 2
    zpair = me_t + 2 - 4 * g

    def vw_rows(yy, part):
        return pl.ds(pl.multiple_of(yy * (E // 2) + part * (E // 4), E // 4), E // 4)

    def vw_send():
        for i in range(1, half):
            for c in range(2):
                v = lax.rem(chip + i, half) * 2 + c
                rows = vw_rows(y, g)
                send(vw.at[pl.ds(pl.multiple_of(v * E + rows.start, E // 4), rows.size)],
                     vwe.at[me_v, rows], vx_s.at[i, c], vx_r.at[me_v], {"voc": v})

    @scoped
    def vw_pass():
        for i in range(1, half):
            ci = lax.rem(chip + i, half)
            for c in range(2):
                arrived(vwe.at[ci * 2 + c, vw_rows(y, g)], vx_r.at[ci * 2 + c], vx_s.at[i, c])
            piece = vwe.at[pl.ds(ci * 2, 2), vw_rows(y, g)]
            send(piece, piece, vwz_s.at[i], vwz_r.at[ci], {"tok": zpair})
            send(piece, piece, vwy_s.at[i, 0], vwy_r.at[ci, 0], {"tok": ypart})

    @scoped
    def vw_turn():
        for i in range(1, half):
            ci = lax.rem(chip + i, half)
            piece = vwe.at[pl.ds(ci * 2, 2), vw_rows(y, 1 - g)]
            arrived(piece, vwz_r.at[ci], vwz_s.at[i])
            send(piece, piece, vwy_s.at[i, 1], vwy_r.at[ci, 1], {"tok": ypart})

    def hid_piece(zz, side, p):
        return hida.at[zz, side, pl.ds(p * (T // 2), T // 2)]

    vw_send()
    for p in range(2):
        piece = hid_piece(z, core, p)
        send(piece, piece, hz_s.at[0, z, p], hz_r.at[z, p], {"tok": me_t + 2}, has_r)
        send(piece, piece, hz_s.at[1, z, p], hz_r.at[z, p], {"tok": me_t - 2}, has_l)
    for c in loads[3:]:
        c.wait()
    for d in range(1, N):
        send(mix, mix_all.at[d], mix_s.at[d], mix_r.at[d], {"voc": lax.rem(me_v + d, N)})
    send(vw.at[rows_of(partner, E)], vwe.at[me_v], vp_s.at[0], vp_r.at[0], {"voc": partner})
    for c in range(chunks):
        unmix(c)

    def context(zz, k):
        both = jnp.dot(hida[zz, 0], w[k, 0:H, :], preferred_element_type=F32)
        both = both + jnp.dot(hida[zz, 1], w[k, H:D, :], preferred_element_type=F32)
        return jnp.tanh(both).astype(BF16)

    for k in range(K):
        with jax.named_scope("context"):
            ctx[me_v, k * T:(k + 1) * T, :] = context(z, k)
        if k == 1:
            vw_pass()
        piece = ctx.at[me_v, pl.ds(k * T, T)]
        for i in range(1, half):
            send(piece, piece, ctx_s.at[i, k], ctx_r.at[me_v, k],
                 {"voc": lax.rem(chip + i, half) * 2 + core})
        send(piece, piece, ctx_s.at[0, k], ctx_r.at[me_v, k], {"voc": partner})

    @scoped
    def add_logits(s, first=False):
        part = jnp.dot(ctx[s], vw[rows_of(s, E), :], preferred_element_type=F32)
        logit[...] = part if first else logit[...] + part

    @scoped
    def relay_hid(j, p, fwd):
        zz = mate(j)
        there, to = onward(zz)
        piece = hid_piece(zz, core, p)
        on = remote(piece, piece, hz_s.at[0, zz, p], hz_r.at[zz, p], {"tok": to})
        over = remote(piece, piece, hp_s.at[zz, p], hp_r.at[zz, p], {"voc": partner})

        @pl.when(there if fwd else jnp.logical_not(there))
        def _():
            arrived(piece, hz_r.at[zz, p], hz_s.at[0, zz, p])
            if fwd:
                on.start()
            over.start()
        if fwd:
            sends.append((there, on))
            sends.append((None, over))

    @scoped
    def ctx_mate(j, ks):
        zz = mate(j)
        if ks[0] == 0:
            for p in range(2):
                arrived(hid_piece(zz, 1 - core, p), hp_r.at[zz, p], hp_s.at[zz, p])
        for k in ks:
            ctxz[zz, k * T:(k + 1) * T, :] = context(zz, k)

    @scoped
    def ctx_pass(k):
        for i in range(1, half):
            s = lax.rem(chip - i + half, half) * 2 + core
            piece = ctx.at[s, pl.ds(k * T, T)]
            arrived(piece, ctx_r.at[s, k], ctx_s.at[i, k])
            send(piece, piece, ctx_f.at[i, k], ctx_r.at[s, k], {"voc": partner})

    add_logits(me_v, True)
    for j in range(1, min(Z, 3)):
        relay_hid(j, 0, True)
    for k in range(K):
        arrived(ctx.at[partner, pl.ds(k * T, T)], ctx_r.at[partner, k], ctx_s.at[0, k])
    add_logits(partner)

    tcol = column(targets[...].astype(F32), V)
    ids = (me_v * V + lax.broadcasted_iota(jnp.int32, (T, V), 1)).astype(F32)
    onehot = (tcol == ids).astype(F32)
    mix_all[0] = mix[...]
    for d in range(1, N):
        arrived(mix_all.at[d], mix_r.at[d], mix_s.at[d])
    mixing = jnp.zeros((K, T), F32)
    for d in range(N):
        s = lax.rem(me_v - d + N, N)
        mixing = mixing + lax.dot_general(
            mix_all[d],
            hida[z, s // half, :, pl.ds(pl.multiple_of((s % half) * E, E), E)], NT,
            preferred_element_type=F32)
    exp_mix = jnp.exp(mixing)
    weights = exp_mix / jnp.sum(exp_mix, axis=0, keepdims=True)

    for j in range(1, min(Z, 3)):
        relay_hid(j, 1, True)
    ctx_pass(0)
    if Z > 1:
        relay_hid(1, 0, False)
        relay_hid(1, 1, False)
    ctx_pass(1)
    vw_turn()
    if Z > 1:
        ctx_mate(1, range(K))
    for j in range(3, Z):
        relay_hid(j, 0, True)
    ctx_pass(2)
    for j in range(3, Z):
        relay_hid(j, 1, True)
    if Z > 2:
        relay_hid(2, 0, False)
    for k in range(3, K):
        ctx_pass(k)
    if Z > 2:
        relay_hid(2, 1, False)
    for i in range(1, half):
        add_logits(lax.rem(chip - i + half, half) * 2 + core)
    for i in range(1, half):
        s = lax.rem(chip - i + half, half) * 2 + 1 - core
        for k in range(K):
            arrived(ctx.at[s, pl.ds(k * T, T)], ctx_r.at[s, k], ctx_s.at[i, k])
        add_logits(s)

    lane = lax.broadcasted_iota(jnp.int32, (T, 128), 1)
    table = jnp.zeros((T, 128), F32)
    for k in range(K):
        part = jnp.sum(logit[k * T:(k + 1) * T, :] * onehot, axis=1, keepdims=True)
        table = jnp.where(lane == k, part, table)
    tgt[0] = table.T[0:8, :]
    for d in range(1, N):
        send(tgt.at[0], tgt.at[d], tgt_s.at[d], tgt_r.at[d], {"voc": lax.rem(me_v + d, N)})
    @scoped
    def scales():
        for d in range(1, N):
            arrived(tgt.at[d], tgt_r.at[d], tgt_s.at[d])
        target = tgt[0]
        for d in range(1, N):
            target = target + tgt[d]
        likely = jnp.exp(target[0:K, :] - logz[...])
        joint = weights * likely
        posterior = joint / jnp.sum(joint, axis=0, keepdims=True)
        scale[z, 0:K, :] = loss[...] * posterior
        mgrad[...] = loss[...] * (weights - posterior)
        for d in range(1, Z):
            send(scale.at[z], scale.at[z], sc_s.at[d], sc_r.at[z], {"tok": lax.rem(me_t + 2 * d, M)})

    def shares(zz, k):
        piece = lgall.at[zz, me_v, k]
        return [
            remote(piece, piece, lx_s.at[i, zz, k], lg_r.at[zz, me_v, k],
                   {"voc": lax.rem(chip + i, half) * 2 + core})
            for i in range(1, half)
        ] + [remote(piece, piece, lp_s.at[0, zz, k], lg_r.at[zz, me_v, k], {"voc": partner})]

    def share(zz, k):
        for c in shares(zz, k):
            c.start()
            sends.append((None, c))

    @scoped
    def own_out(k):
        rows = slice(k * T, (k + 1) * T)
        logit[rows, :] = jnp.exp(logit[rows, :] - column(logz[k:k + 1, :], V)) - onehot
        lgall[z, me_v, k] = logit[rows, :].astype(BF16)

    @scoped
    def own_share(k):
        share(z, k)

    @scoped
    def own_line(k):
        piece = lgall.at[z, me_v, k]
        send(piece, piece, lz_s.at[0, z, k], lg_r.at[z, me_v, k], {"tok": me_t + 2}, has_r)
        send(piece, piece, lz_s.at[1, z, k], lg_r.at[z, me_v, k], {"tok": me_t - 2}, has_l)

    @scoped
    def relay_lg(k, j, fwd):
        zz = mate(j)
        there, to = onward(zz)
        piece = lgall.at[zz, me_v, k]
        on = remote(piece, piece, lz_s.at[0, zz, k], lg_r.at[zz, me_v, k], {"tok": to})

        @pl.when(there if fwd else jnp.logical_not(there))
        def _():
            arrived(piece, lg_r.at[zz, me_v, k], lp_s.at[0, zz, k])
            if fwd:
                on.start()
            for c in shares(zz, k):
                c.start()
        if fwd:
            sends.append((there, on))
            for c in shares(zz, k):
                sends.append((None, c))

    @scoped
    def cross_lg(k, j):
        zz = mate(j)
        for i in range(1, half):
            s = lax.rem(chip - i + half, half) * 2 + core
            piece = lgall.at[zz, s, k]
            arrived(piece, lg_r.at[zz, s, k], lp_s.at[0, zz, k])
            send(piece, piece, lp_s.at[i, zz, k], lg_r.at[zz, s, k], {"voc": partner})

    @scoped
    def pre_grad(k, j):
        zz = mate(j)
        rows = slice(k * T, (k + 1) * T)
        for i in range(half):
            s = lax.rem(chip + i, half) * 2 + 1 - core
            arrived(lgall.at[zz, s, k], lg_r.at[zz, s, k], lp_s.at[0, zz, k])
        total = None
        for s in range(N):
            part = jnp.dot(lgall[zz, s, k], vwt[s], preferred_element_type=F32)
            total = part if total is None else total + part
        c = (ctx[me_v, rows, :] if j == 0 else ctxz[zz, rows, :]).astype(F32)
        if k == 0:
            if j > 0:
                arrived(scale.at[zz], sc_r.at[zz], sc_s.at[1])
        total = total * column(scale[zz, k:k + 1, :], E)
        pg[k, rows_of(zz, T), :] = (total * (1.0 - c * c)).astype(BF16)

    def hid_part(s):
        total = jnp.zeros((T, E), F32)
        for k in range(K):
            total = total + lax.dot_general(
                pg[k, rows_of(z, T), :], w[k, rows_of(s, E), :], NT,
                preferred_element_type=F32)
        return total

    @scoped
    def hid_send(d):
        s = lax.rem(me_v + d, N)
        if d == 0:
            own_hs[...] = hid_part(s)
        else:
            hss[d] = hid_part(s).astype(BF16)
            send(hss.at[d], hsr.at[d], hs_s.at[d], hs_r.at[d], {"voc": s})

    @scoped
    def pair_sums():
        for d in list(range(1, Z)) + [0]:
            zz = lax.rem(z + d, Z)
            arrived(vgy.at[zz], vy_r.at[zz], vy_s.at[zz])
            total = vgb[rows_of(zz * 2 + y, R), :].astype(F32) + vgy[zz].astype(F32)
            if d == 0:
                vsum[...] = total
            else:
                vout[zz] = total.astype(BF16)
                send(vout.at[zz], vin.at[z], vz_s.at[d], vz_r.at[z], {"tok": zz * 2 + y})

    pieces = [(k, 0, E) for k in range(K)]
    if E % 256 == 0:
        pieces[-1:] = [(K - 1, 0, E // 2), (K - 1, E // 2, E // 2)]

    @scoped
    def proj_part(k):
        for p, (kk, lo, wide) in enumerate(pieces):
            if kk == k:
                lanes = slice(lo, lo + wide)
                psend[k, :, lanes] = jnp.dot(
                    htr[1 - y], pg[k, :, lanes], preferred_element_type=F32).astype(BF16)
                send(psend.at[k, :, pl.ds(lo, wide)], precv.at[k, :, pl.ds(lo, wide)],
                     pp_s.at[p], pp_r.at[p], {"tok": ypart})
        acc[k] = jnp.dot(htr[y], pg[k], preferred_element_type=F32)

    @scoped
    def vocab_part():
        for k in range(K):
            rows = slice(k * T, (k + 1) * T)
            lg[rows, :] = (column(scale[z, k:k + 1, :], V) * logit[rows, :]).astype(BF16)
        for s in range(N):
            vgb[s * E:(s + 1) * E, :] = lax.dot_general(
                ctx[s], lg[...], TN, preferred_element_type=F32).astype(BF16)
        for zz in range(Z):
            send(vgb.at[pl.ds((zz * 2 + 1 - y) * R, R)], vgy.at[zz], vy_s.at[zz], vy_r.at[zz],
                 {"tok": ypart})

    @scoped
    def vw_done():
        vwe[me_v] = vw[rows_of(me_v, E), :]
        arrived(vwe.at[partner], vp_r.at[0], vp_s.at[0])
        for i in range(1, half):
            ci = lax.rem(chip + i, half)
            for p, part in enumerate((g, 1 - g)):
                arrived(vwe.at[pl.ds(ci * 2, 2), vw_rows(1 - y, part)], vwy_r.at[ci, p], vwy_s.at[i, p])
        for s in range(N):
            vwt[s] = vwe[s].T

    @scoped
    def turn():
        for b in range(2):
            col = (z * 2 + b) * R
            for zz in range(Z):
                htr[b, :, zz * T:(zz + 1) * T] = hida[
                    zz, col // H, :, pl.ds(pl.multiple_of(col % H, R), R)].T

    def relay_on(k, j):
        relay_lg(k, j, True)

    def relay_in(k, j):
        relay_lg(k, j, False)

    def mate_ctx(j):
        ctx_mate(j, range(K))

    def hid_in(j, p):
        relay_hid(j, p, False)

    steps = (own_out, own_share, own_line, relay_on, relay_in, cross_lg, pre_grad, proj_part,
             scales, vocab_part, mate_ctx, hid_in, vw_done, turn, hid_send, pair_sums)
    for step, *rest in ORDER:
        steps[step](*rest)

    vtot = vsum[...]
    for d in range(1, Z):
        zz = lax.rem(z + d, Z)
        arrived(vin.at[zz], vz_r.at[zz], vz_s.at[d])
        vtot = vtot + vin[zz].astype(F32)
    out_vocab[...] = vtot.astype(BF16)
    htot = own_hs[...]
    for d in range(1, N):
        arrived(hsr.at[d], hs_r.at[d], hs_s.at[d])
        htot = htot + hsr[d].astype(F32)
    mixf = mix[...].astype(F32)
    for k in range(K):
        htot = htot + column(mgrad[k:k + 1, :], E) * mixf[k:k + 1, :]
    out_hidden[...] = htot.astype(BF16)

    back = mix_rows(K, True)
    for p, (k, lo, wide) in enumerate(pieces):
        lanes = slice(lo, lo + wide)
        with jax.named_scope("precv"):
            arrived(precv.at[k, :, pl.ds(lo, wide)], pp_r.at[p], pp_s.at[p])
        psum = (acc[k, :, lanes] + precv[k, :, lanes].astype(F32)).astype(BF16)
        if k < K - 1:
            precv[k, :, lanes] = psum
            continue
        for b in range(R // B):
            rows = slice(b * B, (b + 1) * B)
            x = jnp.concatenate([precv[q, rows, lanes] for q in range(K - 1)] + [psum[rows]], axis=0)
            out = jnp.dot(back, x, preferred_element_type=F32).astype(BF16)
            for j in range(wide // 128):
                out_proj.at[lo // 128 + j].reshape(R * K, 128)[b * 256:(b + 1) * 256, :] = (
                    out[:, j * 128:(j + 1) * 128])
    with jax.named_scope("drain"):
        for pred, c in sends:
            if pred is None:
                c.wait_send()
            else:
                pl.when(pred)(c.wait_send)


def body_fast(M, N, hidden, mix_weight, comp_proj, vocab_weight, log_normalizer, targets, loss_grad):
    T, D = hidden.shape
    K, E = mix_weight.shape
    V = vocab_weight.shape[1]
    R = D // M
    J = E // 128
    half = N // 2
    Z = M // 2
    vm = pltpu.VMEM
    dma = pltpu.SemaphoreType.DMA
    scratch = [
        vm((J, D, K, 128), BF16), vm((K, D, E), BF16), vm((Z, 2, T, D // 2), BF16), vm((D, V), BF16),
        vm((N, E, V), BF16), vm((N, V, E), BF16), vm((K, E), BF16), vm((K, T), F32), vm((1, T), jnp.int32), vm((1, T), F32),
        vm((N, K * T, E), BF16), vm((Z, K * T, E), BF16), vm((N, K, E), BF16), vm((2, R, Z * T), BF16),
        vm((K * T, V), F32), vm((K * T, V), BF16), vm((Z, N, K, T, V), BF16), vm((N, 8, T), F32), vm((Z, 8, T), F32), vm((K, Z * T, E), BF16),
        vm((D, V), BF16), vm((Z, R, V), BF16),
        vm((R, V), F32), vm((Z, R, V), BF16), vm((Z, R, V), BF16),
        vm((N, T, E), BF16), vm((N, T, E), BF16),
        vm((T, E), F32), vm((K, R, E), F32), vm((K, R, E), BF16), vm((K, R, E), BF16),
        vm((K, T), F32),
        dma((7,)), dma((4, J)),
        dma((half, K)), dma((half, K)), dma((N, K)), dma((N,)), dma((N,)),
        dma((2, Z, 2)), dma((Z, 2)), dma((Z, 2)), dma((Z, 2)),
        dma((half, 2)), dma((N,)), dma((1,)), dma((1,)),
        dma((half,)), dma((half,)), dma((half, 2)), dma((half, 2)), dma((N,)), dma((N,)),
        dma((2, Z, K)), dma((half, Z, K)), dma((half, Z, K)), dma((Z, N, K)),
        dma((Z,)), dma((Z,)), dma((Z,)), dma((Z,)), dma((N,)), dma((N,)),
        dma((K + 1,)), dma((K + 1,)), dma((Z,)), dma((Z,)),
    ]
    spec = pl.BlockSpec(memory_space=pltpu.VMEM)
    hbm = pl.BlockSpec(memory_space=pltpu.MemorySpace.HBM)
    hid, proj, voc = pl.pallas_call(
        functools.partial(fast_kernel, M, N),
        out_shape=(
            jax.ShapeDtypeStruct((T, E), BF16),
            jax.ShapeDtypeStruct((J, R, K, 128), BF16),
            jax.ShapeDtypeStruct((R, V), BF16),
        ),
        in_specs=[hbm] * 7,
        out_specs=(spec, spec, spec),
        scratch_shapes=scratch,
        compiler_params=pltpu.CompilerParams(
            collective_id=0, has_side_effects=True, vmem_limit_bytes=47 * 1024 * 1024
        ),
    )(*[
        pltpu.with_memory_space_constraint(x, pltpu.MemorySpace.HBM)
        for x in (hidden, mix_weight, comp_proj, vocab_weight, log_normalizer, targets[None, :], loss_grad[None, :])
    ])
    return pl.pallas_call(
        store_kernel,
        out_shape=(
            jax.ShapeDtypeStruct((T, E), BF16),
            jax.ShapeDtypeStruct((R, K, E), BF16),
            jax.ShapeDtypeStruct((R, V), BF16),
        ),
        in_specs=[spec] * 3,
        out_specs=(hbm, hbm, hbm),
        scratch_shapes=[dma((J + 2,))],
        compiler_params=pltpu.CompilerParams(vmem_limit_bytes=4 * 1024 * 1024),
    )(hid, proj, voc)


def store_kernel(hid, proj, voc, out_hid, out_proj, out_voc, sem):
    J = proj.shape[0]
    copies = [pltpu.make_async_copy(hid, out_hid, sem.at[J]), pltpu.make_async_copy(voc, out_voc, sem.at[J + 1])]
    for j in range(J):
        copies.append(pltpu.make_async_copy(proj.at[j], out_proj.at[:, :, pl.ds(j * 128, 128)], sem.at[j]))
    for c in copies:
        c.start()
    for c in copies:
        c.wait()


def body(M, N, *args):
    hidden, mix_weight, comp_proj, vocab_weight = args[:4]
    T, D = hidden.shape
    K, E = mix_weight.shape
    V = vocab_weight.shape[1]
    gathered = 2 * (M // 2) * T * (K * N * V + D + 2 * K * E)
    shapes = K == 4 and M == 8 and N == 4 and E % 128 == 0 and (D // M) % (256 // K) == 0
    if shapes and gathered + 4 * K * D * E <= 28 * 1024 * 1024:
        return body_fast(M, N, *args)
    return body_base(M, N, *args)


def solution(mesh):
    in_specs = (
        P("tok", None),
        P(None, "voc"),
        P(None, None, "voc"),
        P(None, "voc"),
        P(None, "tok"),
        P("tok"),
        P("tok"),
    )
    out_specs = (P("tok", "voc"), P("tok", None, "voc"), P("tok", "voc"))
    return jax.shard_map(
        functools.partial(body, mesh.shape["tok"], mesh.shape["voc"]),
        mesh=mesh, in_specs=in_specs, out_specs=out_specs, check_vma=False,
    )
```

```python
import functools

import jax
import jax.numpy as jnp
from jax import lax
from jax.experimental import pallas as pl
from jax.experimental.pallas import tpu as pltpu
from jax.sharding import PartitionSpec as P

MESH = pl.DeviceIdType.MESH
F32 = jnp.float32
BF16 = jnp.bfloat16
NT = (((1,), (1,)), ((), ()))
TN = (((0,), (0,)), ((), ()))


def column(row, lanes):
    wide = jnp.broadcast_to(row, (128, row.shape[1])).T
    return jnp.concatenate([wide] * (lanes // 128), axis=1)


def kernel(
    M, N,
    hidden, mix, proj_hbm, vw, logz, targets, loss,
    out_hidden, out_proj, out_vocab,
    w, ctx, mix_all, hblk, hrow, htr, logit, lg, tgt,
    cgs, cgr, cgx, xr, own_cg, vgb, vgy, vsum, vout, vin, pg, hss, hsr, own_hs, acc, psend, precv, mgrad,
    w_sem, ctx_s, ctx_f, ctx_r, mix_s, mix_r, hid_s, hid_r, tgt_s, tgt_r,
    cgp_s, cgp_r, cgx_s, cgx_r, vy_s, vy_r, vz_s, vz_r, hs_s, hs_r, ag_s, ag_r, pp_s, pp_r,
):
    K, D, E = w.shape
    T = hidden.shape[0]
    V = vw.shape[1]
    R = D // M
    half = N // 2
    Z = M // 2
    me_t = lax.axis_index("tok")
    me_v = lax.axis_index("voc")
    chip = me_v // 2
    core = me_v % 2
    partner = me_v + 1 - 2 * core
    z = me_t // 2
    y = me_t % 2
    ypart = me_t + 1 - 2 * y
    sends = []

    def remote(src, dst, ss, rs, dev):
        return pltpu.make_async_remote_copy(
            src_ref=src, dst_ref=dst, send_sem=ss, recv_sem=rs,
            device_id=dev, device_id_type=MESH,
        )

    def send(src, dst, ss, rs, dev):
        c = remote(src, dst, ss, rs, dev)
        c.start()
        sends.append((None, c))

    def arrived(ref, rs, ss):
        remote(ref, ref, ss, rs, {"voc": partner}).wait_recv()

    for k in range(K):
        pltpu.make_async_copy(proj_hbm.at[k], w.at[k], w_sem.at[k]).start()
    for j in range(M):
        hblk[j // 2, j % 2] = hidden[:, j * R:(j + 1) * R]

    bar = pltpu.get_barrier_semaphore()
    for d in range(1, M):
        pl.semaphore_signal(bar, inc=1, device_id={"tok": lax.rem(me_t + d, M)}, device_id_type=MESH)
    for d in range(1, N):
        pl.semaphore_signal(bar, inc=1, device_id={"voc": lax.rem(me_v + d, N)}, device_id_type=MESH)
    pl.semaphore_wait(bar, M + N - 2)

    for d in range(1, N):
        send(mix, mix_all.at[d], mix_s.at[d], mix_r.at[d], {"voc": lax.rem(me_v + d, N)})
    mix_all[0] = mix[...]
    for d in range(1, Z):
        zz = lax.rem(z + d, Z)
        send(hblk.at[zz], hrow.at[:, pl.ds(z * T, T)], hid_s.at[d], hid_r.at[d],
             {"tok": zz * 2 + y})
    hrow[:, rows_of(z, T), :] = hblk[z]

    for k in range(K):
        pltpu.make_async_copy(proj_hbm.at[k], w.at[k], w_sem.at[k]).wait()
        ctx[me_v, k * T:(k + 1) * T, :] = jnp.tanh(
            jnp.dot(hidden[...], w[k], preferred_element_type=F32)
        ).astype(BF16)
        piece = ctx.at[me_v, pl.ds(k * T, T)]
        for i in range(1, half):
            send(piece, piece, ctx_s.at[i, k], ctx_r.at[me_v, k],
                 {"voc": lax.rem(chip + i, half) * 2 + core})
        send(piece, piece, ctx_s.at[0, k], ctx_r.at[me_v, k], {"voc": partner})

    def add_logits(s, first=False):
        part = jnp.dot(ctx[s], vw[pl.ds(pl.multiple_of(s * E, E), E), :],
                       preferred_element_type=F32)
        logit[...] = part if first else logit[...] + part

    add_logits(me_v, True)
    for k in range(K):
        arrived(ctx.at[partner, pl.ds(k * T, T)], ctx_r.at[partner, k], ctx_s.at[0, k])
    add_logits(partner)

    tcol = column(targets[...].astype(F32), V)
    ids = (me_v * V + lax.broadcasted_iota(jnp.int32, (T, V), 1)).astype(F32)
    onehot = (tcol == ids).astype(F32)
    for d in range(1, N):
        arrived(mix_all.at[d], mix_r.at[d], mix_s.at[d])
    mixing = jnp.zeros((K, T), F32)
    for d in range(N):
        s = lax.rem(me_v - d + N, N)
        mixing = mixing + lax.dot_general(
            mix_all[d], hidden[:, pl.ds(pl.multiple_of(s * E, E), E)], NT,
            preferred_element_type=F32)
    exp_mix = jnp.exp(mixing)
    weights = exp_mix / jnp.sum(exp_mix, axis=0, keepdims=True)

    for i in range(1, half):
        s = lax.rem(chip - i + half, half) * 2 + core
        for k in range(K):
            piece = ctx.at[s, pl.ds(k * T, T)]
            arrived(piece, ctx_r.at[s, k], ctx_s.at[i, k])
            send(piece, piece, ctx_f.at[i, k], ctx_r.at[s, k], {"voc": partner})
        add_logits(s)
    for i in range(1, half):
        s = lax.rem(chip - i + half, half) * 2 + 1 - core
        for k in range(K):
            arrived(ctx.at[s, pl.ds(k * T, T)], ctx_r.at[s, k], ctx_s.at[i, k])
        add_logits(s)

    lane = lax.broadcasted_iota(jnp.int32, (T, 128), 1)
    table = jnp.zeros((T, 128), F32)
    for k in range(K):
        part = jnp.sum(logit[k * T:(k + 1) * T, :] * onehot, axis=1, keepdims=True)
        table = jnp.where(lane == k, part, table)
    tgt[0] = table.T[0:8, :]
    for d in range(1, N):
        send(tgt.at[0], tgt.at[d], tgt_s.at[d], tgt_r.at[d], {"voc": lax.rem(me_v + d, N)})
    for k in range(K):
        rows = slice(k * T, (k + 1) * T)
        logit[rows, :] = jnp.exp(logit[rows, :] - column(logz[k:k + 1, :], V)) - onehot
    for d in range(1, N):
        arrived(tgt.at[d], tgt_r.at[d], tgt_s.at[d])
    target = tgt[0]
    for d in range(1, N):
        target = target + tgt[d]
    likely = jnp.exp(target[0:K, :] - logz[...])
    joint = weights * likely
    posterior = joint / jnp.sum(joint, axis=0, keepdims=True)
    factor = loss[...] * posterior
    mgrad[...] = loss[...] * (weights - posterior)
    for k in range(K):
        rows = slice(k * T, (k + 1) * T)
        lg[rows, :] = (column(factor[k:k + 1, :], V) * logit[rows, :]).astype(BF16)

    def cg_part(s, k):
        return lax.dot_general(
            lg[k * T:(k + 1) * T, :], vw[pl.ds(pl.multiple_of(s * E, E), E), :], NT,
            preferred_element_type=F32)

    for i in list(range(1, half)) + [0]:
        s = lax.rem(chip + i, half) * 2
        for k in range(K):
            cgs[i, k] = cg_part(s + 1 - core, k).astype(BF16)
            send(cgs.at[i, k], cgr.at[i, k], cgp_s.at[i, k], cgp_r.at[i, k], {"voc": partner})
        for k in range(K):
            part = cg_part(s + core, k)
            if i == 0:
                own_cg[k] = part
            else:
                arrived(cgr.at[i, k], cgp_r.at[i, k], cgp_s.at[i, k])
                cgx[i, k] = (part + cgr[i, k].astype(F32)).astype(BF16)
                send(cgx.at[i, k], xr.at[i, k], cgx_s.at[i, k], cgx_r.at[i, k], {"voc": s + core})

    for s in range(N):
        vgb[s * E:(s + 1) * E, :] = lax.dot_general(
            ctx[s], lg[...], TN, preferred_element_type=F32).astype(BF16)
    for zz in range(Z):
        send(vgb.at[pl.ds((zz * 2 + 1 - y) * R, R)], vgy.at[zz], vy_s.at[zz], vy_r.at[zz],
             {"tok": ypart})

    for d in range(1, Z):
        src = lax.rem(z - d + Z, Z)
        arrived(hrow.at[:, pl.ds(src * T, T)], hid_r.at[d], hid_s.at[d])
    for b in range(2):
        htr[b] = hrow[b].T

    pieces = [(k, 0, E) for k in range(K)]
    if E % 256 == 0:
        pieces[-1:] = [(K - 1, 0, E // 2), (K - 1, E // 2, E // 2)]

    def relay(t, p, way, pred):
        k, lo, wide = pieces[p]
        piece = pg.at[k, rows_of(t, T), pl.ds(lo, wide)]
        c = remote(piece, piece, ag_s.at[way, t, p], ag_r.at[t, p],
                   {"tok": me_t + 2 - 4 * way})
        pl.when(pred)(c.start)
        sends.append((pred, c))

    has_r = z + 1 < Z
    has_l = z >= 1
    for k in range(K):
        total = own_cg[k]
        arrived(cgr.at[0, k], cgp_r.at[0, k], cgp_s.at[0, k])
        total = total + cgr[0, k].astype(F32)
        for i in range(1, half):
            arrived(xr.at[i, k], cgx_r.at[i, k], cgx_s.at[i, k])
            total = total + xr[i, k].astype(F32)
        c = ctx[me_v, k * T:(k + 1) * T, :].astype(F32)
        pg[k, rows_of(z, T), :] = (total * (1.0 - c * c)).astype(BF16)
        if Z > 1:
            for p in range(len(pieces)):
                if pieces[p][0] == k:
                    relay(z, p, 0, has_r)
                    relay(z, p, 1, has_l)

    def hid_part(s):
        total = jnp.zeros((T, E), F32)
        for k in range(K):
            total = total + lax.dot_general(
                pg[k, rows_of(z, T), :], w[k, pl.ds(pl.multiple_of(s * E, E), E), :], NT,
                preferred_element_type=F32)
        return total

    def hid_send(d):
        s = lax.rem(me_v + d, N)
        if d == 0:
            own_hs[...] = hid_part(s)
        else:
            hss[d] = hid_part(s).astype(BF16)
            send(hss.at[d], hsr.at[d], hs_s.at[d], hs_r.at[d], {"voc": s})

    hid_order = list(range(1, N)) + [0]
    hid_per = -(-N // (len(pieces) - 1))

    def pair_sums():
        for zz in range(Z):
            arrived(vgy.at[zz], vy_r.at[zz], vy_s.at[zz])
            vsum[zz] = vgb[rows_of(zz * 2 + y, R), :].astype(F32) + vgy[zz].astype(F32)

    def hop(h):
        for way, at, ends in ((0, h, range(h + 1, Z)), (1, Z - 1 - h, range(Z - 1 - h))):
            copies = [
                remote(vout.at[way, e], vin.at[way, e], vz_s.at[way, e], vz_r.at[way, e],
                       {"tok": me_t + 2 - 4 * way})
                for e in ends
            ]

            @pl.when(z == at)
            def _(way=way, ends=ends, copies=copies):
                for e, c in zip(ends, copies):
                    part = vsum[e]
                    if h > 0:
                        arrived(vin.at[way, e], vz_r.at[way, e], vz_s.at[way, e])
                        part = part + vin[way, e].astype(F32)
                    vout[way, e] = part.astype(BF16)
                    c.start()
            for c in copies:
                sends.append((z == at, c))

    if Z == 1:
        for e in hid_order:
            hid_send(e)
    per = -(-(Z - 1) // (len(pieces) - 1))
    for p, (k, lo, wide) in enumerate(pieces):
        lanes = slice(lo, lo + wide)
        for d in range(1, Z):
            for there, t, way, more in (
                (z >= d, z - d, 0, has_r), (z + d < Z, z + d, 1, has_l),
            ):
                def _(t=t):
                    arrived(pg.at[k, rows_of(t, T), pl.ds(lo, wide)], ag_r.at[t, p], ag_s.at[0, t, p])
                pl.when(there)(_)
                if d < Z - 1:
                    relay(t, p, way, there & more)
            if d == 1:
                for e in hid_order[p * hid_per:(p + 1) * hid_per]:
                    hid_send(e)
        psend[k, :, lanes] = jnp.dot(
            htr[1 - y], pg[k, :, lanes], preferred_element_type=F32).astype(BF16)
        send(psend.at[k, :, pl.ds(lo, wide)], precv.at[k, :, pl.ds(lo, wide)],
             pp_s.at[p], pp_r.at[p], {"tok": ypart})
        acc[k, :, lanes] = jnp.dot(htr[y], pg[k, :, lanes], preferred_element_type=F32)
        if p == 0:
            pair_sums()
        for h in range(p * per, min((p + 1) * per, Z - 1)):
            hop(h)

    acc_v = vsum.at[z]
    for way, pred in ((0, has_l), (1, has_r)):
        @pl.when(pred)
        def _(way=way):
            arrived(vin.at[way, z], vz_r.at[way, z], vz_s.at[way, z])
            acc_v[...] += vin[way, z].astype(F32)
    out_vocab[...] = acc_v[...].astype(BF16)
    htot = own_hs[...]
    for d in range(1, N):
        arrived(hsr.at[d], hs_r.at[d], hs_s.at[d])
        htot = htot + hsr[d].astype(F32)
    mixf = mix[...].astype(F32)
    for k in range(K):
        htot = htot + column(mgrad[k:k + 1, :], E) * mixf[k:k + 1, :]
    out_hidden[...] = htot.astype(BF16)

    for p, (k, lo, wide) in enumerate(pieces):
        lanes = slice(lo, lo + wide)
        arrived(precv.at[k, :, pl.ds(lo, wide)], pp_r.at[p], pp_s.at[p])
        out_proj[k, :, lanes] = (acc[k, :, lanes] + precv[k, :, lanes].astype(F32)).astype(BF16)
    for pred, c in sends:
        if pred is None:
            c.wait_send()
        else:
            pl.when(pred)(c.wait_send)


def rows_of(block, size):
    return pl.ds(pl.multiple_of(block * size, size), size)


def body_base(M, N, hidden, mix_weight, comp_proj, vocab_weight, log_normalizer, targets, loss_grad):
    T, D = hidden.shape
    K, E = mix_weight.shape
    V = vocab_weight.shape[1]
    R = D // M
    half = N // 2
    Z = M // 2
    w = jnp.transpose(comp_proj, (1, 0, 2))
    vm = pltpu.VMEM
    dma = pltpu.SemaphoreType.DMA
    scratch = [
        vm((K, D, E), BF16), vm((N, K * T, E), BF16), vm((N, K, E), BF16),
        vm((Z, 2, T, R), BF16), vm((2, Z * T, R), BF16), vm((2, R, Z * T), BF16), vm((K * T, V), F32), vm((K * T, V), BF16),
        vm((N, 8, T), F32),
        vm((half, K, T, E), BF16), vm((half, K, T, E), BF16),
        vm((half, K, T, E), BF16), vm((half, K, T, E), BF16),
        vm((K, T, E), F32), vm((D, V), BF16), vm((Z, R, V), BF16),
        vm((Z, R, V), F32), vm((2, Z, R, V), BF16), vm((2, Z, R, V), BF16),
        vm((K, Z * T, E), BF16), vm((N, T, E), BF16), vm((N, T, E), BF16),
        vm((T, E), F32), vm((K, R, E), F32), vm((K, R, E), BF16), vm((K, R, E), BF16),
        vm((K, T), F32),
        dma((K,)), dma((half, K)), dma((half, K)), dma((N, K)), dma((N,)), dma((N,)),
        dma((Z,)), dma((Z,)), dma((N,)), dma((N,)),
        dma((half, K)), dma((half, K)), dma((half, K)), dma((half, K)),
        dma((Z,)), dma((Z,)), dma((2, Z)), dma((2, Z)), dma((N,)), dma((N,)),
        dma((2, Z, K + 1)), dma((Z, K + 1)), dma((K + 1,)), dma((K + 1,)),
    ]
    spec = pl.BlockSpec(memory_space=pltpu.VMEM)
    hidden_grad, proj_grad, vocab_grad = pl.pallas_call(
        functools.partial(kernel, M, N),
        out_shape=(
            jax.ShapeDtypeStruct((T, E), BF16),
            jax.ShapeDtypeStruct((K, R, E), BF16),
            jax.ShapeDtypeStruct((R, V), BF16),
        ),
        in_specs=[spec, spec, pl.BlockSpec(memory_space=pltpu.MemorySpace.HBM)] + [spec] * 4,
        out_specs=(spec, spec, spec),
        scratch_shapes=scratch,
        compiler_params=pltpu.CompilerParams(
            collective_id=0, has_side_effects=True, vmem_limit_bytes=48 * 1024 * 1024
        ),
    )(hidden, mix_weight, w, vocab_weight, log_normalizer, targets[None, :], loss_grad[None, :])
    return hidden_grad, jnp.transpose(proj_grad, (1, 0, 2)), vocab_grad


ORDER = (
    (0, 0), (1, 0), (2, 0), (0, 1), (2, 1), (12,), (0, 2), (1, 1), (0, 3), (1, 3), (10, 2), (8,), (9,),
    (1, 2), (3, 0, 1), (3, 0, 2), (3, 0, 3), (11, 3, 0), (3, 1, 1), (2, 3), (4, 0, 3), (4, 0, 1),
    (3, 1, 2), (11, 3, 1), (2, 2), (10, 3), (5, 0, 0), (4, 0, 2), (4, 1, 1), (5, 2, 0), (13,), (5, 0, 1),
    (4, 3, 1), (3, 1, 3), (3, 3, 2), (3, 3, 1), (6, 0, 1), (5, 0, 3), (6, 0, 0), (5, 0, 2), (4, 1, 2),
    (5, 1, 0), (6, 0, 3), (6, 0, 2), (7, 0), (4, 1, 3), (4, 2, 1), (3, 3, 3), (5, 1, 1), (4, 3, 2),
    (3, 2, 1), (5, 1, 2), (5, 1, 3), (3, 2, 2), (5, 3, 0), (6, 1, 0), (6, 1, 1), (5, 3, 1), (6, 1, 2),
    (3, 2, 3), (4, 3, 3), (6, 1, 3), (7, 1), (6, 2, 0), (4, 2, 2), (6, 3, 1), (6, 3, 0), (5, 3, 2), (15,),
    (4, 2, 3), (5, 3, 3), (6, 3, 2), (5, 2, 1), (5, 2, 2), (6, 3, 3), (7, 3), (5, 2, 3), (6, 2, 2),
    (6, 2, 1), (6, 2, 3), (7, 2), (14, 0), (14, 1), (14, 2), (14, 3),
)


def scoped(fn):
    def run(*args, **kw):
        tag = "_".join(str(a) for a in args if isinstance(a, int))
        with jax.named_scope(fn.__name__ + "_" + tag):
            return fn(*args, **kw)
    return run


def mix_rows(K, flip=False):
    B = 256 // K
    r = lax.broadcasted_iota(jnp.int32, (256, 256), 1 if flip else 0)
    c = lax.broadcasted_iota(jnp.int32, (256, 256), 0 if flip else 1)
    return (c == K * (r % B) + r // B).astype(F32).astype(BF16)


def fast_kernel(
    M, N,
    hid_hbm, mix_hbm, proj_hbm, vw_hbm, logz_hbm, tg_hbm, loss_hbm,
    out_hidden, out_proj, out_vocab,
    raw, w, hida, vw, vwe, vwt, mix, logz, targets, loss,
    ctx, ctxz, mix_all, htr, logit, lg, lgall, tgt, scale, pg,
    vgb, vgy, vsum, vout, vin, hss, hsr, own_hs, acc, psend, precv, mgrad,
    l_sem, w_sem, ctx_s, ctx_f, ctx_r, mix_s, mix_r, hz_s, hz_r, hp_s, hp_r,
    vx_s, vx_r, vp_s, vp_r, vwz_s, vwz_r, vwy_s, vwy_r, tgt_s, tgt_r,
    lz_s, lx_s, lp_s, lg_r, vy_s, vy_r, vz_s, vz_r, hs_s, hs_r, pp_s, pp_r, sc_s, sc_r, le_s,
):
    K, D, E = w.shape
    T = hida.shape[2]
    H = D // 2
    V = vw.shape[1]
    R = D // M
    J = E // 128
    half = N // 2
    Z = M // 2
    B = 256 // K
    me_t = lax.axis_index("tok")
    me_v = lax.axis_index("voc")
    chip = me_v // 2
    core = me_v % 2
    partner = me_v + 1 - 2 * core
    z = me_t // 2
    y = me_t % 2
    ypart = me_t + 1 - 2 * y
    has_r = z + 1 < Z
    has_l = z >= 1
    sends = []

    def remote(src, dst, ss, rs, dev):
        return pltpu.make_async_remote_copy(
            src_ref=src, dst_ref=dst, send_sem=ss, recv_sem=rs,
            device_id=dev, device_id_type=MESH,
        )

    def send(src, dst, ss, rs, dev, pred=None):
        c = remote(src, dst, ss, rs, dev)
        if pred is None:
            c.start()
        else:
            pl.when(pred)(c.start)
        sends.append((pred, c))

    def arrived(ref, rs, ss):
        remote(ref, ref, ss, rs, {"voc": partner}).wait_recv()

    def mate(j):
        if j == 0:
            return z
        near = jnp.minimum(z, Z - 1 - z)
        d = (j + 1) // 2
        both = z + d if j % 2 == 1 else z - d
        return jnp.where(j <= 2 * near, both, jnp.where(2 * z < Z, j, Z - 1 - j))

    def onward(zz):
        right = zz < z
        there = (right & has_r) | (jnp.logical_not(right) & has_l)
        return there, me_t + jnp.where(right, 2, -2)

    chunks = 4
    n = D // chunks

    def w_copy(c, j):
        return pltpu.make_async_copy(
            proj_hbm.at[pl.ds(c * n, n), :, pl.ds(j * 128, 128)],
            raw.at[j, pl.ds(c * n, n)], w_sem.at[c, j])

    loads = [
        pltpu.make_async_copy(hid_hbm.at[:, pl.ds(0, H)], hida.at[z, 0], l_sem.at[0]),
        pltpu.make_async_copy(hid_hbm.at[:, pl.ds(H, H)], hida.at[z, 1], l_sem.at[1]),
        pltpu.make_async_copy(vw_hbm, vw, l_sem.at[2]),
        pltpu.make_async_copy(mix_hbm, mix, l_sem.at[3]),
        pltpu.make_async_copy(logz_hbm, logz, l_sem.at[4]),
        pltpu.make_async_copy(tg_hbm, targets, l_sem.at[5]),
        pltpu.make_async_copy(loss_hbm, loss, l_sem.at[6]),
    ]
    loads[0].start()
    loads[1].start()
    loads[2].start()
    for c in loads[3:]:
        c.start()
    for j in range(J):
        w_copy(0, j).start()

    bar = pltpu.get_barrier_semaphore()
    for d in range(1, M):
        pl.semaphore_signal(bar, inc=1, device_id={"tok": lax.rem(me_t + d, M)}, device_id_type=MESH)
    for d in range(1, N):
        pl.semaphore_signal(bar, inc=1, device_id={"voc": lax.rem(me_v + d, N)}, device_id_type=MESH)

    perm = mix_rows(K)

    @scoped
    def unmix(c):
        for j in range(J):
            w_copy(c, j).wait()
        for b in range(c * n // B, (c + 1) * n // B):
            x = jnp.concatenate(
                [raw.at[j].reshape(D * K, 128)[b * 256:(b + 1) * 256, :] for j in range(J)], axis=1)
            rows = jnp.dot(perm, x, preferred_element_type=F32).astype(BF16)
            for k in range(K):
                w[k, b * B:(b + 1) * B, :] = rows[k * B:(k + 1) * B]

    with jax.named_scope("loads"):
        for c in loads[:3]:
            c.wait()
    for c in range(1, chunks):
        for j in range(J):
            w_copy(c, j).start()
    with jax.named_scope("barrier"):
        pl.semaphore_wait(bar, M + N - 2)

    g = z % 2
    zpair = me_t + 2 - 4 * g

    def vw_rows(yy, part):
        return pl.ds(pl.multiple_of(yy * (E // 2) + part * (E // 4), E // 4), E // 4)

    def vw_send():
        for i in range(1, half):
            for c in range(2):
                v = lax.rem(chip + i, half) * 2 + c
                rows = vw_rows(y, g)
                send(vw.at[pl.ds(pl.multiple_of(v * E + rows.start, E // 4), rows.size)],
                     vwe.at[me_v, rows], vx_s.at[i, c], vx_r.at[me_v], {"voc": v})

    @scoped
    def vw_pass():
        for i in range(1, half):
            ci = lax.rem(chip + i, half)
            for c in range(2):
                arrived(vwe.at[ci * 2 + c, vw_rows(y, g)], vx_r.at[ci * 2 + c], vx_s.at[i, c])
            piece = vwe.at[pl.ds(ci * 2, 2), vw_rows(y, g)]
            send(piece, piece, vwz_s.at[i], vwz_r.at[ci], {"tok": zpair})
            send(piece, piece, vwy_s.at[i, 0], vwy_r.at[ci, 0], {"tok": ypart})

    @scoped
    def vw_turn():
        for i in range(1, half):
            ci = lax.rem(chip + i, half)
            piece = vwe.at[pl.ds(ci * 2, 2), vw_rows(y, 1 - g)]
            arrived(piece, vwz_r.at[ci], vwz_s.at[i])
            send(piece, piece, vwy_s.at[i, 1], vwy_r.at[ci, 1], {"tok": ypart})

    def hid_piece(zz, side, p):
        return hida.at[zz, side, pl.ds(p * (T // 2), T // 2)]

    vw_send()
    for p in range(2):
        piece = hid_piece(z, core, p)
        send(piece, piece, hz_s.at[0, z, p], hz_r.at[z, p], {"tok": me_t + 2}, has_r)
        send(piece, piece, hz_s.at[1, z, p], hz_r.at[z, p], {"tok": me_t - 2}, has_l)
    for c in loads[3:]:
        c.wait()
    for d in range(1, N):
        send(mix, mix_all.at[d], mix_s.at[d], mix_r.at[d], {"voc": lax.rem(me_v + d, N)})
    send(vw.at[rows_of(partner, E)], vwe.at[me_v], vp_s.at[0], vp_r.at[0], {"voc": partner})
    for c in range(chunks):
        unmix(c)

    def context(zz, k):
        both = jnp.dot(hida[zz, 0], w[k, 0:H, :], preferred_element_type=F32)
        both = both + jnp.dot(hida[zz, 1], w[k, H:D, :], preferred_element_type=F32)
        return jnp.tanh(both).astype(BF16)

    for k in range(K):
        with jax.named_scope("context"):
            ctx[me_v, k * T:(k + 1) * T, :] = context(z, k)
        if k == 1:
            vw_pass()
        piece = ctx.at[me_v, pl.ds(k * T, T)]
        for i in range(1, half):
            send(piece, piece, ctx_s.at[i, k], ctx_r.at[me_v, k],
                 {"voc": lax.rem(chip + i, half) * 2 + core})
        send(piece, piece, ctx_s.at[0, k], ctx_r.at[me_v, k], {"voc": partner})

    @scoped
    def add_logits(s, first=False):
        part = jnp.dot(ctx[s], vw[rows_of(s, E), :], preferred_element_type=F32)
        logit[...] = part if first else logit[...] + part

    @scoped
    def relay_hid(j, p, fwd):
        zz = mate(j)
        there, to = onward(zz)
        piece = hid_piece(zz, core, p)
        on = remote(piece, piece, hz_s.at[0, zz, p], hz_r.at[zz, p], {"tok": to})
        over = remote(piece, piece, hp_s.at[zz, p], hp_r.at[zz, p], {"voc": partner})

        @pl.when(there if fwd else jnp.logical_not(there))
        def _():
            arrived(piece, hz_r.at[zz, p], hz_s.at[0, zz, p])
            if fwd:
                on.start()
            over.start()
        if fwd:
            sends.append((there, on))
            sends.append((None, over))

    @scoped
    def ctx_mate(j, ks):
        zz = mate(j)
        if ks[0] == 0:
            for p in range(2):
                arrived(hid_piece(zz, 1 - core, p), hp_r.at[zz, p], hp_s.at[zz, p])
        for k in ks:
            ctxz[zz, k * T:(k + 1) * T, :] = context(zz, k)

    @scoped
    def ctx_pass(k):
        for i in range(1, half):
            s = lax.rem(chip - i + half, half) * 2 + core
            piece = ctx.at[s, pl.ds(k * T, T)]
            arrived(piece, ctx_r.at[s, k], ctx_s.at[i, k])
            send(piece, piece, ctx_f.at[i, k], ctx_r.at[s, k], {"voc": partner})

    add_logits(me_v, True)
    for j in range(1, min(Z, 3)):
        relay_hid(j, 0, True)
    for k in range(K):
        arrived(ctx.at[partner, pl.ds(k * T, T)], ctx_r.at[partner, k], ctx_s.at[0, k])
    add_logits(partner)

    tcol = column(targets[...].astype(F32), V)
    ids = (me_v * V + lax.broadcasted_iota(jnp.int32, (T, V), 1)).astype(F32)
    onehot = (tcol == ids).astype(F32)
    mix_all[0] = mix[...]
    for d in range(1, N):
        arrived(mix_all.at[d], mix_r.at[d], mix_s.at[d])
    mixing = jnp.zeros((K, T), F32)
    for d in range(N):
        s = lax.rem(me_v - d + N, N)
        mixing = mixing + lax.dot_general(
            mix_all[d],
            hida[z, s // half, :, pl.ds(pl.multiple_of((s % half) * E, E), E)], NT,
            preferred_element_type=F32)
    exp_mix = jnp.exp(mixing)
    weights = exp_mix / jnp.sum(exp_mix, axis=0, keepdims=True)

    for j in range(1, min(Z, 3)):
        relay_hid(j, 1, True)
    ctx_pass(0)
    if Z > 1:
        relay_hid(1, 0, False)
        relay_hid(1, 1, False)
    ctx_pass(1)
    vw_turn()
    if Z > 1:
        ctx_mate(1, range(K))
    for j in range(3, Z):
        relay_hid(j, 0, True)
    ctx_pass(2)
    for j in range(3, Z):
        relay_hid(j, 1, True)
    if Z > 2:
        relay_hid(2, 0, False)
    for k in range(3, K):
        ctx_pass(k)
    if Z > 2:
        relay_hid(2, 1, False)
    for i in range(1, half):
        add_logits(lax.rem(chip - i + half, half) * 2 + core)
    for i in range(1, half):
        s = lax.rem(chip - i + half, half) * 2 + 1 - core
        for k in range(K):
            arrived(ctx.at[s, pl.ds(k * T, T)], ctx_r.at[s, k], ctx_s.at[i, k])
        add_logits(s)

    lane = lax.broadcasted_iota(jnp.int32, (T, 128), 1)
    table = jnp.zeros((T, 128), F32)
    for k in range(K):
        part = jnp.sum(logit[k * T:(k + 1) * T, :] * onehot, axis=1, keepdims=True)
        table = jnp.where(lane == k, part, table)
    tgt[0] = table.T[0:8, :]
    for d in range(1, N):
        send(tgt.at[0], tgt.at[d], tgt_s.at[d], tgt_r.at[d], {"voc": lax.rem(me_v + d, N)})
    @scoped
    def scales():
        for d in range(1, N):
            arrived(tgt.at[d], tgt_r.at[d], tgt_s.at[d])
        target = tgt[0]
        for d in range(1, N):
            target = target + tgt[d]
        likely = jnp.exp(target[0:K, :] - logz[...])
        joint = weights * likely
        posterior = joint / jnp.sum(joint, axis=0, keepdims=True)
        scale[z, 0:K, :] = loss[...] * posterior
        mgrad[...] = loss[...] * (weights - posterior)
        for d in range(1, Z):
            send(scale.at[z], scale.at[z], sc_s.at[d], sc_r.at[z], {"tok": lax.rem(me_t + 2 * d, M)})

    def shares(zz, k):
        piece = lgall.at[zz, me_v, k]
        return [
            remote(piece, piece, lx_s.at[i, zz, k], lg_r.at[zz, me_v, k],
                   {"voc": lax.rem(chip + i, half) * 2 + core})
            for i in range(1, half)
        ] + [remote(piece, piece, lp_s.at[0, zz, k], lg_r.at[zz, me_v, k], {"voc": partner})]

    def share(zz, k):
        for c in shares(zz, k):
            c.start()
            sends.append((None, c))

    @scoped
    def own_out(k):
        rows = slice(k * T, (k + 1) * T)
        logit[rows, :] = jnp.exp(logit[rows, :] - column(logz[k:k + 1, :], V)) - onehot
        lgall[z, me_v, k] = logit[rows, :].astype(BF16)

    @scoped
    def own_share(k):
        share(z, k)

    @scoped
    def own_line(k):
        piece = lgall.at[z, me_v, k]
        send(piece, piece, lz_s.at[0, z, k], lg_r.at[z, me_v, k], {"tok": me_t + 2}, has_r)
        send(piece, piece, lz_s.at[1, z, k], lg_r.at[z, me_v, k], {"tok": me_t - 2}, has_l)
        if k == 0:
            send(piece, piece, le_s.at[0], lg_r.at[z, me_v, k], {"tok": me_t + M - 2}, z == 0)
            send(piece, piece, le_s.at[1], lg_r.at[z, me_v, k], {"tok": me_t - M + 2}, z == Z - 1)

    @scoped
    def relay_lg(k, j, fwd):
        zz = mate(j)
        there, to = onward(zz)
        if k == 0:
            end = to // 2
            there = there & (end - zz < Z - 1) & (zz - end < Z - 1)
        piece = lgall.at[zz, me_v, k]
        on = remote(piece, piece, lz_s.at[0, zz, k], lg_r.at[zz, me_v, k], {"tok": to})

        @pl.when(there if fwd else jnp.logical_not(there))
        def _():
            arrived(piece, lg_r.at[zz, me_v, k], lp_s.at[0, zz, k])
            if fwd:
                on.start()
            for c in shares(zz, k):
                c.start()
        if fwd:
            sends.append((there, on))
            for c in shares(zz, k):
                sends.append((None, c))

    @scoped
    def cross_lg(k, j):
        zz = mate(j)
        for i in range(1, half):
            s = lax.rem(chip - i + half, half) * 2 + core
            piece = lgall.at[zz, s, k]
            arrived(piece, lg_r.at[zz, s, k], lp_s.at[0, zz, k])
            send(piece, piece, lp_s.at[i, zz, k], lg_r.at[zz, s, k], {"voc": partner})

    @scoped
    def pre_grad(k, j):
        zz = mate(j)
        rows = slice(k * T, (k + 1) * T)
        for i in range(half):
            s = lax.rem(chip + i, half) * 2 + 1 - core
            arrived(lgall.at[zz, s, k], lg_r.at[zz, s, k], lp_s.at[0, zz, k])
        total = None
        for s in range(N):
            part = jnp.dot(lgall[zz, s, k], vwt[s], preferred_element_type=F32)
            total = part if total is None else total + part
        c = (ctx[me_v, rows, :] if j == 0 else ctxz[zz, rows, :]).astype(F32)
        if k == 0:
            if j > 0:
                arrived(scale.at[zz], sc_r.at[zz], sc_s.at[1])
        total = total * column(scale[zz, k:k + 1, :], E)
        pg[k, rows_of(zz, T), :] = (total * (1.0 - c * c)).astype(BF16)

    def hid_part(s):
        total = jnp.zeros((T, E), F32)
        for k in range(K):
            total = total + lax.dot_general(
                pg[k, rows_of(z, T), :], w[k, rows_of(s, E), :], NT,
                preferred_element_type=F32)
        return total

    @scoped
    def hid_send(d):
        s = lax.rem(me_v + d, N)
        if d == 0:
            own_hs[...] = hid_part(s)
        else:
            hss[d] = hid_part(s).astype(BF16)
            send(hss.at[d], hsr.at[d], hs_s.at[d], hs_r.at[d], {"voc": s})

    @scoped
    def pair_sums():
        for d in list(range(1, Z)) + [0]:
            zz = lax.rem(z + d, Z)
            arrived(vgy.at[zz], vy_r.at[zz], vy_s.at[zz])
            total = vgb[rows_of(zz * 2 + y, R), :].astype(F32) + vgy[zz].astype(F32)
            if d == 0:
                vsum[...] = total
            else:
                vout[zz] = total.astype(BF16)
                send(vout.at[zz], vin.at[z], vz_s.at[d], vz_r.at[z], {"tok": zz * 2 + y})

    pieces = [(k, 0, E) for k in range(K)]
    if E % 256 == 0:
        pieces[-1:] = [(K - 1, 0, E // 2), (K - 1, E // 2, E // 2)]

    @scoped
    def proj_part(k):
        for p, (kk, lo, wide) in enumerate(pieces):
            if kk == k:
                lanes = slice(lo, lo + wide)
                psend[k, :, lanes] = jnp.dot(
                    htr[1 - y], pg[k, :, lanes], preferred_element_type=F32).astype(BF16)
                send(psend.at[k, :, pl.ds(lo, wide)], precv.at[k, :, pl.ds(lo, wide)],
                     pp_s.at[p], pp_r.at[p], {"tok": ypart})
        acc[k] = jnp.dot(htr[y], pg[k], preferred_element_type=F32)

    @scoped
    def vocab_part():
        for k in range(K):
            rows = slice(k * T, (k + 1) * T)
            lg[rows, :] = (column(scale[z, k:k + 1, :], V) * logit[rows, :]).astype(BF16)
        for s in range(N):
            vgb[s * E:(s + 1) * E, :] = lax.dot_general(
                ctx[s], lg[...], TN, preferred_element_type=F32).astype(BF16)
            for zz in range(s * Z // N, (s + 1) * Z // N):
                send(vgb.at[pl.ds((zz * 2 + 1 - y) * R, R)], vgy.at[zz], vy_s.at[zz], vy_r.at[zz],
                     {"tok": ypart})

    @scoped
    def vw_done():
        vwe[me_v] = vw[rows_of(me_v, E), :]
        arrived(vwe.at[partner], vp_r.at[0], vp_s.at[0])
        for i in range(1, half):
            ci = lax.rem(chip + i, half)
            for p, part in enumerate((g, 1 - g)):
                arrived(vwe.at[pl.ds(ci * 2, 2), vw_rows(1 - y, part)], vwy_r.at[ci, p], vwy_s.at[i, p])
        for s in range(N):
            vwt[s] = vwe[s].T

    @scoped
    def turn():
        for b in range(2):
            col = (z * 2 + b) * R
            for zz in range(Z):
                htr[b, :, zz * T:(zz + 1) * T] = hida[
                    zz, col // H, :, pl.ds(pl.multiple_of(col % H, R), R)].T

    def relay_on(k, j):
        relay_lg(k, j, True)

    def relay_in(k, j):
        relay_lg(k, j, False)

    def mate_ctx(j):
        ctx_mate(j, range(K))

    def hid_in(j, p):
        relay_hid(j, p, False)

    steps = (own_out, own_share, own_line, relay_on, relay_in, cross_lg, pre_grad, proj_part,
             scales, vocab_part, mate_ctx, hid_in, vw_done, turn, hid_send, pair_sums)
    for step, *rest in ORDER:
        steps[step](*rest)

    vtot = vsum[...]
    for d in range(1, Z):
        zz = lax.rem(z + d, Z)
        arrived(vin.at[zz], vz_r.at[zz], vz_s.at[d])
        vtot = vtot + vin[zz].astype(F32)
    out_vocab[...] = vtot.astype(BF16)
    htot = own_hs[...]
    for d in range(1, N):
        arrived(hsr.at[d], hs_r.at[d], hs_s.at[d])
        htot = htot + hsr[d].astype(F32)
    mixf = mix[...].astype(F32)
    for k in range(K):
        htot = htot + column(mgrad[k:k + 1, :], E) * mixf[k:k + 1, :]
    out_hidden[...] = htot.astype(BF16)

    back = mix_rows(K, True)
    for p, (k, lo, wide) in enumerate(pieces):
        lanes = slice(lo, lo + wide)
        with jax.named_scope("precv"):
            arrived(precv.at[k, :, pl.ds(lo, wide)], pp_r.at[p], pp_s.at[p])
        psum = (acc[k, :, lanes] + precv[k, :, lanes].astype(F32)).astype(BF16)
        if k < K - 1:
            precv[k, :, lanes] = psum
            continue
        for b in range(R // B):
            rows = slice(b * B, (b + 1) * B)
            x = jnp.concatenate([precv[q, rows, lanes] for q in range(K - 1)] + [psum[rows]], axis=0)
            out = jnp.dot(back, x, preferred_element_type=F32).astype(BF16)
            for j in range(wide // 128):
                out_proj.at[lo // 128 + j].reshape(R * K, 128)[b * 256:(b + 1) * 256, :] = (
                    out[:, j * 128:(j + 1) * 128])
    with jax.named_scope("drain"):
        for pred, c in sends:
            if pred is None:
                c.wait_send()
            else:
                pl.when(pred)(c.wait_send)


def body_fast(M, N, hidden, mix_weight, comp_proj, vocab_weight, log_normalizer, targets, loss_grad):
    T, D = hidden.shape
    K, E = mix_weight.shape
    V = vocab_weight.shape[1]
    R = D // M
    J = E // 128
    half = N // 2
    Z = M // 2
    vm = pltpu.VMEM
    dma = pltpu.SemaphoreType.DMA
    scratch = [
        vm((J, D, K, 128), BF16), vm((K, D, E), BF16), vm((Z, 2, T, D // 2), BF16), vm((D, V), BF16),
        vm((N, E, V), BF16), vm((N, V, E), BF16), vm((K, E), BF16), vm((K, T), F32), vm((1, T), jnp.int32), vm((1, T), F32),
        vm((N, K * T, E), BF16), vm((Z, K * T, E), BF16), vm((N, K, E), BF16), vm((2, R, Z * T), BF16),
        vm((K * T, V), F32), vm((K * T, V), BF16), vm((Z, N, K, T, V), BF16), vm((N, 8, T), F32), vm((Z, 8, T), F32), vm((K, Z * T, E), BF16),
        vm((D, V), BF16), vm((Z, R, V), BF16),
        vm((R, V), F32), vm((Z, R, V), BF16), vm((Z, R, V), BF16),
        vm((N, T, E), BF16), vm((N, T, E), BF16),
        vm((T, E), F32), vm((K, R, E), F32), vm((K, R, E), BF16), vm((K, R, E), BF16),
        vm((K, T), F32),
        dma((7,)), dma((4, J)),
        dma((half, K)), dma((half, K)), dma((N, K)), dma((N,)), dma((N,)),
        dma((2, Z, 2)), dma((Z, 2)), dma((Z, 2)), dma((Z, 2)),
        dma((half, 2)), dma((N,)), dma((1,)), dma((1,)),
        dma((half,)), dma((half,)), dma((half, 2)), dma((half, 2)), dma((N,)), dma((N,)),
        dma((2, Z, K)), dma((half, Z, K)), dma((half, Z, K)), dma((Z, N, K)),
        dma((Z,)), dma((Z,)), dma((Z,)), dma((Z,)), dma((N,)), dma((N,)),
        dma((K + 1,)), dma((K + 1,)), dma((Z,)), dma((Z,)), dma((2,)),
    ]
    spec = pl.BlockSpec(memory_space=pltpu.VMEM)
    hbm = pl.BlockSpec(memory_space=pltpu.MemorySpace.HBM)
    hid, proj, voc = pl.pallas_call(
        functools.partial(fast_kernel, M, N),
        out_shape=(
            jax.ShapeDtypeStruct((T, E), BF16),
            jax.ShapeDtypeStruct((J, R, K, 128), BF16),
            jax.ShapeDtypeStruct((R, V), BF16),
        ),
        in_specs=[hbm] * 7,
        out_specs=(spec, spec, spec),
        scratch_shapes=scratch,
        compiler_params=pltpu.CompilerParams(
            collective_id=0, has_side_effects=True, vmem_limit_bytes=47 * 1024 * 1024
        ),
    )(*[
        pltpu.with_memory_space_constraint(x, pltpu.MemorySpace.HBM)
        for x in (hidden, mix_weight, comp_proj, vocab_weight, log_normalizer, targets[None, :], loss_grad[None, :])
    ])
    return pl.pallas_call(
        store_kernel,
        out_shape=(
            jax.ShapeDtypeStruct((T, E), BF16),
            jax.ShapeDtypeStruct((R, K, E), BF16),
            jax.ShapeDtypeStruct((R, V), BF16),
        ),
        in_specs=[spec] * 3,
        out_specs=(hbm, hbm, hbm),
        scratch_shapes=[dma((J + 2,))],
        compiler_params=pltpu.CompilerParams(vmem_limit_bytes=4 * 1024 * 1024),
    )(hid, proj, voc)


def store_kernel(hid, proj, voc, out_hid, out_proj, out_voc, sem):
    J = proj.shape[0]
    copies = [pltpu.make_async_copy(hid, out_hid, sem.at[J]), pltpu.make_async_copy(voc, out_voc, sem.at[J + 1])]
    for j in range(J):
        copies.append(pltpu.make_async_copy(proj.at[j], out_proj.at[:, :, pl.ds(j * 128, 128)], sem.at[j]))
    for c in copies:
        c.start()
    for c in copies:
        c.wait()


def body(M, N, *args):
    hidden, mix_weight, comp_proj, vocab_weight = args[:4]
    T, D = hidden.shape
    K, E = mix_weight.shape
    V = vocab_weight.shape[1]
    gathered = 2 * (M // 2) * T * (K * N * V + D + 2 * K * E)
    shapes = K == 4 and M == 8 and N == 4 and E % 128 == 0 and (D // M) % (256 // K) == 0
    if shapes and gathered + 4 * K * D * E <= 28 * 1024 * 1024:
        return body_fast(M, N, *args)
    return body_base(M, N, *args)


def solution(mesh):
    in_specs = (
        P("tok", None),
        P(None, "voc"),
        P(None, None, "voc"),
        P(None, "voc"),
        P(None, "tok"),
        P("tok"),
        P("tok"),
    )
    out_specs = (P("tok", "voc"), P("tok", None, "voc"), P("tok", "voc"))
    return jax.shard_map(
        functools.partial(body, mesh.shape["tok"], mesh.shape["voc"]),
        mesh=mesh, in_specs=in_specs, out_specs=out_specs, check_vma=False,
    )
```

```python
import functools
import math

import jax
import jax.numpy as jnp
from jax import lax
from jax.experimental import pallas as pl
from jax.experimental.pallas import tpu as pltpu
from jax.sharding import PartitionSpec as P

MESH = pl.DeviceIdType.MESH
F32 = jnp.float32
BF16 = jnp.bfloat16
NT = (((1,), (1,)), ((), ()))
TN = (((0,), (0,)), ((), ()))


def column(row, lanes):
    wide = jnp.broadcast_to(row, (128, row.shape[1])).T
    return jnp.concatenate([wide] * (lanes // 128), axis=1)


def kernel(
    M, N,
    hidden, mix, proj_hbm, vw, logz, targets, loss,
    out_hidden, out_proj, out_vocab,
    w, ctx, mix_all, hblk, hrow, htr, logit, lg, tgt,
    cgs, cgr, cgx, xr, own_cg, vgb, vgy, vsum, vout, vin, pg, hss, hsr, own_hs, acc, psend, precv, mgrad,
    w_sem, ctx_s, ctx_f, ctx_r, mix_s, mix_r, hid_s, hid_r, tgt_s, tgt_r,
    cgp_s, cgp_r, cgx_s, cgx_r, vy_s, vy_r, vz_s, vz_r, hs_s, hs_r, ag_s, ag_r, pp_s, pp_r,
):
    K, D, E = w.shape
    T = hidden.shape[0]
    V = vw.shape[1]
    R = D // M
    half = N // 2
    Z = M // 2
    me_t = lax.axis_index("tok")
    me_v = lax.axis_index("voc")
    chip = me_v // 2
    core = me_v % 2
    partner = me_v + 1 - 2 * core
    z = me_t // 2
    y = me_t % 2
    ypart = me_t + 1 - 2 * y
    sends = []

    def remote(src, dst, ss, rs, dev):
        return pltpu.make_async_remote_copy(
            src_ref=src, dst_ref=dst, send_sem=ss, recv_sem=rs,
            device_id=dev, device_id_type=MESH,
        )

    def send(src, dst, ss, rs, dev):
        c = remote(src, dst, ss, rs, dev)
        c.start()
        sends.append((None, c))

    def arrived(ref, rs, ss):
        remote(ref, ref, ss, rs, {"voc": partner}).wait_recv()

    for k in range(K):
        pltpu.make_async_copy(proj_hbm.at[k], w.at[k], w_sem.at[k]).start()
    for j in range(M):
        hblk[j // 2, j % 2] = hidden[:, j * R:(j + 1) * R]

    bar = pltpu.get_barrier_semaphore()
    for d in range(1, M):
        pl.semaphore_signal(bar, inc=1, device_id={"tok": lax.rem(me_t + d, M)}, device_id_type=MESH)
    for d in range(1, N):
        pl.semaphore_signal(bar, inc=1, device_id={"voc": lax.rem(me_v + d, N)}, device_id_type=MESH)
    pl.semaphore_wait(bar, M + N - 2)

    for d in range(1, N):
        send(mix, mix_all.at[d], mix_s.at[d], mix_r.at[d], {"voc": lax.rem(me_v + d, N)})
    mix_all[0] = mix[...]
    for d in range(1, Z):
        zz = lax.rem(z + d, Z)
        send(hblk.at[zz], hrow.at[:, pl.ds(z * T, T)], hid_s.at[d], hid_r.at[d],
             {"tok": zz * 2 + y})
    hrow[:, rows_of(z, T), :] = hblk[z]

    for k in range(K):
        pltpu.make_async_copy(proj_hbm.at[k], w.at[k], w_sem.at[k]).wait()
        ctx[me_v, k * T:(k + 1) * T, :] = jnp.tanh(
            jnp.dot(hidden[...], w[k], preferred_element_type=F32)
        ).astype(BF16)
        piece = ctx.at[me_v, pl.ds(k * T, T)]
        for i in range(1, half):
            send(piece, piece, ctx_s.at[i, k], ctx_r.at[me_v, k],
                 {"voc": lax.rem(chip + i, half) * 2 + core})
        send(piece, piece, ctx_s.at[0, k], ctx_r.at[me_v, k], {"voc": partner})

    def add_logits(s, first=False):
        part = jnp.dot(ctx[s], vw[pl.ds(pl.multiple_of(s * E, E), E), :],
                       preferred_element_type=F32)
        logit[...] = part if first else logit[...] + part

    add_logits(me_v, True)
    for k in range(K):
        arrived(ctx.at[partner, pl.ds(k * T, T)], ctx_r.at[partner, k], ctx_s.at[0, k])
    add_logits(partner)

    tcol = column(targets[...].astype(F32), V)
    ids = (me_v * V + lax.broadcasted_iota(jnp.int32, (T, V), 1)).astype(F32)
    onehot = (tcol == ids).astype(F32)
    for d in range(1, N):
        arrived(mix_all.at[d], mix_r.at[d], mix_s.at[d])
    mixing = jnp.zeros((K, T), F32)
    for d in range(N):
        s = lax.rem(me_v - d + N, N)
        mixing = mixing + lax.dot_general(
            mix_all[d], hidden[:, pl.ds(pl.multiple_of(s * E, E), E)], NT,
            preferred_element_type=F32)
    exp_mix = jnp.exp(mixing)
    weights = exp_mix / jnp.sum(exp_mix, axis=0, keepdims=True)

    for i in range(1, half):
        s = lax.rem(chip - i + half, half) * 2 + core
        for k in range(K):
            piece = ctx.at[s, pl.ds(k * T, T)]
            arrived(piece, ctx_r.at[s, k], ctx_s.at[i, k])
            send(piece, piece, ctx_f.at[i, k], ctx_r.at[s, k], {"voc": partner})
        add_logits(s)
    for i in range(1, half):
        s = lax.rem(chip - i + half, half) * 2 + 1 - core
        for k in range(K):
            arrived(ctx.at[s, pl.ds(k * T, T)], ctx_r.at[s, k], ctx_s.at[i, k])
        add_logits(s)

    lane = lax.broadcasted_iota(jnp.int32, (T, 128), 1)
    table = jnp.zeros((T, 128), F32)
    for k in range(K):
        part = jnp.sum(logit[k * T:(k + 1) * T, :] * onehot, axis=1, keepdims=True)
        table = jnp.where(lane == k, part, table)
    tgt[0] = table.T[0:8, :]
    for d in range(1, N):
        send(tgt.at[0], tgt.at[d], tgt_s.at[d], tgt_r.at[d], {"voc": lax.rem(me_v + d, N)})
    for k in range(K):
        rows = slice(k * T, (k + 1) * T)
        logit[rows, :] = jnp.exp(logit[rows, :] - column(logz[k:k + 1, :], V)) - onehot
    for d in range(1, N):
        arrived(tgt.at[d], tgt_r.at[d], tgt_s.at[d])
    target = tgt[0]
    for d in range(1, N):
        target = target + tgt[d]
    likely = jnp.exp(target[0:K, :] - logz[...])
    joint = weights * likely
    posterior = joint / jnp.sum(joint, axis=0, keepdims=True)
    factor = loss[...] * posterior
    mgrad[...] = loss[...] * (weights - posterior)
    for k in range(K):
        rows = slice(k * T, (k + 1) * T)
        lg[rows, :] = (column(factor[k:k + 1, :], V) * logit[rows, :]).astype(BF16)

    def cg_part(s, k):
        return lax.dot_general(
            lg[k * T:(k + 1) * T, :], vw[pl.ds(pl.multiple_of(s * E, E), E), :], NT,
            preferred_element_type=F32)

    for i in list(range(1, half)) + [0]:
        s = lax.rem(chip + i, half) * 2
        for k in range(K):
            cgs[i, k] = cg_part(s + 1 - core, k).astype(BF16)
            send(cgs.at[i, k], cgr.at[i, k], cgp_s.at[i, k], cgp_r.at[i, k], {"voc": partner})
        for k in range(K):
            part = cg_part(s + core, k)
            if i == 0:
                own_cg[k] = part
            else:
                arrived(cgr.at[i, k], cgp_r.at[i, k], cgp_s.at[i, k])
                cgx[i, k] = (part + cgr[i, k].astype(F32)).astype(BF16)
                send(cgx.at[i, k], xr.at[i, k], cgx_s.at[i, k], cgx_r.at[i, k], {"voc": s + core})

    for s in range(N):
        vgb[s * E:(s + 1) * E, :] = lax.dot_general(
            ctx[s], lg[...], TN, preferred_element_type=F32).astype(BF16)
    for zz in range(Z):
        send(vgb.at[pl.ds((zz * 2 + 1 - y) * R, R)], vgy.at[zz], vy_s.at[zz], vy_r.at[zz],
             {"tok": ypart})

    for d in range(1, Z):
        src = lax.rem(z - d + Z, Z)
        arrived(hrow.at[:, pl.ds(src * T, T)], hid_r.at[d], hid_s.at[d])
    for b in range(2):
        htr[b] = hrow[b].T

    pieces = [(k, 0, E) for k in range(K)]
    if E % 256 == 0:
        pieces[-1:] = [(K - 1, 0, E // 2), (K - 1, E // 2, E // 2)]

    def relay(t, p, way, pred):
        k, lo, wide = pieces[p]
        piece = pg.at[k, rows_of(t, T), pl.ds(lo, wide)]
        c = remote(piece, piece, ag_s.at[way, t, p], ag_r.at[t, p],
                   {"tok": me_t + 2 - 4 * way})
        pl.when(pred)(c.start)
        sends.append((pred, c))

    has_r = z + 1 < Z
    has_l = z >= 1
    for k in range(K):
        total = own_cg[k]
        arrived(cgr.at[0, k], cgp_r.at[0, k], cgp_s.at[0, k])
        total = total + cgr[0, k].astype(F32)
        for i in range(1, half):
            arrived(xr.at[i, k], cgx_r.at[i, k], cgx_s.at[i, k])
            total = total + xr[i, k].astype(F32)
        c = ctx[me_v, k * T:(k + 1) * T, :].astype(F32)
        pg[k, rows_of(z, T), :] = (total * (1.0 - c * c)).astype(BF16)
        if Z > 1:
            for p in range(len(pieces)):
                if pieces[p][0] == k:
                    relay(z, p, 0, has_r)
                    relay(z, p, 1, has_l)

    def hid_part(s):
        total = jnp.zeros((T, E), F32)
        for k in range(K):
            total = total + lax.dot_general(
                pg[k, rows_of(z, T), :], w[k, pl.ds(pl.multiple_of(s * E, E), E), :], NT,
                preferred_element_type=F32)
        return total

    def hid_send(d):
        s = lax.rem(me_v + d, N)
        if d == 0:
            own_hs[...] = hid_part(s)
        else:
            hss[d] = hid_part(s).astype(BF16)
            send(hss.at[d], hsr.at[d], hs_s.at[d], hs_r.at[d], {"voc": s})

    hid_order = list(range(1, N)) + [0]
    hid_per = -(-N // (len(pieces) - 1))

    def pair_sums():
        for zz in range(Z):
            arrived(vgy.at[zz], vy_r.at[zz], vy_s.at[zz])
            vsum[zz] = vgb[rows_of(zz * 2 + y, R), :].astype(F32) + vgy[zz].astype(F32)

    def hop(h):
        for way, at, ends in ((0, h, range(h + 1, Z)), (1, Z - 1 - h, range(Z - 1 - h))):
            copies = [
                remote(vout.at[way, e], vin.at[way, e], vz_s.at[way, e], vz_r.at[way, e],
                       {"tok": me_t + 2 - 4 * way})
                for e in ends
            ]

            @pl.when(z == at)
            def _(way=way, ends=ends, copies=copies):
                for e, c in zip(ends, copies):
                    part = vsum[e]
                    if h > 0:
                        arrived(vin.at[way, e], vz_r.at[way, e], vz_s.at[way, e])
                        part = part + vin[way, e].astype(F32)
                    vout[way, e] = part.astype(BF16)
                    c.start()
            for c in copies:
                sends.append((z == at, c))

    if Z == 1:
        for e in hid_order:
            hid_send(e)
    per = -(-(Z - 1) // (len(pieces) - 1))
    for p, (k, lo, wide) in enumerate(pieces):
        lanes = slice(lo, lo + wide)
        for d in range(1, Z):
            for there, t, way, more in (
                (z >= d, z - d, 0, has_r), (z + d < Z, z + d, 1, has_l),
            ):
                def _(t=t):
                    arrived(pg.at[k, rows_of(t, T), pl.ds(lo, wide)], ag_r.at[t, p], ag_s.at[0, t, p])
                pl.when(there)(_)
                if d < Z - 1:
                    relay(t, p, way, there & more)
            if d == 1:
                for e in hid_order[p * hid_per:(p + 1) * hid_per]:
                    hid_send(e)
        psend[k, :, lanes] = jnp.dot(
            htr[1 - y], pg[k, :, lanes], preferred_element_type=F32).astype(BF16)
        send(psend.at[k, :, pl.ds(lo, wide)], precv.at[k, :, pl.ds(lo, wide)],
             pp_s.at[p], pp_r.at[p], {"tok": ypart})
        acc[k, :, lanes] = jnp.dot(htr[y], pg[k, :, lanes], preferred_element_type=F32)
        if p == 0:
            pair_sums()
        for h in range(p * per, min((p + 1) * per, Z - 1)):
            hop(h)

    acc_v = vsum.at[z]
    for way, pred in ((0, has_l), (1, has_r)):
        @pl.when(pred)
        def _(way=way):
            arrived(vin.at[way, z], vz_r.at[way, z], vz_s.at[way, z])
            acc_v[...] += vin[way, z].astype(F32)
    out_vocab[...] = acc_v[...].astype(BF16)
    htot = own_hs[...]
    for d in range(1, N):
        arrived(hsr.at[d], hs_r.at[d], hs_s.at[d])
        htot = htot + hsr[d].astype(F32)
    mixf = mix[...].astype(F32)
    for k in range(K):
        htot = htot + column(mgrad[k:k + 1, :], E) * mixf[k:k + 1, :]
    out_hidden[...] = htot.astype(BF16)

    for p, (k, lo, wide) in enumerate(pieces):
        lanes = slice(lo, lo + wide)
        arrived(precv.at[k, :, pl.ds(lo, wide)], pp_r.at[p], pp_s.at[p])
        out_proj[k, :, lanes] = (acc[k, :, lanes] + precv[k, :, lanes].astype(F32)).astype(BF16)
    for pred, c in sends:
        if pred is None:
            c.wait_send()
        else:
            pl.when(pred)(c.wait_send)


def rows_of(block, size):
    return pl.ds(pl.multiple_of(block * size, size), size)


def body_base(M, N, hidden, mix_weight, comp_proj, vocab_weight, log_normalizer, targets, loss_grad):
    T, D = hidden.shape
    K, E = mix_weight.shape
    V = vocab_weight.shape[1]
    R = D // M
    half = N // 2
    Z = M // 2
    w = jnp.transpose(comp_proj, (1, 0, 2))
    vm = pltpu.VMEM
    dma = pltpu.SemaphoreType.DMA
    scratch = [
        vm((K, D, E), BF16), vm((N, K * T, E), BF16), vm((N, K, E), BF16),
        vm((Z, 2, T, R), BF16), vm((2, Z * T, R), BF16), vm((2, R, Z * T), BF16), vm((K * T, V), F32), vm((K * T, V), BF16),
        vm((N, 8, T), F32),
        vm((half, K, T, E), BF16), vm((half, K, T, E), BF16),
        vm((half, K, T, E), BF16), vm((half, K, T, E), BF16),
        vm((K, T, E), F32), vm((D, V), BF16), vm((Z, R, V), BF16),
        vm((Z, R, V), F32), vm((2, Z, R, V), BF16), vm((2, Z, R, V), BF16),
        vm((K, Z * T, E), BF16), vm((N, T, E), BF16), vm((N, T, E), BF16),
        vm((T, E), F32), vm((K, R, E), F32), vm((K, R, E), BF16), vm((K, R, E), BF16),
        vm((K, T), F32),
        dma((K,)), dma((half, K)), dma((half, K)), dma((N, K)), dma((N,)), dma((N,)),
        dma((Z,)), dma((Z,)), dma((N,)), dma((N,)),
        dma((half, K)), dma((half, K)), dma((half, K)), dma((half, K)),
        dma((Z,)), dma((Z,)), dma((2, Z)), dma((2, Z)), dma((N,)), dma((N,)),
        dma((2, Z, K + 1)), dma((Z, K + 1)), dma((K + 1,)), dma((K + 1,)),
    ]
    spec = pl.BlockSpec(memory_space=pltpu.VMEM)
    hidden_grad, proj_grad, vocab_grad = pl.pallas_call(
        functools.partial(kernel, M, N),
        out_shape=(
            jax.ShapeDtypeStruct((T, E), BF16),
            jax.ShapeDtypeStruct((K, R, E), BF16),
            jax.ShapeDtypeStruct((R, V), BF16),
        ),
        in_specs=[spec, spec, pl.BlockSpec(memory_space=pltpu.MemorySpace.HBM)] + [spec] * 4,
        out_specs=(spec, spec, spec),
        scratch_shapes=scratch,
        compiler_params=pltpu.CompilerParams(
            collective_id=0, has_side_effects=True, vmem_limit_bytes=48 * 1024 * 1024
        ),
    )(hidden, mix_weight, w, vocab_weight, log_normalizer, targets[None, :], loss_grad[None, :])
    return hidden_grad, jnp.transpose(proj_grad, (1, 0, 2)), vocab_grad


ORDER = (
    (0, 0), (1, 0), (2, 0), (0, 1), (2, 1), (12,), (0, 2), (1, 1), (0, 3), (1, 3), (10, 2), (8,), (9,),
    (1, 2), (3, 0, 1), (3, 0, 2), (3, 0, 3), (11, 3, 0), (3, 1, 1), (2, 3), (4, 0, 3), (4, 0, 1),
    (3, 1, 2), (11, 3, 1), (2, 2), (10, 3), (5, 0, 0), (4, 0, 2), (4, 1, 1), (5, 2, 0), (13,), (5, 0, 1),
    (4, 3, 1), (3, 1, 3), (3, 3, 2), (3, 3, 1), (6, 0, 1), (5, 0, 3), (6, 0, 0), (5, 0, 2), (4, 1, 2),
    (5, 1, 0), (6, 0, 3), (6, 0, 2), (7, 0), (4, 1, 3), (4, 2, 1), (3, 3, 3), (5, 1, 1), (4, 3, 2),
    (3, 2, 1), (5, 1, 2), (5, 1, 3), (3, 2, 2), (5, 3, 0), (6, 1, 0), (6, 1, 1), (5, 3, 1), (6, 1, 2),
    (3, 2, 3), (4, 3, 3), (6, 1, 3), (7, 1), (6, 2, 0), (4, 2, 2), (6, 3, 1), (6, 3, 0), (5, 3, 2), (15,),
    (4, 2, 3), (5, 3, 3), (6, 3, 2), (5, 2, 1), (5, 2, 2), (6, 3, 3), (7, 3), (5, 2, 3), (6, 2, 2),
    (6, 2, 1), (6, 2, 3), (7, 2), (14, 0), (14, 1), (14, 2), (14, 3),
)


def scoped(fn):
    def run(*args, **kw):
        tag = "_".join(str(a) for a in args if isinstance(a, int))
        with jax.named_scope(fn.__name__ + "_" + tag):
            return fn(*args, **kw)
    return run


def mix_rows(K, flip=False):
    B = 256 // K
    r = lax.broadcasted_iota(jnp.int32, (256, 256), 1 if flip else 0)
    c = lax.broadcasted_iota(jnp.int32, (256, 256), 0 if flip else 1)
    return (c == K * (r % B) + r // B).astype(F32).astype(BF16)


def fast_kernel(
    M, N,
    hid_hbm, mix_hbm, proj_hbm, vw_hbm, logz_hbm, tg_hbm, loss_hbm,
    out_hidden, out_proj, out_vocab,
    raw, w, hida, vw, vwe, vwt, mix, logz, targets, loss,
    ctx, ctxz, mix_all, htr, logit, lg, lgall, tgt, scale, pg,
    vgb, vgy, vsum, vout, vin, hss, hsr, own_hs, acc, psend, precv, mgrad,
    l_sem, w_sem, all_s, over_s, own_s, on_s,
    ctx_r, mix_r, hz_r, hp_r, vx_r, vp_r, vwz_r, vwy_r,
    tgt_r, lg_r, vy_r, vz_r, hs_r, pp_r, sc_r,
):
    K, D, E = w.shape
    T = hida.shape[2]
    H = D // 2
    V = vw.shape[1]
    R = D // M
    J = E // 128
    half = N // 2
    Z = M // 2
    B = 256 // K
    me_t = lax.axis_index("tok")
    me_v = lax.axis_index("voc")
    chip = me_v // 2
    core = me_v % 2
    partner = me_v + 1 - 2 * core
    z = me_t // 2
    y = me_t % 2
    ypart = me_t + 1 - 2 * y
    has_r = z + 1 < Z
    has_l = z >= 1

    def remote(src, dst, ss, rs, dev):
        return pltpu.make_async_remote_copy(
            src_ref=src, dst_ref=dst, send_sem=ss, recv_sem=rs,
            device_id=dev, device_id_type=MESH,
        )

    groups = [0]

    def send(src, dst, rs, dev):
        size = math.prod(src.shape) * jnp.dtype(src.dtype).itemsize
        if groups[-1] + size > D * K * 256:
            groups.append(0)
        groups[-1] += size
        remote(src, dst, all_s.at[len(groups) - 1], rs, dev).start()

    def sent(sem, size):
        ref = raw.at[0, pl.ds(0, size // (K * 256))]
        remote(ref, ref, sem, vp_r.at[0], {"voc": partner}).wait_send()

    def arrived(ref, rs):
        remote(ref, ref, all_s.at[0], rs, {"voc": partner}).wait_recv()

    def mate(j):
        if j == 0:
            return z
        near = jnp.minimum(z, Z - 1 - z)
        d = (j + 1) // 2
        both = z + d if j % 2 == 1 else z - d
        return jnp.where(j <= 2 * near, both, jnp.where(2 * z < Z, j, Z - 1 - j))

    def onward(zz):
        right = zz < z
        there = (right & has_r) | (jnp.logical_not(right) & has_l)
        return there, me_t + jnp.where(right, 2, -2)

    chunks = 4
    n = D // chunks

    def w_copy(c, j):
        return pltpu.make_async_copy(
            proj_hbm.at[pl.ds(c * n, n), :, pl.ds(j * 128, 128)],
            raw.at[j, pl.ds(c * n, n)], w_sem.at[c])

    loads = [
        pltpu.make_async_copy(hid_hbm.at[:, pl.ds(0, H)], hida.at[z, 0], l_sem.at[0]),
        pltpu.make_async_copy(hid_hbm.at[:, pl.ds(H, H)], hida.at[z, 1], l_sem.at[1]),
        pltpu.make_async_copy(vw_hbm, vw, l_sem.at[2]),
        pltpu.make_async_copy(mix_hbm, mix, l_sem.at[3]),
        pltpu.make_async_copy(logz_hbm, logz, l_sem.at[4]),
        pltpu.make_async_copy(tg_hbm, targets, l_sem.at[5]),
        pltpu.make_async_copy(loss_hbm, loss, l_sem.at[6]),
    ]
    loads[0].start()
    loads[1].start()
    loads[2].start()
    for c in loads[3:]:
        c.start()
    for j in range(J):
        w_copy(0, j).start()

    bar = pltpu.get_barrier_semaphore()
    for d in range(1, M):
        pl.semaphore_signal(bar, inc=1, device_id={"tok": lax.rem(me_t + d, M)}, device_id_type=MESH)
    for d in range(1, N):
        pl.semaphore_signal(bar, inc=1, device_id={"voc": lax.rem(me_v + d, N)}, device_id_type=MESH)

    perm = mix_rows(K)

    @scoped
    def unmix(c):
        chunk = raw.at[:, pl.ds(c * n, n)]
        pltpu.make_async_copy(chunk, chunk, w_sem.at[c]).wait()
        for b in range(c * n // B, (c + 1) * n // B):
            x = jnp.concatenate(
                [raw.at[j].reshape(D * K, 128)[b * 256:(b + 1) * 256, :] for j in range(J)], axis=1)
            rows = jnp.dot(perm, x, preferred_element_type=F32).astype(BF16)
            for k in range(K):
                w[k, b * B:(b + 1) * B, :] = rows[k * B:(k + 1) * B]

    with jax.named_scope("loads"):
        for c in loads[:3]:
            c.wait()
    for c in range(1, chunks):
        for j in range(J):
            w_copy(c, j).start()
    with jax.named_scope("barrier"):
        pl.semaphore_wait(bar, M + N - 2)

    g = z % 2
    zpair = me_t + 2 - 4 * g

    def vw_rows(yy, part):
        return pl.ds(pl.multiple_of(yy * (E // 2) + part * (E // 4), E // 4), E // 4)

    def vw_send():
        for i in range(1, half):
            for c in range(2):
                v = lax.rem(chip + i, half) * 2 + c
                rows = vw_rows(y, g)
                send(vw.at[pl.ds(pl.multiple_of(v * E + rows.start, E // 4), rows.size)],
                     vwe.at[me_v, rows], vx_r.at[me_v], {"voc": v})

    @scoped
    def vw_pass():
        for i in range(1, half):
            ci = lax.rem(chip + i, half)
            for c in range(2):
                arrived(vwe.at[ci * 2 + c, vw_rows(y, g)], vx_r.at[ci * 2 + c])
            piece = vwe.at[pl.ds(ci * 2, 2), vw_rows(y, g)]
            send(piece, piece, vwz_r.at[ci], {"tok": zpair})
            send(piece, piece, vwy_r.at[ci, 0], {"tok": ypart})

    @scoped
    def vw_turn():
        for i in range(1, half):
            ci = lax.rem(chip + i, half)
            piece = vwe.at[pl.ds(ci * 2, 2), vw_rows(y, 1 - g)]
            arrived(piece, vwz_r.at[ci])
            send(piece, piece, vwy_r.at[ci, 1], {"tok": ypart})

    def hid_piece(zz, side, p):
        return hida.at[zz, side, pl.ds(p * (T // 2), T // 2)]

    vw_send()
    for p in range(2):
        piece = hid_piece(z, core, p)
        pl.when(has_r)(remote(piece, piece, own_s.at[0], hz_r.at[z, p], {"tok": me_t + 2}).start)
        pl.when(has_l)(remote(piece, piece, own_s.at[1], hz_r.at[z, p], {"tok": me_t - 2}).start)
    for c in loads[3:]:
        c.wait()
    for d in range(1, N):
        send(mix, mix_all.at[d], mix_r.at[d], {"voc": lax.rem(me_v + d, N)})
    send(vw.at[rows_of(partner, E)], vwe.at[me_v], vp_r.at[0], {"voc": partner})
    for c in range(chunks):
        unmix(c)

    def context(zz, k):
        both = jnp.dot(hida[zz, 0], w[k, 0:H, :], preferred_element_type=F32)
        both = both + jnp.dot(hida[zz, 1], w[k, H:D, :], preferred_element_type=F32)
        return jnp.tanh(both).astype(BF16)

    for k in range(K):
        with jax.named_scope("context"):
            ctx[me_v, k * T:(k + 1) * T, :] = context(z, k)
        if k == 1:
            vw_pass()
        piece = ctx.at[me_v, pl.ds(k * T, T)]
        for i in range(1, half):
            send(piece, piece, ctx_r.at[me_v, k],
                 {"voc": lax.rem(chip + i, half) * 2 + core})
        send(piece, piece, ctx_r.at[me_v, k], {"voc": partner})

    @scoped
    def add_logits(s, first=False):
        part = jnp.dot(ctx[s], vw[rows_of(s, E), :], preferred_element_type=F32)
        logit[...] = part if first else logit[...] + part

    @scoped
    def relay_hid(j, p, fwd):
        zz = mate(j)
        there, to = onward(zz)
        piece = hid_piece(zz, core, p)
        on = remote(piece, piece, on_s.at[0, j], hz_r.at[zz, p], {"tok": to})
        over = remote(piece, piece, over_s.at[0], hp_r.at[zz, p], {"voc": partner})

        @pl.when(there if fwd else jnp.logical_not(there))
        def _():
            arrived(piece, hz_r.at[zz, p])
            if fwd:
                on.start()
            over.start()

    @scoped
    def ctx_mate(j, ks):
        zz = mate(j)
        if ks[0] == 0:
            for p in range(2):
                arrived(hid_piece(zz, 1 - core, p), hp_r.at[zz, p])
        for k in ks:
            ctxz[zz, k * T:(k + 1) * T, :] = context(zz, k)

    @scoped
    def ctx_pass(k):
        for i in range(1, half):
            s = lax.rem(chip - i + half, half) * 2 + core
            piece = ctx.at[s, pl.ds(k * T, T)]
            arrived(piece, ctx_r.at[s, k])
            send(piece, piece, ctx_r.at[s, k], {"voc": partner})

    add_logits(me_v, True)
    for j in range(1, min(Z, 3)):
        relay_hid(j, 0, True)
    for k in range(K):
        arrived(ctx.at[partner, pl.ds(k * T, T)], ctx_r.at[partner, k])
    add_logits(partner)

    tcol = column(targets[...].astype(F32), V)
    ids = (me_v * V + lax.broadcasted_iota(jnp.int32, (T, V), 1)).astype(F32)
    onehot = (tcol == ids).astype(F32)
    mix_all[0] = mix[...]
    for d in range(1, N):
        arrived(mix_all.at[d], mix_r.at[d])
    mixing = jnp.zeros((K, T), F32)
    for d in range(N):
        s = lax.rem(me_v - d + N, N)
        mixing = mixing + lax.dot_general(
            mix_all[d],
            hida[z, s // half, :, pl.ds(pl.multiple_of((s % half) * E, E), E)], NT,
            preferred_element_type=F32)
    exp_mix = jnp.exp(mixing)
    weights = exp_mix / jnp.sum(exp_mix, axis=0, keepdims=True)

    for j in range(1, min(Z, 3)):
        relay_hid(j, 1, True)
    ctx_pass(0)
    if Z > 1:
        relay_hid(1, 0, False)
        relay_hid(1, 1, False)
    ctx_pass(1)
    vw_turn()
    if Z > 1:
        ctx_mate(1, range(K))
    for j in range(3, Z):
        relay_hid(j, 0, True)
    ctx_pass(2)
    for j in range(3, Z):
        relay_hid(j, 1, True)
    if Z > 2:
        relay_hid(2, 0, False)
    for k in range(3, K):
        ctx_pass(k)
    if Z > 2:
        relay_hid(2, 1, False)
    for i in range(1, half):
        add_logits(lax.rem(chip - i + half, half) * 2 + core)
    for i in range(1, half):
        s = lax.rem(chip - i + half, half) * 2 + 1 - core
        for k in range(K):
            arrived(ctx.at[s, pl.ds(k * T, T)], ctx_r.at[s, k])
        add_logits(s)

    lane = lax.broadcasted_iota(jnp.int32, (T, 128), 1)
    table = jnp.zeros((T, 128), F32)
    for k in range(K):
        part = jnp.sum(logit[k * T:(k + 1) * T, :] * onehot, axis=1, keepdims=True)
        table = jnp.where(lane == k, part, table)
    tgt[0] = table.T[0:8, :]
    for d in range(1, N):
        send(tgt.at[0], tgt.at[d], tgt_r.at[d], {"voc": lax.rem(me_v + d, N)})
    @scoped
    def scales():
        for d in range(1, N):
            arrived(tgt.at[d], tgt_r.at[d])
        target = tgt[0]
        for d in range(1, N):
            target = target + tgt[d]
        likely = jnp.exp(target[0:K, :] - logz[...])
        joint = weights * likely
        posterior = joint / jnp.sum(joint, axis=0, keepdims=True)
        scale[z, 0:K, :] = loss[...] * posterior
        mgrad[...] = loss[...] * (weights - posterior)
        for d in range(1, Z):
            send(scale.at[z], scale.at[z], sc_r.at[z], {"tok": lax.rem(me_t + 2 * d, M)})

    def shares(zz, k):
        piece = lgall.at[zz, me_v, k]
        return [
            remote(piece, piece, over_s.at[1], lg_r.at[zz, me_v, k],
                   {"voc": lax.rem(chip + i, half) * 2 + core})
            for i in range(1, half)
        ] + [remote(piece, piece, over_s.at[2], lg_r.at[zz, me_v, k], {"voc": partner})]

    def share(zz, k):
        for c in shares(zz, k):
            c.start()

    @scoped
    def own_out(k):
        rows = slice(k * T, (k + 1) * T)
        logit[rows, :] = jnp.exp(logit[rows, :] - column(logz[k:k + 1, :], V)) - onehot
        lgall[z, me_v, k] = logit[rows, :].astype(BF16)

    @scoped
    def own_share(k):
        share(z, k)

    @scoped
    def own_line(k):
        piece = lgall.at[z, me_v, k]
        pl.when(has_r)(remote(piece, piece, own_s.at[0], lg_r.at[z, me_v, k], {"tok": me_t + 2}).start)
        pl.when(has_l)(remote(piece, piece, own_s.at[1], lg_r.at[z, me_v, k], {"tok": me_t - 2}).start)
        if k == 0:
            for way, end in ((0, 0), (1, Z - 1)):
                far = remote(piece, piece, own_s.at[2 + way], lg_r.at[z, me_v, k],
                             {"tok": me_t + (1 - 2 * way) * (M - 2)})
                pl.when(z == end)(far.start)

    def near_end(zz, there, to):
        end = to // 2
        return there & (end - zz < Z - 1) & (zz - end < Z - 1)

    @scoped
    def relay_lg(k, j, fwd):
        zz = mate(j)
        there, to = onward(zz)
        if k == 0:
            there = near_end(zz, there, to)
        piece = lgall.at[zz, me_v, k]
        on = remote(piece, piece, on_s.at[1 if k == 0 else 0, j], lg_r.at[zz, me_v, k], {"tok": to})

        @pl.when(there if fwd else jnp.logical_not(there))
        def _():
            arrived(piece, lg_r.at[zz, me_v, k])
            if fwd:
                on.start()
            share(zz, k)

    @scoped
    def cross_lg(k, j):
        zz = mate(j)
        for i in range(1, half):
            s = lax.rem(chip - i + half, half) * 2 + core
            piece = lgall.at[zz, s, k]
            arrived(piece, lg_r.at[zz, s, k])
            remote(piece, piece, over_s.at[3], lg_r.at[zz, s, k], {"voc": partner}).start()

    @scoped
    def pre_grad(k, j):
        zz = mate(j)
        rows = slice(k * T, (k + 1) * T)
        for i in range(half):
            s = lax.rem(chip + i, half) * 2 + 1 - core
            arrived(lgall.at[zz, s, k], lg_r.at[zz, s, k])
        total = None
        for s in range(N):
            part = jnp.dot(lgall[zz, s, k], vwt[s], preferred_element_type=F32)
            total = part if total is None else total + part
        c = (ctx[me_v, rows, :] if j == 0 else ctxz[zz, rows, :]).astype(F32)
        if k == 0:
            if j > 0:
                arrived(scale.at[zz], sc_r.at[zz])
        total = total * column(scale[zz, k:k + 1, :], E)
        pg[k, rows_of(zz, T), :] = (total * (1.0 - c * c)).astype(BF16)

    def hid_part(s):
        total = jnp.zeros((T, E), F32)
        for k in range(K):
            total = total + lax.dot_general(
                pg[k, rows_of(z, T), :], w[k, rows_of(s, E), :], NT,
                preferred_element_type=F32)
        return total

    @scoped
    def hid_send(d):
        s = lax.rem(me_v + d, N)
        if d == 0:
            own_hs[...] = hid_part(s)
        else:
            hss[d] = hid_part(s).astype(BF16)
            send(hss.at[d], hsr.at[d], hs_r.at[d], {"voc": s})

    @scoped
    def pair_sums():
        for d in list(range(1, Z)) + [0]:
            zz = lax.rem(z + d, Z)
            arrived(vgy.at[zz], vy_r.at[zz])
            total = vgb[rows_of(zz * 2 + y, R), :].astype(F32) + vgy[zz].astype(F32)
            if d == 0:
                vsum[...] = total
            else:
                vout[zz] = total.astype(BF16)
                send(vout.at[zz], vin.at[z], vz_r.at[z], {"tok": zz * 2 + y})

    pieces = [(k, 0, E) for k in range(K)]
    if E % 256 == 0:
        pieces[-1:] = [(K - 1, 0, E // 2), (K - 1, E // 2, E // 2)]

    @scoped
    def proj_part(k):
        for p, (kk, lo, wide) in enumerate(pieces):
            if kk == k:
                lanes = slice(lo, lo + wide)
                psend[k, :, lanes] = jnp.dot(
                    htr[1 - y], pg[k, :, lanes], preferred_element_type=F32).astype(BF16)
                send(psend.at[k, :, pl.ds(lo, wide)], precv.at[k, :, pl.ds(lo, wide)],
                     pp_r.at[p], {"tok": ypart})
        acc[k] = jnp.dot(htr[y], pg[k], preferred_element_type=F32)

    @scoped
    def vocab_part():
        for k in range(K):
            rows = slice(k * T, (k + 1) * T)
            lg[rows, :] = (column(scale[z, k:k + 1, :], V) * logit[rows, :]).astype(BF16)
        for s in range(N):
            vgb[s * E:(s + 1) * E, :] = lax.dot_general(
                ctx[s], lg[...], TN, preferred_element_type=F32).astype(BF16)
            for zz in range(s * Z // N, (s + 1) * Z // N):
                send(vgb.at[pl.ds((zz * 2 + 1 - y) * R, R)], vgy.at[zz], vy_r.at[zz],
                     {"tok": ypart})

    @scoped
    def vw_done():
        vwe[me_v] = vw[rows_of(me_v, E), :]
        arrived(vwe.at[partner], vp_r.at[0])
        for i in range(1, half):
            ci = lax.rem(chip + i, half)
            for p, part in enumerate((g, 1 - g)):
                arrived(vwe.at[pl.ds(ci * 2, 2), vw_rows(1 - y, part)], vwy_r.at[ci, p])
        for s in range(N):
            vwt[s] = vwe[s].T

    @scoped
    def turn():
        for b in range(2):
            col = (z * 2 + b) * R
            for zz in range(Z):
                htr[b, :, zz * T:(zz + 1) * T] = hida[
                    zz, col // H, :, pl.ds(pl.multiple_of(col % H, R), R)].T

    def relay_on(k, j):
        relay_lg(k, j, True)

    def relay_in(k, j):
        relay_lg(k, j, False)

    def mate_ctx(j):
        ctx_mate(j, range(K))

    def hid_in(j, p):
        relay_hid(j, p, False)

    steps = (own_out, own_share, own_line, relay_on, relay_in, cross_lg, pre_grad, proj_part,
             scales, vocab_part, mate_ctx, hid_in, vw_done, turn, hid_send, pair_sums)
    for step, *rest in ORDER:
        steps[step](*rest)

    vtot = vsum[...]
    for d in range(1, Z):
        zz = lax.rem(z + d, Z)
        arrived(vin.at[zz], vz_r.at[zz])
        vtot = vtot + vin[zz].astype(F32)
    out_vocab[...] = vtot.astype(BF16)
    htot = own_hs[...]
    for d in range(1, N):
        arrived(hsr.at[d], hs_r.at[d])
        htot = htot + hsr[d].astype(F32)
    mixf = mix[...].astype(F32)
    for k in range(K):
        htot = htot + column(mgrad[k:k + 1, :], E) * mixf[k:k + 1, :]
    out_hidden[...] = htot.astype(BF16)

    back = mix_rows(K, True)
    for p, (k, lo, wide) in enumerate(pieces):
        lanes = slice(lo, lo + wide)
        with jax.named_scope("precv"):
            arrived(precv.at[k, :, pl.ds(lo, wide)], pp_r.at[p])
        psum = (acc[k, :, lanes] + precv[k, :, lanes].astype(F32)).astype(BF16)
        if k < K - 1:
            precv[k, :, lanes] = psum
            continue
        for b in range(R // B):
            rows = slice(b * B, (b + 1) * B)
            x = jnp.concatenate([precv[q, rows, lanes] for q in range(K - 1)] + [psum[rows]], axis=0)
            out = jnp.dot(back, x, preferred_element_type=F32).astype(BF16)
            for j in range(wide // 128):
                out_proj.at[lo // 128 + j].reshape(R * K, 128)[b * 256:(b + 1) * 256, :] = (
                    out[:, j * 128:(j + 1) * 128])
    with jax.named_scope("drain"):
        for i, size in enumerate(groups):
            sent(all_s.at[i], size)
        piece = T * V * 2
        sent(over_s.at[0], (Z - 1) * T * D)
        for i in range(1, 4):
            for _ in range(half - 1):
                sent(over_s.at[i], Z * K * piece)
        for way, pred in ((0, has_r), (1, has_l)):
            pl.when(pred)(functools.partial(sent, own_s.at[way], T * D + K * piece))
        for way, end in ((0, 0), (1, Z - 1)):
            pl.when(z == end)(functools.partial(sent, own_s.at[2 + way], piece))
        for j in range(1, Z):
            zz = mate(j)
            there, to = onward(zz)
            pl.when(there)(functools.partial(sent, on_s.at[0, j], T * D + (K - 1) * piece))
            pl.when(near_end(zz, there, to))(functools.partial(sent, on_s.at[1, j], piece))


def body_fast(M, N, hidden, mix_weight, comp_proj, vocab_weight, log_normalizer, targets, loss_grad):
    T, D = hidden.shape
    K, E = mix_weight.shape
    V = vocab_weight.shape[1]
    R = D // M
    J = E // 128
    half = N // 2
    Z = M // 2
    vm = pltpu.VMEM
    dma = pltpu.SemaphoreType.DMA
    scratch = [
        vm((J, D, K, 128), BF16), vm((K, D, E), BF16), vm((Z, 2, T, D // 2), BF16), vm((D, V), BF16),
        vm((N, E, V), BF16), vm((N, V, E), BF16), vm((K, E), BF16), vm((K, T), F32), vm((1, T), jnp.int32), vm((1, T), F32),
        vm((N, K * T, E), BF16), vm((Z, K * T, E), BF16), vm((N, K, E), BF16), vm((2, R, Z * T), BF16),
        vm((K * T, V), F32), vm((K * T, V), BF16), vm((Z, N, K, T, V), BF16), vm((N, 8, T), F32), vm((Z, 8, T), F32), vm((K, Z * T, E), BF16),
        vm((D, V), BF16), vm((Z, R, V), BF16),
        vm((R, V), F32), vm((Z, R, V), BF16), vm((Z, R, V), BF16),
        vm((N, T, E), BF16), vm((N, T, E), BF16),
        vm((T, E), F32), vm((K, R, E), F32), vm((K, R, E), BF16), vm((K, R, E), BF16),
        vm((K, T), F32),
        dma((7,)), dma((4,)), dma((8,)), dma((4,)), dma((4,)), dma((2, Z)),
        dma((N, K)), dma((N,)), dma((Z, 2)), dma((Z, 2)), dma((N,)), dma((1,)), dma((half,)), dma((half, 2)),
        dma((N,)), dma((Z, N, K)), dma((Z,)), dma((Z,)), dma((N,)), dma((K + 1,)), dma((Z,)),
    ]
    spec = pl.BlockSpec(memory_space=pltpu.VMEM)
    hbm = pl.BlockSpec(memory_space=pltpu.MemorySpace.HBM)
    hid, proj, voc = pl.pallas_call(
        functools.partial(fast_kernel, M, N),
        out_shape=(
            jax.ShapeDtypeStruct((T, E), BF16),
            jax.ShapeDtypeStruct((J, R, K, 128), BF16),
            jax.ShapeDtypeStruct((R, V), BF16),
        ),
        in_specs=[hbm] * 7,
        out_specs=(spec, spec, spec),
        scratch_shapes=scratch,
        compiler_params=pltpu.CompilerParams(
            collective_id=0, has_side_effects=True, vmem_limit_bytes=47 * 1024 * 1024
        ),
    )(*[
        pltpu.with_memory_space_constraint(x, pltpu.MemorySpace.HBM)
        for x in (hidden, mix_weight, comp_proj, vocab_weight, log_normalizer, targets[None, :], loss_grad[None, :])
    ])
    return pl.pallas_call(
        store_kernel,
        out_shape=(
            jax.ShapeDtypeStruct((T, E), BF16),
            jax.ShapeDtypeStruct((R, K, E), BF16),
            jax.ShapeDtypeStruct((R, V), BF16),
        ),
        in_specs=[spec] * 3,
        out_specs=(hbm, hbm, hbm),
        scratch_shapes=[dma((J + 2,))],
        compiler_params=pltpu.CompilerParams(vmem_limit_bytes=4 * 1024 * 1024),
    )(hid, proj, voc)


def store_kernel(hid, proj, voc, out_hid, out_proj, out_voc, sem):
    J = proj.shape[0]
    copies = [pltpu.make_async_copy(hid, out_hid, sem.at[J]), pltpu.make_async_copy(voc, out_voc, sem.at[J + 1])]
    for j in range(J):
        copies.append(pltpu.make_async_copy(proj.at[j], out_proj.at[:, :, pl.ds(j * 128, 128)], sem.at[j]))
    for c in copies:
        c.start()
    for c in copies:
        c.wait()


def body(M, N, *args):
    hidden, mix_weight, comp_proj, vocab_weight = args[:4]
    T, D = hidden.shape
    K, E = mix_weight.shape
    V = vocab_weight.shape[1]
    gathered = 2 * (M // 2) * T * (K * N * V + D + 2 * K * E)
    shapes = K == 4 and M == 8 and N == 4 and E % 128 == 0 and (D // M) % (256 // K) == 0
    if shapes and gathered + 4 * K * D * E <= 28 * 1024 * 1024:
        return body_fast(M, N, *args)
    return body_base(M, N, *args)


def solution(mesh):
    in_specs = (
        P("tok", None),
        P(None, "voc"),
        P(None, None, "voc"),
        P(None, "voc"),
        P(None, "tok"),
        P("tok"),
        P("tok"),
    )
    out_specs = (P("tok", "voc"), P("tok", None, "voc"), P("tok", "voc"))
    return jax.shard_map(
        functools.partial(body, mesh.shape["tok"], mesh.shape["voc"]),
        mesh=mesh, in_specs=in_specs, out_specs=out_specs, check_vma=False,
    )
```

```python
import functools
import math

import jax
import jax.numpy as jnp
from jax import lax
from jax.experimental import pallas as pl
from jax.experimental.pallas import tpu as pltpu
from jax.sharding import PartitionSpec as P

MESH = pl.DeviceIdType.MESH
F32 = jnp.float32
BF16 = jnp.bfloat16
NT = (((1,), (1,)), ((), ()))
TN = (((0,), (0,)), ((), ()))


def column(row, lanes):
    wide = jnp.broadcast_to(row, (128, row.shape[1])).T
    return jnp.concatenate([wide] * (lanes // 128), axis=1)


def kernel(
    M, N,
    hidden, mix, proj_hbm, vw, logz, targets, loss,
    out_hidden, out_proj, out_vocab,
    w, ctx, mix_all, hblk, hrow, htr, logit, lg, tgt,
    cgs, cgr, cgx, xr, own_cg, vgb, vgy, vsum, vout, vin, pg, hss, hsr, own_hs, acc, psend, precv, mgrad,
    w_sem, ctx_s, ctx_f, ctx_r, mix_s, mix_r, hid_s, hid_r, tgt_s, tgt_r,
    cgp_s, cgp_r, cgx_s, cgx_r, vy_s, vy_r, vz_s, vz_r, hs_s, hs_r, ag_s, ag_r, pp_s, pp_r,
):
    K, D, E = w.shape
    T = hidden.shape[0]
    V = vw.shape[1]
    R = D // M
    half = N // 2
    Z = M // 2
    me_t = lax.axis_index("tok")
    me_v = lax.axis_index("voc")
    chip = me_v // 2
    core = me_v % 2
    partner = me_v + 1 - 2 * core
    z = me_t // 2
    y = me_t % 2
    ypart = me_t + 1 - 2 * y
    sends = []

    def remote(src, dst, ss, rs, dev):
        return pltpu.make_async_remote_copy(
            src_ref=src, dst_ref=dst, send_sem=ss, recv_sem=rs,
            device_id=dev, device_id_type=MESH,
        )

    def send(src, dst, ss, rs, dev):
        c = remote(src, dst, ss, rs, dev)
        c.start()
        sends.append((None, c))

    def arrived(ref, rs, ss):
        remote(ref, ref, ss, rs, {"voc": partner}).wait_recv()

    for k in range(K):
        pltpu.make_async_copy(proj_hbm.at[k], w.at[k], w_sem.at[k]).start()
    for j in range(M):
        hblk[j // 2, j % 2] = hidden[:, j * R:(j + 1) * R]

    bar = pltpu.get_barrier_semaphore()
    for d in range(1, M):
        pl.semaphore_signal(bar, inc=1, device_id={"tok": lax.rem(me_t + d, M)}, device_id_type=MESH)
    for d in range(1, N):
        pl.semaphore_signal(bar, inc=1, device_id={"voc": lax.rem(me_v + d, N)}, device_id_type=MESH)
    pl.semaphore_wait(bar, M + N - 2)

    for d in range(1, N):
        send(mix, mix_all.at[d], mix_s.at[d], mix_r.at[d], {"voc": lax.rem(me_v + d, N)})
    mix_all[0] = mix[...]
    for d in range(1, Z):
        zz = lax.rem(z + d, Z)
        send(hblk.at[zz], hrow.at[:, pl.ds(z * T, T)], hid_s.at[d], hid_r.at[d],
             {"tok": zz * 2 + y})
    hrow[:, rows_of(z, T), :] = hblk[z]

    for k in range(K):
        pltpu.make_async_copy(proj_hbm.at[k], w.at[k], w_sem.at[k]).wait()
        ctx[me_v, k * T:(k + 1) * T, :] = jnp.tanh(
            jnp.dot(hidden[...], w[k], preferred_element_type=F32)
        ).astype(BF16)
        piece = ctx.at[me_v, pl.ds(k * T, T)]
        for i in range(1, half):
            send(piece, piece, ctx_s.at[i, k], ctx_r.at[me_v, k],
                 {"voc": lax.rem(chip + i, half) * 2 + core})
        send(piece, piece, ctx_s.at[0, k], ctx_r.at[me_v, k], {"voc": partner})

    def add_logits(s, first=False):
        part = jnp.dot(ctx[s], vw[pl.ds(pl.multiple_of(s * E, E), E), :],
                       preferred_element_type=F32)
        logit[...] = part if first else logit[...] + part

    add_logits(me_v, True)
    for k in range(K):
        arrived(ctx.at[partner, pl.ds(k * T, T)], ctx_r.at[partner, k], ctx_s.at[0, k])
    add_logits(partner)

    tcol = column(targets[...].astype(F32), V)
    ids = (me_v * V + lax.broadcasted_iota(jnp.int32, (T, V), 1)).astype(F32)
    onehot = (tcol == ids).astype(F32)
    for d in range(1, N):
        arrived(mix_all.at[d], mix_r.at[d], mix_s.at[d])
    mixing = jnp.zeros((K, T), F32)
    for d in range(N):
        s = lax.rem(me_v - d + N, N)
        mixing = mixing + lax.dot_general(
            mix_all[d], hidden[:, pl.ds(pl.multiple_of(s * E, E), E)], NT,
            preferred_element_type=F32)
    exp_mix = jnp.exp(mixing)
    weights = exp_mix / jnp.sum(exp_mix, axis=0, keepdims=True)

    for i in range(1, half):
        s = lax.rem(chip - i + half, half) * 2 + core
        for k in range(K):
            piece = ctx.at[s, pl.ds(k * T, T)]
            arrived(piece, ctx_r.at[s, k], ctx_s.at[i, k])
            send(piece, piece, ctx_f.at[i, k], ctx_r.at[s, k], {"voc": partner})
        add_logits(s)
    for i in range(1, half):
        s = lax.rem(chip - i + half, half) * 2 + 1 - core
        for k in range(K):
            arrived(ctx.at[s, pl.ds(k * T, T)], ctx_r.at[s, k], ctx_s.at[i, k])
        add_logits(s)

    lane = lax.broadcasted_iota(jnp.int32, (T, 128), 1)
    table = jnp.zeros((T, 128), F32)
    for k in range(K):
        part = jnp.sum(logit[k * T:(k + 1) * T, :] * onehot, axis=1, keepdims=True)
        table = jnp.where(lane == k, part, table)
    tgt[0] = table.T[0:8, :]
    for d in range(1, N):
        send(tgt.at[0], tgt.at[d], tgt_s.at[d], tgt_r.at[d], {"voc": lax.rem(me_v + d, N)})
    for k in range(K):
        rows = slice(k * T, (k + 1) * T)
        logit[rows, :] = jnp.exp(logit[rows, :] - column(logz[k:k + 1, :], V)) - onehot
    for d in range(1, N):
        arrived(tgt.at[d], tgt_r.at[d], tgt_s.at[d])
    target = tgt[0]
    for d in range(1, N):
        target = target + tgt[d]
    likely = jnp.exp(target[0:K, :] - logz[...])
    joint = weights * likely
    posterior = joint / jnp.sum(joint, axis=0, keepdims=True)
    factor = loss[...] * posterior
    mgrad[...] = loss[...] * (weights - posterior)
    for k in range(K):
        rows = slice(k * T, (k + 1) * T)
        lg[rows, :] = (column(factor[k:k + 1, :], V) * logit[rows, :]).astype(BF16)

    def cg_part(s, k):
        return lax.dot_general(
            lg[k * T:(k + 1) * T, :], vw[pl.ds(pl.multiple_of(s * E, E), E), :], NT,
            preferred_element_type=F32)

    for i in list(range(1, half)) + [0]:
        s = lax.rem(chip + i, half) * 2
        for k in range(K):
            cgs[i, k] = cg_part(s + 1 - core, k).astype(BF16)
            send(cgs.at[i, k], cgr.at[i, k], cgp_s.at[i, k], cgp_r.at[i, k], {"voc": partner})
        for k in range(K):
            part = cg_part(s + core, k)
            if i == 0:
                own_cg[k] = part
            else:
                arrived(cgr.at[i, k], cgp_r.at[i, k], cgp_s.at[i, k])
                cgx[i, k] = (part + cgr[i, k].astype(F32)).astype(BF16)
                send(cgx.at[i, k], xr.at[i, k], cgx_s.at[i, k], cgx_r.at[i, k], {"voc": s + core})

    for s in range(N):
        vgb[s * E:(s + 1) * E, :] = lax.dot_general(
            ctx[s], lg[...], TN, preferred_element_type=F32).astype(BF16)
    for zz in range(Z):
        send(vgb.at[pl.ds((zz * 2 + 1 - y) * R, R)], vgy.at[zz], vy_s.at[zz], vy_r.at[zz],
             {"tok": ypart})

    for d in range(1, Z):
        src = lax.rem(z - d + Z, Z)
        arrived(hrow.at[:, pl.ds(src * T, T)], hid_r.at[d], hid_s.at[d])
    for b in range(2):
        htr[b] = hrow[b].T

    pieces = [(k, 0, E) for k in range(K)]
    if E % 256 == 0:
        pieces[-1:] = [(K - 1, 0, E // 2), (K - 1, E // 2, E // 2)]

    def relay(t, p, way, pred):
        k, lo, wide = pieces[p]
        piece = pg.at[k, rows_of(t, T), pl.ds(lo, wide)]
        c = remote(piece, piece, ag_s.at[way, t, p], ag_r.at[t, p],
                   {"tok": me_t + 2 - 4 * way})
        pl.when(pred)(c.start)
        sends.append((pred, c))

    has_r = z + 1 < Z
    has_l = z >= 1
    for k in range(K):
        total = own_cg[k]
        arrived(cgr.at[0, k], cgp_r.at[0, k], cgp_s.at[0, k])
        total = total + cgr[0, k].astype(F32)
        for i in range(1, half):
            arrived(xr.at[i, k], cgx_r.at[i, k], cgx_s.at[i, k])
            total = total + xr[i, k].astype(F32)
        c = ctx[me_v, k * T:(k + 1) * T, :].astype(F32)
        pg[k, rows_of(z, T), :] = (total * (1.0 - c * c)).astype(BF16)
        if Z > 1:
            for p in range(len(pieces)):
                if pieces[p][0] == k:
                    relay(z, p, 0, has_r)
                    relay(z, p, 1, has_l)

    def hid_part(s):
        total = jnp.zeros((T, E), F32)
        for k in range(K):
            total = total + lax.dot_general(
                pg[k, rows_of(z, T), :], w[k, pl.ds(pl.multiple_of(s * E, E), E), :], NT,
                preferred_element_type=F32)
        return total

    def hid_send(d):
        s = lax.rem(me_v + d, N)
        if d == 0:
            own_hs[...] = hid_part(s)
        else:
            hss[d] = hid_part(s).astype(BF16)
            send(hss.at[d], hsr.at[d], hs_s.at[d], hs_r.at[d], {"voc": s})

    hid_order = list(range(1, N)) + [0]
    hid_per = -(-N // (len(pieces) - 1))

    def pair_sums():
        for zz in range(Z):
            arrived(vgy.at[zz], vy_r.at[zz], vy_s.at[zz])
            vsum[zz] = vgb[rows_of(zz * 2 + y, R), :].astype(F32) + vgy[zz].astype(F32)

    def hop(h):
        for way, at, ends in ((0, h, range(h + 1, Z)), (1, Z - 1 - h, range(Z - 1 - h))):
            copies = [
                remote(vout.at[way, e], vin.at[way, e], vz_s.at[way, e], vz_r.at[way, e],
                       {"tok": me_t + 2 - 4 * way})
                for e in ends
            ]

            @pl.when(z == at)
            def _(way=way, ends=ends, copies=copies):
                for e, c in zip(ends, copies):
                    part = vsum[e]
                    if h > 0:
                        arrived(vin.at[way, e], vz_r.at[way, e], vz_s.at[way, e])
                        part = part + vin[way, e].astype(F32)
                    vout[way, e] = part.astype(BF16)
                    c.start()
            for c in copies:
                sends.append((z == at, c))

    if Z == 1:
        for e in hid_order:
            hid_send(e)
    per = -(-(Z - 1) // (len(pieces) - 1))
    for p, (k, lo, wide) in enumerate(pieces):
        lanes = slice(lo, lo + wide)
        for d in range(1, Z):
            for there, t, way, more in (
                (z >= d, z - d, 0, has_r), (z + d < Z, z + d, 1, has_l),
            ):
                def _(t=t):
                    arrived(pg.at[k, rows_of(t, T), pl.ds(lo, wide)], ag_r.at[t, p], ag_s.at[0, t, p])
                pl.when(there)(_)
                if d < Z - 1:
                    relay(t, p, way, there & more)
            if d == 1:
                for e in hid_order[p * hid_per:(p + 1) * hid_per]:
                    hid_send(e)
        psend[k, :, lanes] = jnp.dot(
            htr[1 - y], pg[k, :, lanes], preferred_element_type=F32).astype(BF16)
        send(psend.at[k, :, pl.ds(lo, wide)], precv.at[k, :, pl.ds(lo, wide)],
             pp_s.at[p], pp_r.at[p], {"tok": ypart})
        acc[k, :, lanes] = jnp.dot(htr[y], pg[k, :, lanes], preferred_element_type=F32)
        if p == 0:
            pair_sums()
        for h in range(p * per, min((p + 1) * per, Z - 1)):
            hop(h)

    acc_v = vsum.at[z]
    for way, pred in ((0, has_l), (1, has_r)):
        @pl.when(pred)
        def _(way=way):
            arrived(vin.at[way, z], vz_r.at[way, z], vz_s.at[way, z])
            acc_v[...] += vin[way, z].astype(F32)
    out_vocab[...] = acc_v[...].astype(BF16)
    htot = own_hs[...]
    for d in range(1, N):
        arrived(hsr.at[d], hs_r.at[d], hs_s.at[d])
        htot = htot + hsr[d].astype(F32)
    mixf = mix[...].astype(F32)
    for k in range(K):
        htot = htot + column(mgrad[k:k + 1, :], E) * mixf[k:k + 1, :]
    out_hidden[...] = htot.astype(BF16)

    for p, (k, lo, wide) in enumerate(pieces):
        lanes = slice(lo, lo + wide)
        arrived(precv.at[k, :, pl.ds(lo, wide)], pp_r.at[p], pp_s.at[p])
        out_proj[k, :, lanes] = (acc[k, :, lanes] + precv[k, :, lanes].astype(F32)).astype(BF16)
    for pred, c in sends:
        if pred is None:
            c.wait_send()
        else:
            pl.when(pred)(c.wait_send)


def rows_of(block, size):
    return pl.ds(pl.multiple_of(block * size, size), size)


def body_base(M, N, hidden, mix_weight, comp_proj, vocab_weight, log_normalizer, targets, loss_grad):
    T, D = hidden.shape
    K, E = mix_weight.shape
    V = vocab_weight.shape[1]
    R = D // M
    half = N // 2
    Z = M // 2
    w = jnp.transpose(comp_proj, (1, 0, 2))
    vm = pltpu.VMEM
    dma = pltpu.SemaphoreType.DMA
    scratch = [
        vm((K, D, E), BF16), vm((N, K * T, E), BF16), vm((N, K, E), BF16),
        vm((Z, 2, T, R), BF16), vm((2, Z * T, R), BF16), vm((2, R, Z * T), BF16), vm((K * T, V), F32), vm((K * T, V), BF16),
        vm((N, 8, T), F32),
        vm((half, K, T, E), BF16), vm((half, K, T, E), BF16),
        vm((half, K, T, E), BF16), vm((half, K, T, E), BF16),
        vm((K, T, E), F32), vm((D, V), BF16), vm((Z, R, V), BF16),
        vm((Z, R, V), F32), vm((2, Z, R, V), BF16), vm((2, Z, R, V), BF16),
        vm((K, Z * T, E), BF16), vm((N, T, E), BF16), vm((N, T, E), BF16),
        vm((T, E), F32), vm((K, R, E), F32), vm((K, R, E), BF16), vm((K, R, E), BF16),
        vm((K, T), F32),
        dma((K,)), dma((half, K)), dma((half, K)), dma((N, K)), dma((N,)), dma((N,)),
        dma((Z,)), dma((Z,)), dma((N,)), dma((N,)),
        dma((half, K)), dma((half, K)), dma((half, K)), dma((half, K)),
        dma((Z,)), dma((Z,)), dma((2, Z)), dma((2, Z)), dma((N,)), dma((N,)),
        dma((2, Z, K + 1)), dma((Z, K + 1)), dma((K + 1,)), dma((K + 1,)),
    ]
    spec = pl.BlockSpec(memory_space=pltpu.VMEM)
    hidden_grad, proj_grad, vocab_grad = pl.pallas_call(
        functools.partial(kernel, M, N),
        out_shape=(
            jax.ShapeDtypeStruct((T, E), BF16),
            jax.ShapeDtypeStruct((K, R, E), BF16),
            jax.ShapeDtypeStruct((R, V), BF16),
        ),
        in_specs=[spec, spec, pl.BlockSpec(memory_space=pltpu.MemorySpace.HBM)] + [spec] * 4,
        out_specs=(spec, spec, spec),
        scratch_shapes=scratch,
        compiler_params=pltpu.CompilerParams(
            collective_id=0, has_side_effects=True, vmem_limit_bytes=48 * 1024 * 1024
        ),
    )(hidden, mix_weight, w, vocab_weight, log_normalizer, targets[None, :], loss_grad[None, :])
    return hidden_grad, jnp.transpose(proj_grad, (1, 0, 2)), vocab_grad


ORDER = (
    (0, 0), (1, 0), (2, 0), (0, 1), (0, 2), (1, 1), (1, 2), (2, 1), (0, 3), (12,), (8,), (3, 0, 1), (9,),
    (1, 3), (10, 2), (3, 0, 2), (4, 0, 1), (11, 3, 1), (2, 2), (5, 0, 0), (3, 1, 1), (4, 0, 3), (11, 3, 0),
    (5, 2, 0), (4, 0, 2), (3, 1, 2), (5, 1, 0), (6, 0, 0), (3, 0, 3), (2, 3), (5, 0, 1), (4, 2, 1),
    (10, 3), (4, 1, 1), (3, 1, 3), (3, 2, 1), (5, 0, 3), (5, 0, 2), (6, 0, 1), (4, 1, 2), (5, 3, 0),
    (3, 2, 2), (13,), (6, 2, 0), (3, 3, 1), (6, 0, 3), (6, 0, 2), (7, 0), (4, 1, 3), (4, 2, 2), (3, 2, 3),
    (5, 1, 2), (5, 1, 1), (3, 3, 2), (6, 1, 0), (4, 3, 1), (5, 1, 3), (6, 1, 1), (6, 1, 2), (4, 2, 3),
    (3, 3, 3), (6, 3, 0), (6, 1, 3), (7, 1), (5, 2, 1), (4, 3, 2), (5, 2, 2), (4, 3, 3), (5, 3, 1),
    (6, 2, 1), (5, 2, 3), (6, 3, 1), (6, 2, 2), (5, 3, 2), (14, 2), (15,), (6, 2, 3), (5, 3, 3), (7, 2),
    (6, 3, 2), (6, 3, 3), (7, 3), (14, 3), (14, 0), (14, 1),
)


def scoped(fn):
    def run(*args, **kw):
        tag = "_".join(str(a) for a in args if isinstance(a, int))
        with jax.named_scope(fn.__name__ + "_" + tag):
            return fn(*args, **kw)
    return run


def mix_rows(K, flip=False):
    B = 256 // K
    r = lax.broadcasted_iota(jnp.int32, (256, 256), 1 if flip else 0)
    c = lax.broadcasted_iota(jnp.int32, (256, 256), 0 if flip else 1)
    return (c == K * (r % B) + r // B).astype(F32).astype(BF16)


def fast_kernel(
    M, N,
    hid_hbm, mix_hbm, proj_hbm, vw_hbm, logz_hbm, tg_hbm, loss_hbm,
    out_hidden, out_proj, out_vocab,
    raw, w, hida, vw, vwe, vwt, mix, logz, targets, loss,
    ctx, ctxz, mix_all, htr, logit, lg, lgall, tgt, scale, pg,
    vgb, vgy, vsum, vout, vin, hss, hsr, own_hs, acc, psend, precv, mgrad,
    l_sem, w_sem, all_s, over_s, own_s, on_s,
    ctx_r, mix_r, hz_r, hp_r, vx_r, vp_r, vwz_r, vwy_r,
    tgt_r, lg_r, ld_r, vy_r, vz_r, hs_r, pp_r, sc_r,
):
    K, D, E = w.shape
    T = hida.shape[2]
    H = D // 2
    V = vw.shape[1]
    R = D // M
    J = E // 128
    half = N // 2
    Z = M // 2
    B = 256 // K
    me_t = lax.axis_index("tok")
    me_v = lax.axis_index("voc")
    chip = me_v // 2
    core = me_v % 2
    partner = me_v + 1 - 2 * core
    z = me_t // 2
    y = me_t % 2
    ypart = me_t + 1 - 2 * y
    has_r = z + 1 < Z
    has_l = z >= 1

    def remote(src, dst, ss, rs, dev):
        return pltpu.make_async_remote_copy(
            src_ref=src, dst_ref=dst, send_sem=ss, recv_sem=rs,
            device_id=dev, device_id_type=MESH,
        )

    groups = [0]

    def send(src, dst, rs, dev):
        size = math.prod(src.shape) * jnp.dtype(src.dtype).itemsize
        if groups[-1] + size > D * K * 256:
            groups.append(0)
        groups[-1] += size
        remote(src, dst, all_s.at[len(groups) - 1], rs, dev).start()

    def sent(sem, size):
        ref = raw.at[0, pl.ds(0, size // (K * 256))]
        remote(ref, ref, sem, vp_r.at[0], {"voc": partner}).wait_send()

    def arrived(ref, rs):
        remote(ref, ref, all_s.at[0], rs, {"voc": partner}).wait_recv()

    def mate(j):
        if j == 0:
            return z
        near = jnp.minimum(z, Z - 1 - z)
        d = (j + 1) // 2
        both = z + d if j % 2 == 1 else z - d
        return jnp.where(j <= 2 * near, both, jnp.where(2 * z < Z, j, Z - 1 - j))

    def onward(zz):
        right = zz < z
        there = (right & has_r) | (jnp.logical_not(right) & has_l)
        return there, me_t + jnp.where(right, 2, -2)

    chunks = 4
    n = D // chunks

    def w_copy(c, j):
        return pltpu.make_async_copy(
            proj_hbm.at[pl.ds(c * n, n), :, pl.ds(j * 128, 128)],
            raw.at[j, pl.ds(c * n, n)], w_sem.at[c])

    loads = [
        pltpu.make_async_copy(hid_hbm.at[:, pl.ds(0, H)], hida.at[z, 0], l_sem.at[0]),
        pltpu.make_async_copy(hid_hbm.at[:, pl.ds(H, H)], hida.at[z, 1], l_sem.at[1]),
        pltpu.make_async_copy(vw_hbm, vw, l_sem.at[2]),
        pltpu.make_async_copy(mix_hbm, mix, l_sem.at[3]),
        pltpu.make_async_copy(logz_hbm, logz, l_sem.at[4]),
        pltpu.make_async_copy(tg_hbm, targets, l_sem.at[5]),
        pltpu.make_async_copy(loss_hbm, loss, l_sem.at[6]),
    ]
    loads[0].start()
    loads[1].start()
    loads[2].start()
    for c in loads[3:]:
        c.start()
    for j in range(J):
        w_copy(0, j).start()

    bar = pltpu.get_barrier_semaphore()
    for d in range(1, M):
        pl.semaphore_signal(bar, inc=1, device_id={"tok": lax.rem(me_t + d, M)}, device_id_type=MESH)
    for d in range(1, N):
        pl.semaphore_signal(bar, inc=1, device_id={"voc": lax.rem(me_v + d, N)}, device_id_type=MESH)

    perm = mix_rows(K)

    @scoped
    def unmix(c):
        chunk = raw.at[:, pl.ds(c * n, n)]
        pltpu.make_async_copy(chunk, chunk, w_sem.at[c]).wait()
        for b in range(c * n // B, (c + 1) * n // B):
            x = jnp.concatenate(
                [raw.at[j].reshape(D * K, 128)[b * 256:(b + 1) * 256, :] for j in range(J)], axis=1)
            rows = jnp.dot(perm, x, preferred_element_type=F32).astype(BF16)
            for k in range(K):
                w[k, b * B:(b + 1) * B, :] = rows[k * B:(k + 1) * B]

    with jax.named_scope("loads"):
        for c in loads[:3]:
            c.wait()
    for c in range(1, chunks):
        for j in range(J):
            w_copy(c, j).start()
    with jax.named_scope("barrier"):
        pl.semaphore_wait(bar, M + N - 2)

    g = z % 2
    zpair = me_t + 2 - 4 * g

    def vw_rows(yy, part):
        return pl.ds(pl.multiple_of(yy * (E // 2) + part * (E // 4), E // 4), E // 4)

    def vw_send():
        for i in range(1, half):
            for c in range(2):
                v = lax.rem(chip + i, half) * 2 + c
                rows = vw_rows(y, g)
                send(vw.at[pl.ds(pl.multiple_of(v * E + rows.start, E // 4), rows.size)],
                     vwe.at[me_v, rows], vx_r.at[me_v], {"voc": v})

    @scoped
    def vw_pass():
        for i in range(1, half):
            ci = lax.rem(chip + i, half)
            for c in range(2):
                arrived(vwe.at[ci * 2 + c, vw_rows(y, g)], vx_r.at[ci * 2 + c])
            piece = vwe.at[pl.ds(ci * 2, 2), vw_rows(y, g)]
            send(piece, piece, vwz_r.at[ci], {"tok": zpair})
            send(piece, piece, vwy_r.at[ci, 0], {"tok": ypart})

    @scoped
    def vw_turn():
        for i in range(1, half):
            ci = lax.rem(chip + i, half)
            piece = vwe.at[pl.ds(ci * 2, 2), vw_rows(y, 1 - g)]
            arrived(piece, vwz_r.at[ci])
            send(piece, piece, vwy_r.at[ci, 1], {"tok": ypart})

    def hid_piece(zz, side, p):
        return hida.at[zz, side, pl.ds(p * (T // 2), T // 2)]

    vw_send()
    for p in range(2):
        piece = hid_piece(z, core, p)
        pl.when(has_r)(remote(piece, piece, own_s.at[0], hz_r.at[z, p], {"tok": me_t + 2}).start)
        pl.when(has_l)(remote(piece, piece, own_s.at[1], hz_r.at[z, p], {"tok": me_t - 2}).start)
    for c in loads[3:]:
        c.wait()
    for d in range(1, N):
        send(mix, mix_all.at[d], mix_r.at[d], {"voc": lax.rem(me_v + d, N)})
    send(vw.at[rows_of(partner, E)], vwe.at[me_v], vp_r.at[0], {"voc": partner})
    for c in range(chunks):
        unmix(c)

    def context(zz, k):
        both = jnp.dot(hida[zz, 0], w[k, 0:H, :], preferred_element_type=F32)
        both = both + jnp.dot(hida[zz, 1], w[k, H:D, :], preferred_element_type=F32)
        return jnp.tanh(both).astype(BF16)

    for k in range(K):
        with jax.named_scope("context"):
            ctx[me_v, k * T:(k + 1) * T, :] = context(z, k)
        if k == 1:
            vw_pass()
        piece = ctx.at[me_v, pl.ds(k * T, T)]
        for i in range(1, half):
            send(piece, piece, ctx_r.at[me_v, k],
                 {"voc": lax.rem(chip + i, half) * 2 + core})
        send(piece, piece, ctx_r.at[me_v, k], {"voc": partner})

    @scoped
    def add_logits(s, first=False):
        part = jnp.dot(ctx[s], vw[rows_of(s, E), :], preferred_element_type=F32)
        logit[...] = part if first else logit[...] + part

    @scoped
    def relay_hid(j, p, fwd):
        zz = mate(j)
        there, to = onward(zz)
        piece = hid_piece(zz, core, p)
        on = remote(piece, piece, on_s.at[0, j], hz_r.at[zz, p], {"tok": to})
        over = remote(piece, piece, over_s.at[0], hp_r.at[zz, p], {"voc": partner})

        @pl.when(there if fwd else jnp.logical_not(there))
        def _():
            arrived(piece, hz_r.at[zz, p])
            if fwd:
                on.start()
            over.start()

    @scoped
    def ctx_mate(j, ks):
        zz = mate(j)
        if ks[0] == 0:
            for p in range(2):
                arrived(hid_piece(zz, 1 - core, p), hp_r.at[zz, p])
        for k in ks:
            ctxz[zz, k * T:(k + 1) * T, :] = context(zz, k)

    @scoped
    def ctx_pass(k):
        for i in range(1, half):
            s = lax.rem(chip - i + half, half) * 2 + core
            piece = ctx.at[s, pl.ds(k * T, T)]
            arrived(piece, ctx_r.at[s, k])
            send(piece, piece, ctx_r.at[s, k], {"voc": partner})

    add_logits(me_v, True)
    for j in range(1, min(Z, 3)):
        relay_hid(j, 0, True)
    for k in range(K):
        arrived(ctx.at[partner, pl.ds(k * T, T)], ctx_r.at[partner, k])
    add_logits(partner)

    tcol = column(targets[...].astype(F32), V)
    ids = (me_v * V + lax.broadcasted_iota(jnp.int32, (T, V), 1)).astype(F32)
    onehot = (tcol == ids).astype(F32)
    mix_all[0] = mix[...]
    for d in range(1, N):
        arrived(mix_all.at[d], mix_r.at[d])
    mixing = jnp.zeros((K, T), F32)
    for d in range(N):
        s = lax.rem(me_v - d + N, N)
        mixing = mixing + lax.dot_general(
            mix_all[d],
            hida[z, s // half, :, pl.ds(pl.multiple_of((s % half) * E, E), E)], NT,
            preferred_element_type=F32)
    exp_mix = jnp.exp(mixing)
    weights = exp_mix / jnp.sum(exp_mix, axis=0, keepdims=True)

    for j in range(1, min(Z, 3)):
        relay_hid(j, 1, True)
    ctx_pass(0)
    if Z > 1:
        relay_hid(1, 0, False)
        relay_hid(1, 1, False)
    ctx_pass(1)
    vw_turn()
    if Z > 1:
        ctx_mate(1, range(K))
    for j in range(3, Z):
        relay_hid(j, 0, True)
    ctx_pass(2)
    for j in range(3, Z):
        relay_hid(j, 1, True)
    if Z > 2:
        relay_hid(2, 0, False)
    for k in range(3, K):
        ctx_pass(k)
    if Z > 2:
        relay_hid(2, 1, False)
    for i in range(1, half):
        add_logits(lax.rem(chip - i + half, half) * 2 + core)
    for i in range(1, half):
        s = lax.rem(chip - i + half, half) * 2 + 1 - core
        for k in range(K):
            arrived(ctx.at[s, pl.ds(k * T, T)], ctx_r.at[s, k])
        add_logits(s)

    lane = lax.broadcasted_iota(jnp.int32, (T, 128), 1)
    table = jnp.zeros((T, 128), F32)
    for k in range(K):
        part = jnp.sum(logit[k * T:(k + 1) * T, :] * onehot, axis=1, keepdims=True)
        table = jnp.where(lane == k, part, table)
    tgt[0] = table.T[0:8, :]
    for d in range(1, N):
        send(tgt.at[0], tgt.at[d], tgt_r.at[d], {"voc": lax.rem(me_v + d, N)})
    @scoped
    def scales():
        for d in range(1, N):
            arrived(tgt.at[d], tgt_r.at[d])
        target = tgt[0]
        for d in range(1, N):
            target = target + tgt[d]
        likely = jnp.exp(target[0:K, :] - logz[...])
        joint = weights * likely
        posterior = joint / jnp.sum(joint, axis=0, keepdims=True)
        scale[z, 0:K, :] = loss[...] * posterior
        mgrad[...] = loss[...] * (weights - posterior)
        for d in range(1, Z):
            send(scale.at[z], scale.at[z], sc_r.at[z], {"tok": lax.rem(me_t + 2 * d, M)})

    def shares(zz, k):
        piece = lgall.at[zz, me_v, k]
        return [
            remote(piece, piece, over_s.at[1], lg_r.at[zz, chip, k],
                   {"voc": lax.rem(chip + i, half) * 2 + core})
            for i in range(1, half)
        ] + [remote(piece, piece, over_s.at[2], ld_r.at[zz, k], {"voc": partner})]

    def share(zz, k):
        for c in shares(zz, k):
            c.start()

    @scoped
    def own_out(k):
        rows = slice(k * T, (k + 1) * T)
        logit[rows, :] = jnp.exp(logit[rows, :] - column(logz[k:k + 1, :], V)) - onehot
        lgall[z, me_v, k] = logit[rows, :].astype(BF16)

    @scoped
    def own_share(k):
        share(z, k)

    @scoped
    def own_line(k):
        piece = lgall.at[z, me_v, k]
        pl.when(has_r)(remote(piece, piece, own_s.at[0], lg_r.at[z, chip, k], {"tok": me_t + 2}).start)
        pl.when(has_l)(remote(piece, piece, own_s.at[1], lg_r.at[z, chip, k], {"tok": me_t - 2}).start)
        if k == 0:
            for way, end in ((0, 0), (1, Z - 1)):
                far = remote(piece, piece, own_s.at[2 + way], lg_r.at[z, chip, k],
                             {"tok": me_t + (1 - 2 * way) * (M - 2)})
                pl.when(z == end)(far.start)

    def near_end(zz, there, to):
        end = to // 2
        return there & (end - zz < Z - 1) & (zz - end < Z - 1)

    @scoped
    def relay_lg(k, j, fwd):
        zz = mate(j)
        there, to = onward(zz)
        if k == 0:
            there = near_end(zz, there, to)
        piece = lgall.at[zz, me_v, k]
        on = remote(piece, piece, on_s.at[1 if k == 0 else 0, j], lg_r.at[zz, chip, k], {"tok": to})

        @pl.when(there if fwd else jnp.logical_not(there))
        def _():
            arrived(piece, lg_r.at[zz, chip, k])
            if fwd:
                on.start()
            share(zz, k)

    @scoped
    def cross_lg(k, j):
        zz = mate(j)
        for i in range(1, half):
            s = lax.rem(chip - i + half, half) * 2 + core
            piece = lgall.at[zz, s, k]
            arrived(piece, lg_r.at[zz, s // 2, k])
            remote(piece, piece, over_s.at[3], ld_r.at[zz, k], {"voc": partner}).start()

    @scoped
    def pre_grad(k, j):
        zz = mate(j)
        rows = slice(k * T, (k + 1) * T)
        arrived(lgall.at[zz, 0:half, k], ld_r.at[zz, k])
        total = None
        for s in range(N):
            part = jnp.dot(lgall[zz, s, k], vwt[s], preferred_element_type=F32)
            total = part if total is None else total + part
        c = (ctx[me_v, rows, :] if j == 0 else ctxz[zz, rows, :]).astype(F32)
        if k == 0:
            if j > 0:
                arrived(scale.at[zz], sc_r.at[zz])
        total = total * column(scale[zz, k:k + 1, :], E)
        pg[k, rows_of(zz, T), :] = (total * (1.0 - c * c)).astype(BF16)

    def hid_part(s):
        total = jnp.zeros((T, E), F32)
        for k in range(K):
            total = total + lax.dot_general(
                pg[k, rows_of(z, T), :], w[k, rows_of(s, E), :], NT,
                preferred_element_type=F32)
        return total

    @scoped
    def hid_send(d):
        s = lax.rem(me_v + d, N)
        if d == 0:
            own_hs[...] = hid_part(s)
        else:
            hss[d] = hid_part(s).astype(BF16)
            send(hss.at[d], hsr.at[d], hs_r.at[d], {"voc": s})

    @scoped
    def pair_sums():
        for d in list(range(1, Z)) + [0]:
            zz = lax.rem(z + d, Z)
            arrived(vgy.at[zz], vy_r.at[zz])
            total = vgb[rows_of(zz * 2 + y, R), :].astype(F32) + vgy[zz].astype(F32)
            if d == 0:
                vsum[...] = total
            else:
                vout[zz] = total.astype(BF16)
                send(vout.at[zz], vin.at[z], vz_r.at[z], {"tok": zz * 2 + y})

    pieces = [(k, 0, E) for k in range(K)]
    if E % 256 == 0:
        pieces[-1:] = [(K - 1, 0, E // 2), (K - 1, E // 2, E // 2)]

    @scoped
    def proj_part(k):
        for p, (kk, lo, wide) in enumerate(pieces):
            if kk == k:
                lanes = slice(lo, lo + wide)
                psend[k, :, lanes] = jnp.dot(
                    htr[1 - y], pg[k, :, lanes], preferred_element_type=F32).astype(BF16)
                send(psend.at[k, :, pl.ds(lo, wide)], precv.at[k, :, pl.ds(lo, wide)],
                     pp_r.at[p], {"tok": ypart})
        acc[k] = jnp.dot(htr[y], pg[k], preferred_element_type=F32)

    @scoped
    def vocab_part():
        for k in range(K):
            rows = slice(k * T, (k + 1) * T)
            lg[rows, :] = (column(scale[z, k:k + 1, :], V) * logit[rows, :]).astype(BF16)
        for part in range(0, N, half):
            for s in range(part, part + half):
                vgb[s * E:(s + 1) * E, :] = lax.dot_general(
                    ctx[s], lg[...], TN, preferred_element_type=F32).astype(BF16)
            for zz in range(part * Z // N, (part + half) * Z // N):
                send(vgb.at[pl.ds((zz * 2 + 1 - y) * R, R)], vgy.at[zz], vy_r.at[zz], {"tok": ypart})

    @scoped
    def vw_done():
        vwe[me_v] = vw[rows_of(me_v, E), :]
        arrived(vwe.at[partner], vp_r.at[0])
        for i in range(1, half):
            ci = lax.rem(chip + i, half)
            for p, part in enumerate((g, 1 - g)):
                arrived(vwe.at[pl.ds(ci * 2, 2), vw_rows(1 - y, part)], vwy_r.at[ci, p])
        for s in range(N):
            vwt[s] = vwe[s].T

    @scoped
    def turn():
        for b in range(2):
            col = (z * 2 + b) * R
            for zz in range(Z):
                htr[b, :, zz * T:(zz + 1) * T] = hida[
                    zz, col // H, :, pl.ds(pl.multiple_of(col % H, R), R)].T

    def relay_on(k, j):
        relay_lg(k, j, True)

    def relay_in(k, j):
        relay_lg(k, j, False)

    def mate_ctx(j):
        ctx_mate(j, range(K))

    def hid_in(j, p):
        relay_hid(j, p, False)

    steps = (own_out, own_share, own_line, relay_on, relay_in, cross_lg, pre_grad, proj_part,
             scales, vocab_part, mate_ctx, hid_in, vw_done, turn, hid_send, pair_sums)
    for step, *rest in ORDER:
        steps[step](*rest)

    vtot = vsum[...]
    for d in range(1, Z):
        zz = lax.rem(z + d, Z)
        arrived(vin.at[zz], vz_r.at[zz])
        vtot = vtot + vin[zz].astype(F32)
    out_vocab[...] = vtot.astype(BF16)
    htot = own_hs[...]
    for d in range(1, N):
        arrived(hsr.at[d], hs_r.at[d])
        htot = htot + hsr[d].astype(F32)
    mixf = mix[...].astype(F32)
    for k in range(K):
        htot = htot + column(mgrad[k:k + 1, :], E) * mixf[k:k + 1, :]
    out_hidden[...] = htot.astype(BF16)

    back = mix_rows(K, True)
    for p, (k, lo, wide) in enumerate(pieces):
        lanes = slice(lo, lo + wide)
        with jax.named_scope("precv"):
            arrived(precv.at[k, :, pl.ds(lo, wide)], pp_r.at[p])
        psum = (acc[k, :, lanes] + precv[k, :, lanes].astype(F32)).astype(BF16)
        if k < K - 1:
            precv[k, :, lanes] = psum
            continue
        for b in range(R // B):
            rows = slice(b * B, (b + 1) * B)
            x = jnp.concatenate([precv[q, rows, lanes] for q in range(K - 1)] + [psum[rows]], axis=0)
            out = jnp.dot(back, x, preferred_element_type=F32).astype(BF16)
            for j in range(wide // 128):
                out_proj.at[lo // 128 + j].reshape(R * K, 128)[b * 256:(b + 1) * 256, :] = (
                    out[:, j * 128:(j + 1) * 128])
    with jax.named_scope("drain"):
        for i, size in enumerate(groups):
            sent(all_s.at[i], size)
        piece = T * V * 2
        sent(over_s.at[0], (Z - 1) * T * D)
        for i in range(1, 4):
            for _ in range(half - 1):
                sent(over_s.at[i], Z * K * piece)
        for way, pred in ((0, has_r), (1, has_l)):
            pl.when(pred)(functools.partial(sent, own_s.at[way], T * D + K * piece))
        for way, end in ((0, 0), (1, Z - 1)):
            pl.when(z == end)(functools.partial(sent, own_s.at[2 + way], piece))
        for j in range(1, Z):
            zz = mate(j)
            there, to = onward(zz)
            pl.when(there)(functools.partial(sent, on_s.at[0, j], T * D + (K - 1) * piece))
            pl.when(near_end(zz, there, to))(functools.partial(sent, on_s.at[1, j], piece))


def body_fast(M, N, hidden, mix_weight, comp_proj, vocab_weight, log_normalizer, targets, loss_grad):
    T, D = hidden.shape
    K, E = mix_weight.shape
    V = vocab_weight.shape[1]
    R = D // M
    J = E // 128
    half = N // 2
    Z = M // 2
    vm = pltpu.VMEM
    dma = pltpu.SemaphoreType.DMA
    scratch = [
        vm((J, D, K, 128), BF16), vm((K, D, E), BF16), vm((Z, 2, T, D // 2), BF16), vm((D, V), BF16),
        vm((N, E, V), BF16), vm((N, V, E), BF16), vm((K, E), BF16), vm((K, T), F32), vm((1, T), jnp.int32), vm((1, T), F32),
        vm((N, K * T, E), BF16), vm((Z, K * T, E), BF16), vm((N, K, E), BF16), vm((2, R, Z * T), BF16),
        vm((K * T, V), F32), vm((K * T, V), BF16), vm((Z, N, K, T, V), BF16), vm((N, 8, T), F32), vm((Z, 8, T), F32), vm((K, Z * T, E), BF16),
        vm((D, V), BF16), vm((Z, R, V), BF16),
        vm((R, V), F32), vm((Z, R, V), BF16), vm((Z, R, V), BF16),
        vm((N, T, E), BF16), vm((N, T, E), BF16),
        vm((T, E), F32), vm((K, R, E), F32), vm((K, R, E), BF16), vm((K, R, E), BF16),
        vm((K, T), F32),
        dma((7,)), dma((4,)), dma((8,)), dma((4,)), dma((4,)), dma((2, Z)),
        dma((N, K)), dma((N,)), dma((Z, 2)), dma((Z, 2)), dma((N,)), dma((1,)), dma((half,)), dma((half, 2)),
        dma((N,)), dma((Z, half, K)), dma((Z, K)), dma((Z,)), dma((Z,)), dma((N,)), dma((K + 1,)), dma((Z,)),
    ]
    spec = pl.BlockSpec(memory_space=pltpu.VMEM)
    hbm = pl.BlockSpec(memory_space=pltpu.MemorySpace.HBM)
    hid, proj, voc = pl.pallas_call(
        functools.partial(fast_kernel, M, N),
        out_shape=(
            jax.ShapeDtypeStruct((T, E), BF16),
            jax.ShapeDtypeStruct((J, R, K, 128), BF16),
            jax.ShapeDtypeStruct((R, V), BF16),
        ),
        in_specs=[hbm] * 7,
        out_specs=(spec, spec, spec),
        scratch_shapes=scratch,
        compiler_params=pltpu.CompilerParams(
            collective_id=0, has_side_effects=True, vmem_limit_bytes=47 * 1024 * 1024
        ),
    )(*[
        pltpu.with_memory_space_constraint(x, pltpu.MemorySpace.HBM)
        for x in (hidden, mix_weight, comp_proj, vocab_weight, log_normalizer, targets[None, :], loss_grad[None, :])
    ])
    return pl.pallas_call(
        store_kernel,
        out_shape=(
            jax.ShapeDtypeStruct((T, E), BF16),
            jax.ShapeDtypeStruct((R, K, E), BF16),
            jax.ShapeDtypeStruct((R, V), BF16),
        ),
        in_specs=[spec] * 3,
        out_specs=(hbm, hbm, hbm),
        scratch_shapes=[dma((J + 2,))],
        compiler_params=pltpu.CompilerParams(vmem_limit_bytes=4 * 1024 * 1024),
    )(hid, proj, voc)


def store_kernel(hid, proj, voc, out_hid, out_proj, out_voc, sem):
    J = proj.shape[0]
    copies = [pltpu.make_async_copy(hid, out_hid, sem.at[J]), pltpu.make_async_copy(voc, out_voc, sem.at[J + 1])]
    for j in range(J):
        copies.append(pltpu.make_async_copy(proj.at[j], out_proj.at[:, :, pl.ds(j * 128, 128)], sem.at[j]))
    for c in copies:
        c.start()
    for c in copies:
        c.wait()


def body(M, N, *args):
    hidden, mix_weight, comp_proj, vocab_weight = args[:4]
    T, D = hidden.shape
    K, E = mix_weight.shape
    V = vocab_weight.shape[1]
    gathered = 2 * (M // 2) * T * (K * N * V + D + 2 * K * E)
    shapes = K == 4 and M == 8 and N == 4 and E % 128 == 0 and (D // M) % (256 // K) == 0
    if shapes and gathered + 4 * K * D * E <= 28 * 1024 * 1024:
        return body_fast(M, N, *args)
    return body_base(M, N, *args)


def solution(mesh):
    in_specs = (
        P("tok", None),
        P(None, "voc"),
        P(None, None, "voc"),
        P(None, "voc"),
        P(None, "tok"),
        P("tok"),
        P("tok"),
    )
    out_specs = (P("tok", "voc"), P("tok", None, "voc"), P("tok", "voc"))
    return jax.shard_map(
        functools.partial(body, mesh.shape["tok"], mesh.shape["voc"]),
        mesh=mesh, in_specs=in_specs, out_specs=out_specs, check_vma=False,
    )
```

```python
import functools
import math

import jax
import jax.numpy as jnp
from jax import lax
from jax.experimental import pallas as pl
from jax.experimental.pallas import tpu as pltpu
from jax.sharding import PartitionSpec as P

MESH = pl.DeviceIdType.MESH
F32 = jnp.float32
BF16 = jnp.bfloat16
NT = (((1,), (1,)), ((), ()))
TN = (((0,), (0,)), ((), ()))


def column(row, lanes):
    wide = jnp.broadcast_to(row, (128, row.shape[1])).T
    return jnp.concatenate([wide] * (lanes // 128), axis=1)


def kernel(
    M, N,
    hidden, mix, proj_hbm, vw, logz, targets, loss,
    out_hidden, out_proj, out_vocab,
    w, ctx, mix_all, hblk, hrow, htr, logit, lg, tgt,
    cgs, cgr, cgx, xr, own_cg, vgb, vgy, vsum, vout, vin, pg, hss, hsr, own_hs, acc, psend, precv, mgrad,
    w_sem, ctx_s, ctx_f, ctx_r, mix_s, mix_r, hid_s, hid_r, tgt_s, tgt_r,
    cgp_s, cgp_r, cgx_s, cgx_r, vy_s, vy_r, vz_s, vz_r, hs_s, hs_r, ag_s, ag_r, pp_s, pp_r,
):
    K, D, E = w.shape
    T = hidden.shape[0]
    V = vw.shape[1]
    R = D // M
    half = N // 2
    Z = M // 2
    me_t = lax.axis_index("tok")
    me_v = lax.axis_index("voc")
    chip = me_v // 2
    core = me_v % 2
    partner = me_v + 1 - 2 * core
    z = me_t // 2
    y = me_t % 2
    ypart = me_t + 1 - 2 * y
    sends = []

    def remote(src, dst, ss, rs, dev):
        return pltpu.make_async_remote_copy(
            src_ref=src, dst_ref=dst, send_sem=ss, recv_sem=rs,
            device_id=dev, device_id_type=MESH,
        )

    def send(src, dst, ss, rs, dev):
        c = remote(src, dst, ss, rs, dev)
        c.start()
        sends.append((None, c))

    def arrived(ref, rs, ss):
        remote(ref, ref, ss, rs, {"voc": partner}).wait_recv()

    for k in range(K):
        pltpu.make_async_copy(proj_hbm.at[k], w.at[k], w_sem.at[k]).start()
    for j in range(M):
        hblk[j // 2, j % 2] = hidden[:, j * R:(j + 1) * R]

    bar = pltpu.get_barrier_semaphore()
    for d in range(1, M):
        pl.semaphore_signal(bar, inc=1, device_id={"tok": lax.rem(me_t + d, M)}, device_id_type=MESH)
    for d in range(1, N):
        pl.semaphore_signal(bar, inc=1, device_id={"voc": lax.rem(me_v + d, N)}, device_id_type=MESH)
    pl.semaphore_wait(bar, M + N - 2)

    for d in range(1, N):
        send(mix, mix_all.at[d], mix_s.at[d], mix_r.at[d], {"voc": lax.rem(me_v + d, N)})
    mix_all[0] = mix[...]
    for d in range(1, Z):
        zz = lax.rem(z + d, Z)
        send(hblk.at[zz], hrow.at[:, pl.ds(z * T, T)], hid_s.at[d], hid_r.at[d],
             {"tok": zz * 2 + y})
    hrow[:, rows_of(z, T), :] = hblk[z]

    for k in range(K):
        pltpu.make_async_copy(proj_hbm.at[k], w.at[k], w_sem.at[k]).wait()
        ctx[me_v, k * T:(k + 1) * T, :] = jnp.tanh(
            jnp.dot(hidden[...], w[k], preferred_element_type=F32)
        ).astype(BF16)
        piece = ctx.at[me_v, pl.ds(k * T, T)]
        for i in range(1, half):
            send(piece, piece, ctx_s.at[i, k], ctx_r.at[me_v, k],
                 {"voc": lax.rem(chip + i, half) * 2 + core})
        send(piece, piece, ctx_s.at[0, k], ctx_r.at[me_v, k], {"voc": partner})

    def add_logits(s, first=False):
        part = jnp.dot(ctx[s], vw[pl.ds(pl.multiple_of(s * E, E), E), :],
                       preferred_element_type=F32)
        logit[...] = part if first else logit[...] + part

    add_logits(me_v, True)
    for k in range(K):
        arrived(ctx.at[partner, pl.ds(k * T, T)], ctx_r.at[partner, k], ctx_s.at[0, k])
    add_logits(partner)

    tcol = column(targets[...].astype(F32), V)
    ids = (me_v * V + lax.broadcasted_iota(jnp.int32, (T, V), 1)).astype(F32)
    onehot = (tcol == ids).astype(F32)
    for d in range(1, N):
        arrived(mix_all.at[d], mix_r.at[d], mix_s.at[d])
    mixing = jnp.zeros((K, T), F32)
    for d in range(N):
        s = lax.rem(me_v - d + N, N)
        mixing = mixing + lax.dot_general(
            mix_all[d], hidden[:, pl.ds(pl.multiple_of(s * E, E), E)], NT,
            preferred_element_type=F32)
    exp_mix = jnp.exp(mixing)
    weights = exp_mix / jnp.sum(exp_mix, axis=0, keepdims=True)

    for i in range(1, half):
        s = lax.rem(chip - i + half, half) * 2 + core
        for k in range(K):
            piece = ctx.at[s, pl.ds(k * T, T)]
            arrived(piece, ctx_r.at[s, k], ctx_s.at[i, k])
            send(piece, piece, ctx_f.at[i, k], ctx_r.at[s, k], {"voc": partner})
        add_logits(s)
    for i in range(1, half):
        s = lax.rem(chip - i + half, half) * 2 + 1 - core
        for k in range(K):
            arrived(ctx.at[s, pl.ds(k * T, T)], ctx_r.at[s, k], ctx_s.at[i, k])
        add_logits(s)

    lane = lax.broadcasted_iota(jnp.int32, (T, 128), 1)
    table = jnp.zeros((T, 128), F32)
    for k in range(K):
        part = jnp.sum(logit[k * T:(k + 1) * T, :] * onehot, axis=1, keepdims=True)
        table = jnp.where(lane == k, part, table)
    tgt[0] = table.T[0:8, :]
    for d in range(1, N):
        send(tgt.at[0], tgt.at[d], tgt_s.at[d], tgt_r.at[d], {"voc": lax.rem(me_v + d, N)})
    for k in range(K):
        rows = slice(k * T, (k + 1) * T)
        logit[rows, :] = jnp.exp(logit[rows, :] - column(logz[k:k + 1, :], V)) - onehot
    for d in range(1, N):
        arrived(tgt.at[d], tgt_r.at[d], tgt_s.at[d])
    target = tgt[0]
    for d in range(1, N):
        target = target + tgt[d]
    likely = jnp.exp(target[0:K, :] - logz[...])
    joint = weights * likely
    posterior = joint / jnp.sum(joint, axis=0, keepdims=True)
    factor = loss[...] * posterior
    mgrad[...] = loss[...] * (weights - posterior)
    for k in range(K):
        rows = slice(k * T, (k + 1) * T)
        lg[rows, :] = (column(factor[k:k + 1, :], V) * logit[rows, :]).astype(BF16)

    def cg_part(s, k):
        return lax.dot_general(
            lg[k * T:(k + 1) * T, :], vw[pl.ds(pl.multiple_of(s * E, E), E), :], NT,
            preferred_element_type=F32)

    for i in list(range(1, half)) + [0]:
        s = lax.rem(chip + i, half) * 2
        for k in range(K):
            cgs[i, k] = cg_part(s + 1 - core, k).astype(BF16)
            send(cgs.at[i, k], cgr.at[i, k], cgp_s.at[i, k], cgp_r.at[i, k], {"voc": partner})
        for k in range(K):
            part = cg_part(s + core, k)
            if i == 0:
                own_cg[k] = part
            else:
                arrived(cgr.at[i, k], cgp_r.at[i, k], cgp_s.at[i, k])
                cgx[i, k] = (part + cgr[i, k].astype(F32)).astype(BF16)
                send(cgx.at[i, k], xr.at[i, k], cgx_s.at[i, k], cgx_r.at[i, k], {"voc": s + core})

    for s in range(N):
        vgb[s * E:(s + 1) * E, :] = lax.dot_general(
            ctx[s], lg[...], TN, preferred_element_type=F32).astype(BF16)
    for zz in range(Z):
        send(vgb.at[pl.ds((zz * 2 + 1 - y) * R, R)], vgy.at[zz], vy_s.at[zz], vy_r.at[zz],
             {"tok": ypart})

    for d in range(1, Z):
        src = lax.rem(z - d + Z, Z)
        arrived(hrow.at[:, pl.ds(src * T, T)], hid_r.at[d], hid_s.at[d])
    for b in range(2):
        htr[b] = hrow[b].T

    pieces = [(k, 0, E) for k in range(K)]
    if E % 256 == 0:
        pieces[-1:] = [(K - 1, 0, E // 2), (K - 1, E // 2, E // 2)]

    def relay(t, p, way, pred):
        k, lo, wide = pieces[p]
        piece = pg.at[k, rows_of(t, T), pl.ds(lo, wide)]
        c = remote(piece, piece, ag_s.at[way, t, p], ag_r.at[t, p],
                   {"tok": me_t + 2 - 4 * way})
        pl.when(pred)(c.start)
        sends.append((pred, c))

    has_r = z + 1 < Z
    has_l = z >= 1
    for k in range(K):
        total = own_cg[k]
        arrived(cgr.at[0, k], cgp_r.at[0, k], cgp_s.at[0, k])
        total = total + cgr[0, k].astype(F32)
        for i in range(1, half):
            arrived(xr.at[i, k], cgx_r.at[i, k], cgx_s.at[i, k])
            total = total + xr[i, k].astype(F32)
        c = ctx[me_v, k * T:(k + 1) * T, :].astype(F32)
        pg[k, rows_of(z, T), :] = (total * (1.0 - c * c)).astype(BF16)
        if Z > 1:
            for p in range(len(pieces)):
                if pieces[p][0] == k:
                    relay(z, p, 0, has_r)
                    relay(z, p, 1, has_l)

    def hid_part(s):
        total = jnp.zeros((T, E), F32)
        for k in range(K):
            total = total + lax.dot_general(
                pg[k, rows_of(z, T), :], w[k, pl.ds(pl.multiple_of(s * E, E), E), :], NT,
                preferred_element_type=F32)
        return total

    def hid_send(d):
        s = lax.rem(me_v + d, N)
        if d == 0:
            own_hs[...] = hid_part(s)
        else:
            hss[d] = hid_part(s).astype(BF16)
            send(hss.at[d], hsr.at[d], hs_s.at[d], hs_r.at[d], {"voc": s})

    hid_order = list(range(1, N)) + [0]
    hid_per = -(-N // (len(pieces) - 1))

    def pair_sums():
        for zz in range(Z):
            arrived(vgy.at[zz], vy_r.at[zz], vy_s.at[zz])
            vsum[zz] = vgb[rows_of(zz * 2 + y, R), :].astype(F32) + vgy[zz].astype(F32)

    def hop(h):
        for way, at, ends in ((0, h, range(h + 1, Z)), (1, Z - 1 - h, range(Z - 1 - h))):
            copies = [
                remote(vout.at[way, e], vin.at[way, e], vz_s.at[way, e], vz_r.at[way, e],
                       {"tok": me_t + 2 - 4 * way})
                for e in ends
            ]

            @pl.when(z == at)
            def _(way=way, ends=ends, copies=copies):
                for e, c in zip(ends, copies):
                    part = vsum[e]
                    if h > 0:
                        arrived(vin.at[way, e], vz_r.at[way, e], vz_s.at[way, e])
                        part = part + vin[way, e].astype(F32)
                    vout[way, e] = part.astype(BF16)
                    c.start()
            for c in copies:
                sends.append((z == at, c))

    if Z == 1:
        for e in hid_order:
            hid_send(e)
    per = -(-(Z - 1) // (len(pieces) - 1))
    for p, (k, lo, wide) in enumerate(pieces):
        lanes = slice(lo, lo + wide)
        for d in range(1, Z):
            for there, t, way, more in (
                (z >= d, z - d, 0, has_r), (z + d < Z, z + d, 1, has_l),
            ):
                def _(t=t):
                    arrived(pg.at[k, rows_of(t, T), pl.ds(lo, wide)], ag_r.at[t, p], ag_s.at[0, t, p])
                pl.when(there)(_)
                if d < Z - 1:
                    relay(t, p, way, there & more)
            if d == 1:
                for e in hid_order[p * hid_per:(p + 1) * hid_per]:
                    hid_send(e)
        psend[k, :, lanes] = jnp.dot(
            htr[1 - y], pg[k, :, lanes], preferred_element_type=F32).astype(BF16)
        send(psend.at[k, :, pl.ds(lo, wide)], precv.at[k, :, pl.ds(lo, wide)],
             pp_s.at[p], pp_r.at[p], {"tok": ypart})
        acc[k, :, lanes] = jnp.dot(htr[y], pg[k, :, lanes], preferred_element_type=F32)
        if p == 0:
            pair_sums()
        for h in range(p * per, min((p + 1) * per, Z - 1)):
            hop(h)

    acc_v = vsum.at[z]
    for way, pred in ((0, has_l), (1, has_r)):
        @pl.when(pred)
        def _(way=way):
            arrived(vin.at[way, z], vz_r.at[way, z], vz_s.at[way, z])
            acc_v[...] += vin[way, z].astype(F32)
    out_vocab[...] = acc_v[...].astype(BF16)
    htot = own_hs[...]
    for d in range(1, N):
        arrived(hsr.at[d], hs_r.at[d], hs_s.at[d])
        htot = htot + hsr[d].astype(F32)
    mixf = mix[...].astype(F32)
    for k in range(K):
        htot = htot + column(mgrad[k:k + 1, :], E) * mixf[k:k + 1, :]
    out_hidden[...] = htot.astype(BF16)

    for p, (k, lo, wide) in enumerate(pieces):
        lanes = slice(lo, lo + wide)
        arrived(precv.at[k, :, pl.ds(lo, wide)], pp_r.at[p], pp_s.at[p])
        out_proj[k, :, lanes] = (acc[k, :, lanes] + precv[k, :, lanes].astype(F32)).astype(BF16)
    for pred, c in sends:
        if pred is None:
            c.wait_send()
        else:
            pl.when(pred)(c.wait_send)


def rows_of(block, size):
    return pl.ds(pl.multiple_of(block * size, size), size)


def body_base(M, N, hidden, mix_weight, comp_proj, vocab_weight, log_normalizer, targets, loss_grad):
    T, D = hidden.shape
    K, E = mix_weight.shape
    V = vocab_weight.shape[1]
    R = D // M
    half = N // 2
    Z = M // 2
    w = jnp.transpose(comp_proj, (1, 0, 2))
    vm = pltpu.VMEM
    dma = pltpu.SemaphoreType.DMA
    scratch = [
        vm((K, D, E), BF16), vm((N, K * T, E), BF16), vm((N, K, E), BF16),
        vm((Z, 2, T, R), BF16), vm((2, Z * T, R), BF16), vm((2, R, Z * T), BF16), vm((K * T, V), F32), vm((K * T, V), BF16),
        vm((N, 8, T), F32),
        vm((half, K, T, E), BF16), vm((half, K, T, E), BF16),
        vm((half, K, T, E), BF16), vm((half, K, T, E), BF16),
        vm((K, T, E), F32), vm((D, V), BF16), vm((Z, R, V), BF16),
        vm((Z, R, V), F32), vm((2, Z, R, V), BF16), vm((2, Z, R, V), BF16),
        vm((K, Z * T, E), BF16), vm((N, T, E), BF16), vm((N, T, E), BF16),
        vm((T, E), F32), vm((K, R, E), F32), vm((K, R, E), BF16), vm((K, R, E), BF16),
        vm((K, T), F32),
        dma((K,)), dma((half, K)), dma((half, K)), dma((N, K)), dma((N,)), dma((N,)),
        dma((Z,)), dma((Z,)), dma((N,)), dma((N,)),
        dma((half, K)), dma((half, K)), dma((half, K)), dma((half, K)),
        dma((Z,)), dma((Z,)), dma((2, Z)), dma((2, Z)), dma((N,)), dma((N,)),
        dma((2, Z, K + 1)), dma((Z, K + 1)), dma((K + 1,)), dma((K + 1,)),
    ]
    spec = pl.BlockSpec(memory_space=pltpu.VMEM)
    hidden_grad, proj_grad, vocab_grad = pl.pallas_call(
        functools.partial(kernel, M, N),
        out_shape=(
            jax.ShapeDtypeStruct((T, E), BF16),
            jax.ShapeDtypeStruct((K, R, E), BF16),
            jax.ShapeDtypeStruct((R, V), BF16),
        ),
        in_specs=[spec, spec, pl.BlockSpec(memory_space=pltpu.MemorySpace.HBM)] + [spec] * 4,
        out_specs=(spec, spec, spec),
        scratch_shapes=scratch,
        compiler_params=pltpu.CompilerParams(
            collective_id=0, has_side_effects=True, vmem_limit_bytes=48 * 1024 * 1024
        ),
    )(hidden, mix_weight, w, vocab_weight, log_normalizer, targets[None, :], loss_grad[None, :])
    return hidden_grad, jnp.transpose(proj_grad, (1, 0, 2)), vocab_grad


ORDER = (
    (0, 0), (1, 0), (2, 0), (0, 1), (0, 2), (1, 1), (1, 2), (2, 1), (0, 3), (12,), (8,), (3, 0, 1), (9,),
    (1, 3), (10, 2), (3, 0, 2), (4, 0, 1), (11, 3, 1), (2, 2), (5, 0, 0), (3, 1, 1), (4, 0, 3), (11, 3, 0),
    (5, 2, 0), (4, 0, 2), (3, 1, 2), (5, 1, 0), (6, 0, 0), (3, 0, 3), (2, 3), (5, 0, 1), (4, 2, 1),
    (10, 3), (4, 1, 1), (3, 1, 3), (3, 2, 1), (5, 0, 3), (5, 0, 2), (6, 0, 1), (4, 1, 2), (5, 3, 0),
    (3, 2, 2), (13,), (6, 2, 0), (3, 3, 1), (6, 0, 3), (6, 0, 2), (7, 0), (4, 1, 3), (4, 2, 2), (3, 2, 3),
    (5, 1, 2), (5, 1, 1), (3, 3, 2), (6, 1, 0), (4, 3, 1), (5, 1, 3), (6, 1, 1), (6, 1, 2), (4, 2, 3),
    (3, 3, 3), (6, 3, 0), (6, 1, 3), (7, 1), (5, 2, 1), (4, 3, 2), (5, 2, 2), (4, 3, 3), (5, 3, 1),
    (6, 2, 1), (5, 2, 3), (6, 3, 1), (6, 2, 2), (5, 3, 2), (14, 2), (15,), (6, 2, 3), (5, 3, 3), (7, 2),
    (6, 3, 2), (6, 3, 3), (7, 3), (14, 3), (14, 0), (14, 1),
)


def scoped(fn):
    def run(*args, **kw):
        tag = "_".join(str(a) for a in args if isinstance(a, int))
        with jax.named_scope(fn.__name__ + "_" + tag):
            return fn(*args, **kw)
    return run


def mix_rows(K, flip=False):
    B = 256 // K
    r = lax.broadcasted_iota(jnp.int32, (256, 256), 1 if flip else 0)
    c = lax.broadcasted_iota(jnp.int32, (256, 256), 0 if flip else 1)
    return (c == K * (r % B) + r // B).astype(F32).astype(BF16)


def fast_kernel(
    M, N,
    hid_hbm, mix_hbm, proj_hbm, vw_hbm, logz_hbm, tg_hbm, loss_hbm,
    out_hidden, out_proj, out_vocab,
    raw, w, hida, vw, vwe, vwt, mix, logz, targets, loss,
    ctx, ctxz, mix_all, htr, logit, lg, lgall, tgt, scale, pg,
    vgb, vgy, vsum, vout, vin, hss, hsr, own_hs, acc, psend, precv, mgrad,
    l_sem, w_sem, all_s, over_s, own_s, on_s,
    ctx_r, ctd_r, mix_r, hz_r, hp_r, vx_r, vp_r, vwz_r, vwy_r,
    tgt_r, lg_r, ld_r, vy_r, vz_r, hs_r, pp_r, sc_r,
):
    K, D, E = w.shape
    T = hida.shape[2]
    H = D // 2
    V = vw.shape[1]
    R = D // M
    J = E // 128
    half = N // 2
    Z = M // 2
    B = 256 // K
    me_t = lax.axis_index("tok")
    me_v = lax.axis_index("voc")
    chip = me_v // 2
    core = me_v % 2
    partner = me_v + 1 - 2 * core
    z = me_t // 2
    y = me_t % 2
    ypart = me_t + 1 - 2 * y
    has_r = z + 1 < Z
    has_l = z >= 1

    def remote(src, dst, ss, rs, dev):
        return pltpu.make_async_remote_copy(
            src_ref=src, dst_ref=dst, send_sem=ss, recv_sem=rs,
            device_id=dev, device_id_type=MESH,
        )

    groups = [0]

    def send(src, dst, rs, dev):
        size = math.prod(src.shape) * jnp.dtype(src.dtype).itemsize
        if groups[-1] + size > D * K * 256:
            groups.append(0)
        groups[-1] += size
        remote(src, dst, all_s.at[len(groups) - 1], rs, dev).start()

    def sent(sem, size):
        ref = raw.at[0, pl.ds(0, size // (K * 256))]
        remote(ref, ref, sem, vp_r.at[0], {"voc": partner}).wait_send()

    def arrived(ref, rs):
        remote(ref, ref, all_s.at[0], rs, {"voc": partner}).wait_recv()

    def mate(j):
        if j == 0:
            return z
        near = jnp.minimum(z, Z - 1 - z)
        d = (j + 1) // 2
        both = z + d if j % 2 == 1 else z - d
        return jnp.where(j <= 2 * near, both, jnp.where(2 * z < Z, j, Z - 1 - j))

    def onward(zz):
        right = zz < z
        there = (right & has_r) | (jnp.logical_not(right) & has_l)
        return there, me_t + jnp.where(right, 2, -2)

    chunks = 4
    n = D // chunks

    def w_copy(c, j):
        return pltpu.make_async_copy(
            proj_hbm.at[pl.ds(c * n, n), :, pl.ds(j * 128, 128)],
            raw.at[j, pl.ds(c * n, n)], w_sem.at[c])

    loads = [
        pltpu.make_async_copy(hid_hbm.at[:, pl.ds(0, H)], hida.at[z, 0], l_sem.at[0]),
        pltpu.make_async_copy(hid_hbm.at[:, pl.ds(H, H)], hida.at[z, 1], l_sem.at[1]),
        pltpu.make_async_copy(vw_hbm, vw, l_sem.at[2]),
        pltpu.make_async_copy(mix_hbm, mix, l_sem.at[3]),
        pltpu.make_async_copy(logz_hbm, logz, l_sem.at[4]),
        pltpu.make_async_copy(tg_hbm, targets, l_sem.at[5]),
        pltpu.make_async_copy(loss_hbm, loss, l_sem.at[6]),
    ]
    loads[0].start()
    loads[1].start()
    loads[2].start()
    for c in loads[3:]:
        c.start()
    for j in range(J):
        w_copy(0, j).start()

    bar = pltpu.get_barrier_semaphore()
    for d in range(1, M):
        pl.semaphore_signal(bar, inc=1, device_id={"tok": lax.rem(me_t + d, M)}, device_id_type=MESH)
    for d in range(1, N):
        pl.semaphore_signal(bar, inc=1, device_id={"voc": lax.rem(me_v + d, N)}, device_id_type=MESH)

    perm = mix_rows(K)

    @scoped
    def unmix(c):
        chunk = raw.at[:, pl.ds(c * n, n)]
        pltpu.make_async_copy(chunk, chunk, w_sem.at[c]).wait()
        for b in range(c * n // B, (c + 1) * n // B):
            x = jnp.concatenate(
                [raw.at[j].reshape(D * K, 128)[b * 256:(b + 1) * 256, :] for j in range(J)], axis=1)
            rows = jnp.dot(perm, x, preferred_element_type=F32).astype(BF16)
            for k in range(K):
                w[k, b * B:(b + 1) * B, :] = rows[k * B:(k + 1) * B]

    with jax.named_scope("loads"):
        for c in loads[:3]:
            c.wait()
    for c in range(1, chunks):
        for j in range(J):
            w_copy(c, j).start()
    with jax.named_scope("barrier"):
        pl.semaphore_wait(bar, M + N - 2)

    g = z % 2
    zpair = me_t + 2 - 4 * g

    def vw_rows(yy, part):
        return pl.ds(pl.multiple_of(yy * (E // 2) + part * (E // 4), E // 4), E // 4)

    def vw_send():
        for i in range(1, half):
            for c in range(2):
                v = lax.rem(chip + i, half) * 2 + c
                rows = vw_rows(y, g)
                send(vw.at[pl.ds(pl.multiple_of(v * E + rows.start, E // 4), rows.size)],
                     vwe.at[me_v, rows], vx_r.at[me_v], {"voc": v})

    @scoped
    def vw_pass():
        for i in range(1, half):
            ci = lax.rem(chip + i, half)
            for c in range(2):
                arrived(vwe.at[ci * 2 + c, vw_rows(y, g)], vx_r.at[ci * 2 + c])
            piece = vwe.at[pl.ds(ci * 2, 2), vw_rows(y, g)]
            send(piece, piece, vwz_r.at[ci], {"tok": zpair})
            send(piece, piece, vwy_r.at[ci, 0], {"tok": ypart})

    @scoped
    def vw_turn():
        for i in range(1, half):
            ci = lax.rem(chip + i, half)
            piece = vwe.at[pl.ds(ci * 2, 2), vw_rows(y, 1 - g)]
            arrived(piece, vwz_r.at[ci])
            send(piece, piece, vwy_r.at[ci, 1], {"tok": ypart})

    def hid_piece(zz, side, p):
        return hida.at[zz, side, pl.ds(p * (T // 2), T // 2)]

    vw_send()
    for p in range(2):
        piece = hid_piece(z, core, p)
        pl.when(has_r)(remote(piece, piece, own_s.at[0], hz_r.at[z, p], {"tok": me_t + 2}).start)
        pl.when(has_l)(remote(piece, piece, own_s.at[1], hz_r.at[z, p], {"tok": me_t - 2}).start)
    for c in loads[3:]:
        c.wait()
    for d in range(1, N):
        send(mix, mix_all.at[d], mix_r.at[0], {"voc": lax.rem(me_v + d, N)})
    send(vw.at[rows_of(partner, E)], vwe.at[me_v], vp_r.at[0], {"voc": partner})
    for c in range(chunks):
        unmix(c)

    def context(zz, k):
        both = jnp.dot(hida[zz, 0], w[k, 0:H, :], preferred_element_type=F32)
        both = both + jnp.dot(hida[zz, 1], w[k, H:D, :], preferred_element_type=F32)
        return jnp.tanh(both).astype(BF16)

    for k in range(K):
        with jax.named_scope("context"):
            ctx[me_v, k * T:(k + 1) * T, :] = context(z, k)
        if k == 1:
            vw_pass()
        piece = ctx.at[me_v, pl.ds(k * T, T)]
        for i in range(1, half):
            send(piece, piece, ctx_r.at[chip, k],
                 {"voc": lax.rem(chip + i, half) * 2 + core})
        send(piece, piece, ctd_r.at[chip], {"voc": partner})

    @scoped
    def add_logits(s, first=False):
        part = jnp.dot(ctx[s], vw[rows_of(s, E), :], preferred_element_type=F32)
        logit[...] = part if first else logit[...] + part

    @scoped
    def relay_hid(j, p, fwd):
        zz = mate(j)
        there, to = onward(zz)
        piece = hid_piece(zz, core, p)
        on = remote(piece, piece, on_s.at[0, j], hz_r.at[zz, p], {"tok": to})
        over = remote(piece, piece, over_s.at[0], hp_r.at[zz], {"voc": partner})

        @pl.when(there if fwd else jnp.logical_not(there))
        def _():
            arrived(piece, hz_r.at[zz, p])
            if fwd:
                on.start()
            over.start()

    @scoped
    def ctx_mate(j, ks):
        zz = mate(j)
        if ks[0] == 0:
            arrived(hida.at[zz, 1 - core], hp_r.at[zz])
        for k in ks:
            ctxz[zz, k * T:(k + 1) * T, :] = context(zz, k)

    @scoped
    def ctx_pass(k):
        for i in range(1, half):
            s = lax.rem(chip - i + half, half) * 2 + core
            piece = ctx.at[s, pl.ds(k * T, T)]
            arrived(piece, ctx_r.at[s // 2, k])
            send(piece, piece, ctd_r.at[s // 2], {"voc": partner})

    add_logits(me_v, True)
    for j in range(1, min(Z, 3)):
        relay_hid(j, 0, True)
    arrived(ctx.at[partner], ctd_r.at[chip])
    add_logits(partner)

    tcol = column(targets[...].astype(F32), V)
    ids = (me_v * V + lax.broadcasted_iota(jnp.int32, (T, V), 1)).astype(F32)
    onehot = (tcol == ids).astype(F32)
    mix_all[0] = mix[...]
    arrived(mix_all.at[1:N], mix_r.at[0])
    mixing = jnp.zeros((K, T), F32)
    for d in range(N):
        s = lax.rem(me_v - d + N, N)
        mixing = mixing + lax.dot_general(
            mix_all[d],
            hida[z, s // half, :, pl.ds(pl.multiple_of((s % half) * E, E), E)], NT,
            preferred_element_type=F32)
    exp_mix = jnp.exp(mixing)
    weights = exp_mix / jnp.sum(exp_mix, axis=0, keepdims=True)

    for j in range(1, min(Z, 3)):
        relay_hid(j, 1, True)
    ctx_pass(0)
    if Z > 1:
        relay_hid(1, 0, False)
        relay_hid(1, 1, False)
    ctx_pass(1)
    vw_turn()
    if Z > 1:
        ctx_mate(1, range(K))
    for j in range(3, Z):
        relay_hid(j, 0, True)
    ctx_pass(2)
    for j in range(3, Z):
        relay_hid(j, 1, True)
    if Z > 2:
        relay_hid(2, 0, False)
    for k in range(3, K):
        ctx_pass(k)
    if Z > 2:
        relay_hid(2, 1, False)
    for i in range(1, half):
        add_logits(lax.rem(chip - i + half, half) * 2 + core)
    for i in range(1, half):
        s = lax.rem(chip - i + half, half) * 2 + 1 - core
        arrived(ctx.at[s], ctd_r.at[s // 2])
        add_logits(s)

    lane = lax.broadcasted_iota(jnp.int32, (T, 128), 1)
    table = jnp.zeros((T, 128), F32)
    for k in range(K):
        part = jnp.sum(logit[k * T:(k + 1) * T, :] * onehot, axis=1, keepdims=True)
        table = jnp.where(lane == k, part, table)
    tgt[0] = table.T[0:8, :]
    for d in range(1, N):
        send(tgt.at[0], tgt.at[d], tgt_r.at[0], {"voc": lax.rem(me_v + d, N)})
    @scoped
    def scales():
        arrived(tgt.at[1:N], tgt_r.at[0])
        target = tgt[0]
        for d in range(1, N):
            target = target + tgt[d]
        likely = jnp.exp(target[0:K, :] - logz[...])
        joint = weights * likely
        posterior = joint / jnp.sum(joint, axis=0, keepdims=True)
        scale[z, 0:K, :] = loss[...] * posterior
        mgrad[...] = loss[...] * (weights - posterior)
        for d in range(1, Z):
            send(scale.at[z], scale.at[z], sc_r.at[z], {"tok": lax.rem(me_t + 2 * d, M)})

    def shares(zz, k):
        piece = lgall.at[zz, me_v, k]
        return [
            remote(piece, piece, over_s.at[1], lg_r.at[zz, chip, k],
                   {"voc": lax.rem(chip + i, half) * 2 + core})
            for i in range(1, half)
        ] + [remote(piece, piece, over_s.at[2], ld_r.at[zz, k], {"voc": partner})]

    def share(zz, k):
        for c in shares(zz, k):
            c.start()

    @scoped
    def own_out(k):
        rows = slice(k * T, (k + 1) * T)
        logit[rows, :] = jnp.exp(logit[rows, :] - column(logz[k:k + 1, :], V)) - onehot
        lgall[z, me_v, k] = logit[rows, :].astype(BF16)

    @scoped
    def own_share(k):
        share(z, k)

    @scoped
    def own_line(k):
        piece = lgall.at[z, me_v, k]
        pl.when(has_r)(remote(piece, piece, own_s.at[0], lg_r.at[z, chip, k], {"tok": me_t + 2}).start)
        pl.when(has_l)(remote(piece, piece, own_s.at[1], lg_r.at[z, chip, k], {"tok": me_t - 2}).start)
        if k == 0:
            for way, end in ((0, 0), (1, Z - 1)):
                far = remote(piece, piece, own_s.at[2 + way], lg_r.at[z, chip, k],
                             {"tok": me_t + (1 - 2 * way) * (M - 2)})
                pl.when(z == end)(far.start)

    def near_end(zz, there, to):
        end = to // 2
        return there & (end - zz < Z - 1) & (zz - end < Z - 1)

    @scoped
    def relay_lg(k, j, fwd):
        zz = mate(j)
        there, to = onward(zz)
        if k == 0:
            there = near_end(zz, there, to)
        piece = lgall.at[zz, me_v, k]
        on = remote(piece, piece, on_s.at[1 if k == 0 else 0, j], lg_r.at[zz, chip, k], {"tok": to})

        @pl.when(there if fwd else jnp.logical_not(there))
        def _():
            arrived(piece, lg_r.at[zz, chip, k])
            if fwd:
                on.start()
            share(zz, k)

    @scoped
    def cross_lg(k, j):
        zz = mate(j)
        for i in range(1, half):
            s = lax.rem(chip - i + half, half) * 2 + core
            piece = lgall.at[zz, s, k]
            arrived(piece, lg_r.at[zz, s // 2, k])
            remote(piece, piece, over_s.at[3], ld_r.at[zz, k], {"voc": partner}).start()

    @scoped
    def pre_grad(k, j):
        zz = mate(j)
        rows = slice(k * T, (k + 1) * T)
        arrived(lgall.at[zz, 0:half, k], ld_r.at[zz, k])
        total = None
        for s in range(N):
            part = jnp.dot(lgall[zz, s, k], vwt[s], preferred_element_type=F32)
            total = part if total is None else total + part
        c = (ctx[me_v, rows, :] if j == 0 else ctxz[zz, rows, :]).astype(F32)
        if k == 0:
            if j > 0:
                arrived(scale.at[zz], sc_r.at[zz])
        total = total * column(scale[zz, k:k + 1, :], E)
        pg[k, rows_of(zz, T), :] = (total * (1.0 - c * c)).astype(BF16)

    def hid_part(s):
        total = jnp.zeros((T, E), F32)
        for k in range(K):
            total = total + lax.dot_general(
                pg[k, rows_of(z, T), :], w[k, rows_of(s, E), :], NT,
                preferred_element_type=F32)
        return total

    @scoped
    def hid_send(d):
        s = lax.rem(me_v + d, N)
        if d == 0:
            own_hs[...] = hid_part(s)
        else:
            hss[d] = hid_part(s).astype(BF16)
            send(hss.at[d], hsr.at[d], hs_r.at[d], {"voc": s})

    @scoped
    def pair_sums():
        for d in list(range(1, Z)) + [0]:
            zz = lax.rem(z + d, Z)
            arrived(vgy.at[zz], vy_r.at[zz])
            total = vgb[rows_of(zz * 2 + y, R), :].astype(F32) + vgy[zz].astype(F32)
            if d == 0:
                vsum[...] = total
            else:
                vout[zz] = total.astype(BF16)
                send(vout.at[zz], vin.at[z], vz_r.at[z], {"tok": zz * 2 + y})

    pieces = [(k, 0, E) for k in range(K)]
    if E % 256 == 0:
        pieces[-1:] = [(K - 1, 0, E // 2), (K - 1, E // 2, E // 2)]

    @scoped
    def proj_part(k):
        for p, (kk, lo, wide) in enumerate(pieces):
            if kk == k:
                lanes = slice(lo, lo + wide)
                psend[k, :, lanes] = jnp.dot(
                    htr[1 - y], pg[k, :, lanes], preferred_element_type=F32).astype(BF16)
                send(psend.at[k, :, pl.ds(lo, wide)], precv.at[k, :, pl.ds(lo, wide)],
                     pp_r.at[p], {"tok": ypart})
        acc[k] = jnp.dot(htr[y], pg[k], preferred_element_type=F32)

    @scoped
    def vocab_part():
        for k in range(K):
            rows = slice(k * T, (k + 1) * T)
            lg[rows, :] = (column(scale[z, k:k + 1, :], V) * logit[rows, :]).astype(BF16)
        for part in range(0, N, half):
            for s in range(part, part + half):
                vgb[s * E:(s + 1) * E, :] = lax.dot_general(
                    ctx[s], lg[...], TN, preferred_element_type=F32).astype(BF16)
            for zz in range(part * Z // N, (part + half) * Z // N):
                send(vgb.at[pl.ds((zz * 2 + 1 - y) * R, R)], vgy.at[zz], vy_r.at[zz], {"tok": ypart})

    @scoped
    def vw_done():
        vwe[me_v] = vw[rows_of(me_v, E), :]
        arrived(vwe.at[partner], vp_r.at[0])
        for i in range(1, half):
            ci = lax.rem(chip + i, half)
            for p, part in enumerate((g, 1 - g)):
                arrived(vwe.at[pl.ds(ci * 2, 2), vw_rows(1 - y, part)], vwy_r.at[ci, p])
        for s in range(N):
            vwt[s] = vwe[s].T

    @scoped
    def turn():
        for b in range(2):
            col = (z * 2 + b) * R
            for zz in range(Z):
                htr[b, :, zz * T:(zz + 1) * T] = hida[
                    zz, col // H, :, pl.ds(pl.multiple_of(col % H, R), R)].T

    def relay_on(k, j):
        relay_lg(k, j, True)

    def relay_in(k, j):
        relay_lg(k, j, False)

    def mate_ctx(j):
        ctx_mate(j, range(K))

    def hid_in(j, p):
        relay_hid(j, p, False)

    steps = (own_out, own_share, own_line, relay_on, relay_in, cross_lg, pre_grad, proj_part,
             scales, vocab_part, mate_ctx, hid_in, vw_done, turn, hid_send, pair_sums)
    for step, *rest in ORDER:
        steps[step](*rest)

    vtot = vsum[...]
    for d in range(1, Z):
        zz = lax.rem(z + d, Z)
        arrived(vin.at[zz], vz_r.at[zz])
        vtot = vtot + vin[zz].astype(F32)
    out_vocab[...] = vtot.astype(BF16)
    htot = own_hs[...]
    for d in range(1, N):
        arrived(hsr.at[d], hs_r.at[d])
        htot = htot + hsr[d].astype(F32)
    mixf = mix[...].astype(F32)
    for k in range(K):
        htot = htot + column(mgrad[k:k + 1, :], E) * mixf[k:k + 1, :]
    out_hidden[...] = htot.astype(BF16)

    back = mix_rows(K, True)
    for p, (k, lo, wide) in enumerate(pieces):
        lanes = slice(lo, lo + wide)
        with jax.named_scope("precv"):
            arrived(precv.at[k, :, pl.ds(lo, wide)], pp_r.at[p])
        psum = (acc[k, :, lanes] + precv[k, :, lanes].astype(F32)).astype(BF16)
        if k < K - 1:
            precv[k, :, lanes] = psum
            continue
        for b in range(R // B):
            rows = slice(b * B, (b + 1) * B)
            x = jnp.concatenate([precv[q, rows, lanes] for q in range(K - 1)] + [psum[rows]], axis=0)
            out = jnp.dot(back, x, preferred_element_type=F32).astype(BF16)
            for j in range(wide // 128):
                out_proj.at[lo // 128 + j].reshape(R * K, 128)[b * 256:(b + 1) * 256, :] = (
                    out[:, j * 128:(j + 1) * 128])
    with jax.named_scope("drain"):
        for i, size in enumerate(groups):
            sent(all_s.at[i], size)
        piece = T * V * 2
        sent(over_s.at[0], (Z - 1) * T * D)
        for i in range(1, 4):
            for _ in range(half - 1):
                sent(over_s.at[i], Z * K * piece)
        for way, pred in ((0, has_r), (1, has_l)):
            pl.when(pred)(functools.partial(sent, own_s.at[way], T * D + K * piece))
        for way, end in ((0, 0), (1, Z - 1)):
            pl.when(z == end)(functools.partial(sent, own_s.at[2 + way], piece))
        for j in range(1, Z):
            zz = mate(j)
            there, to = onward(zz)
            pl.when(there)(functools.partial(sent, on_s.at[0, j], T * D + (K - 1) * piece))
            pl.when(near_end(zz, there, to))(functools.partial(sent, on_s.at[1, j], piece))


def body_fast(M, N, hidden, mix_weight, comp_proj, vocab_weight, log_normalizer, targets, loss_grad):
    T, D = hidden.shape
    K, E = mix_weight.shape
    V = vocab_weight.shape[1]
    R = D // M
    J = E // 128
    half = N // 2
    Z = M // 2
    vm = pltpu.VMEM
    dma = pltpu.SemaphoreType.DMA
    scratch = [
        vm((J, D, K, 128), BF16), vm((K, D, E), BF16), vm((Z, 2, T, D // 2), BF16), vm((D, V), BF16),
        vm((N, E, V), BF16), vm((N, V, E), BF16), vm((K, E), BF16), vm((K, T), F32), vm((1, T), jnp.int32), vm((1, T), F32),
        vm((N, K * T, E), BF16), vm((Z, K * T, E), BF16), vm((N, K, E), BF16), vm((2, R, Z * T), BF16),
        vm((K * T, V), F32), vm((K * T, V), BF16), vm((Z, N, K, T, V), BF16), vm((N, 8, T), F32), vm((Z, 8, T), F32), vm((K, Z * T, E), BF16),
        vm((D, V), BF16), vm((Z, R, V), BF16),
        vm((R, V), F32), vm((Z, R, V), BF16), vm((Z, R, V), BF16),
        vm((N, T, E), BF16), vm((N, T, E), BF16),
        vm((T, E), F32), vm((K, R, E), F32), vm((K, R, E), BF16), vm((K, R, E), BF16),
        vm((K, T), F32),
        dma((7,)), dma((4,)), dma((8,)), dma((4,)), dma((4,)), dma((2, Z)),
        dma((half, K)), dma((half,)), dma((1,)), dma((Z, 2)), dma((Z,)), dma((N,)), dma((1,)), dma((half,)), dma((half, 2)),
        dma((1,)), dma((Z, half, K)), dma((Z, K)), dma((Z,)), dma((Z,)), dma((N,)), dma((K + 1,)), dma((Z,)),
    ]
    spec = pl.BlockSpec(memory_space=pltpu.VMEM)
    hbm = pl.BlockSpec(memory_space=pltpu.MemorySpace.HBM)
    hid, proj, voc = pl.pallas_call(
        functools.partial(fast_kernel, M, N),
        out_shape=(
            jax.ShapeDtypeStruct((T, E), BF16),
            jax.ShapeDtypeStruct((J, R, K, 128), BF16),
            jax.ShapeDtypeStruct((R, V), BF16),
        ),
        in_specs=[hbm] * 7,
        out_specs=(spec, spec, spec),
        scratch_shapes=scratch,
        compiler_params=pltpu.CompilerParams(
            collective_id=0, has_side_effects=True, vmem_limit_bytes=47 * 1024 * 1024
        ),
    )(*[
        pltpu.with_memory_space_constraint(x, pltpu.MemorySpace.HBM)
        for x in (hidden, mix_weight, comp_proj, vocab_weight, log_normalizer, targets[None, :], loss_grad[None, :])
    ])
    return pl.pallas_call(
        store_kernel,
        out_shape=(
            jax.ShapeDtypeStruct((T, E), BF16),
            jax.ShapeDtypeStruct((R, K, E), BF16),
            jax.ShapeDtypeStruct((R, V), BF16),
        ),
        in_specs=[spec] * 3,
        out_specs=(hbm, hbm, hbm),
        scratch_shapes=[dma((J + 2,))],
        compiler_params=pltpu.CompilerParams(vmem_limit_bytes=4 * 1024 * 1024),
    )(hid, proj, voc)


def store_kernel(hid, proj, voc, out_hid, out_proj, out_voc, sem):
    J = proj.shape[0]
    copies = [pltpu.make_async_copy(hid, out_hid, sem.at[J]), pltpu.make_async_copy(voc, out_voc, sem.at[J + 1])]
    for j in range(J):
        copies.append(pltpu.make_async_copy(proj.at[j], out_proj.at[:, :, pl.ds(j * 128, 128)], sem.at[j]))
    for c in copies:
        c.start()
    for c in copies:
        c.wait()


def body(M, N, *args):
    hidden, mix_weight, comp_proj, vocab_weight = args[:4]
    T, D = hidden.shape
    K, E = mix_weight.shape
    V = vocab_weight.shape[1]
    gathered = 2 * (M // 2) * T * (K * N * V + D + 2 * K * E)
    shapes = K == 4 and M == 8 and N == 4 and E % 128 == 0 and (D // M) % (256 // K) == 0
    if shapes and gathered + 4 * K * D * E <= 28 * 1024 * 1024:
        return body_fast(M, N, *args)
    return body_base(M, N, *args)


def solution(mesh):
    in_specs = (
        P("tok", None),
        P(None, "voc"),
        P(None, None, "voc"),
        P(None, "voc"),
        P(None, "tok"),
        P("tok"),
        P("tok"),
    )
    out_specs = (P("tok", "voc"), P("tok", None, "voc"), P("tok", "voc"))
    return jax.shard_map(
        functools.partial(body, mesh.shape["tok"], mesh.shape["voc"]),
        mesh=mesh, in_specs=in_specs, out_specs=out_specs, check_vma=False,
    )
```
